128 devices in a mesh: ctx: 32 (over z, y, x_hi), dp: 4 (over x_lo, core).
Axes of the slice: x: 4 (x_hi: 2, x_lo: 2; x = x_hi * 2 + x_lo), y: 4, z: 4, core: 2. Of those that a mesh axis runs over, the one named last changes fastest.
Arguments:
- tokens: bfloat16 [8, 2048, 4096], P('dp', 'ctx'), may hold values from -6 to 6
- queries: bfloat16 [8, 2048, 2048], P('dp', 'ctx'), may hold values from -160 to 160
- d_attended: bfloat16 [8, 2048, 2048], P('dp', 'ctx'), may hold values from -6 to 6
- span_order: int32 [64], replicated, may hold values from 0 to 63, each once
- norm_gain: float32 [4096], replicated, may hold values from 0.1 to 1.9
- key_weight: bfloat16 [4096, 512], replicated, may hold values from -0.09375 to 0.09375
- value_weight: bfloat16 [4096, 512], replicated, may hold values from -0.09375 to 0.09375
Outputs:
- attended: bfloat16 [8, 2048, 2048], P('dp', 'ctx')
- grad_queries: bfloat16 [8, 2048, 2048], P('dp', 'ctx')
- grad_tokens: bfloat16 [8, 2048, 4096], P('dp', 'ctx')
- grad_key_weight: float32 [4096, 512], P(('ctx', 'dp'))
- grad_value_weight: float32 [4096, 512], P(('ctx', 'dp'))
- grad_gain: float32 [4096], P(('ctx', 'dp'))
The draws below stay inside these ranges and needn't reach their ends.
All inputs are finite; a program needn't handle non-finite values.
Results may differ from the reference program's by a relative error of at most 0.025.
The reference program's roundings to bfloat16 on the way (of `normed`, `rotated_keys`, `value_rows`, `probability_b`, `dscores`, `key_pre_grad` and `value_pre_grad`) count: a program that leaves them out, or rounds other values in their place, can miss the bound.
Values may be sent and summed in bfloat16 or wider, within the bound.
A program may use at most 192 MiB of HBM per device.

```python
import jax
import jax.numpy as jnp
from jax import lax

D = 4096
HEADS = 16
KV_HEADS = 4
HEAD_DIM = 128
SEQ_DEV = 64
SEQ = 2048
SEQS = 8
N_CTX = 32


def draw_queries(key, part):
    full_shape = (SEQS, SEQ, HEADS * HEAD_DIM)
    sample = jnp.clip(jax.random.normal(key, full_shape, jnp.float32), -4.0, 4.0)
    return sample.astype(jnp.bfloat16)


def shard_levels(own_key, extent, shards, smallest, largest):
    factor_of = 1.0
    for axis_at, parts in shards:
        heights = jax.random.uniform(jax.random.fold_in(jax.random.fold_in(own_key, 6), axis_at), (parts,), jnp.float32, smallest / len(shards), largest / len(shards))
        factor_of = factor_of * jnp.repeat(jnp.exp(heights), extent[axis_at] // parts).reshape((-1,) + (1,) * (len(extent) - 1 - axis_at))
    return factor_of


def gaussian(key, shape, scale, limit, shards=(), kind=jnp.bfloat16):
    factor_of = shard_levels(key, shape, shards, -0.22, 0.18) if shards else 1.0
    entries = jax.random.normal(key, shape, jnp.float32) * scale * factor_of
    return jnp.minimum(jnp.maximum(entries, -limit), limit).astype(kind)


def setup_inputs(seed: int = 0) -> dict:
    arg_keys = jax.random.split(jax.random.key(seed), 8)
    return {
        "tokens": gaussian(arg_keys[0], (SEQS, SEQ, D), 1.0, 6.0, ((0, 4), (1, 32))),
        "queries": draw_queries(jax.random.fold_in(arg_keys[7], 71), 0),
        "d_attended": gaussian(arg_keys[2], (SEQS, SEQ, HEADS * HEAD_DIM), 1.0, 6.0, ((0, 4), (1, 32))),
        "span_order": jax.random.permutation(arg_keys[3], 2 * N_CTX).astype(jnp.int32),
        "norm_gain": jnp.clip(1.0 + 0.18 * jax.random.normal(arg_keys[4], (D,), jnp.float32), 0.1, 1.9),
        "key_weight": gaussian(arg_keys[5], (D, KV_HEADS * HEAD_DIM), D ** -0.5, 0.09375),
        "value_weight": gaussian(arg_keys[6], (D, KV_HEADS * HEAD_DIM), D ** -0.5, 0.09375),
    }


ROPE_BASE = 500000.0
EPSILON = 1e-05

def positions(span_order, span_len):
    offsets = jnp.arange(span_len, dtype=jnp.int32)
    return (span_order[:, None] * span_len + offsets[None, :]).reshape(-1).astype(jnp.int32)

def rotation(token_pos, head_size):
    half_dim = head_size // 2
    frequency = ROPE_BASE ** (-2.0 * jnp.arange(half_dim, dtype=jnp.float32) / head_size)
    angles = token_pos.astype(jnp.float32)[:, None] * frequency[None, :]
    angles = jnp.concatenate([angles, angles], axis=1)
    return (jnp.cos(angles), jnp.sin(angles))

def rotate_half(values):
    half_dim = values.shape[-1] // 2
    return jnp.concatenate([-values[..., half_dim:], values[..., :half_dim]], axis=-1)

def rotate_back(values):
    half_dim = values.shape[-1] // 2
    return jnp.concatenate([values[..., half_dim:], -values[..., :half_dim]], axis=-1)

def normalize(tokens, norm_gain):
    widened = tokens.astype(jnp.float32)
    rms_scale = lax.rsqrt(lax.optimization_barrier(jnp.mean(widened * widened, axis=-1, keepdims=True)) + EPSILON)
    return ((widened * rms_scale * norm_gain).astype(jnp.bfloat16), rms_scale)

def project_keys(normed, key_weight, value_weight, cosine, sine_table, kv_heads, head_size):
    row_count = normed.shape[0]
    key_pre = jnp.dot(normed, key_weight, preferred_element_type=jnp.float32).reshape(row_count, kv_heads, head_size)
    rotated = key_pre * cosine[:, None, :] + rotate_half(key_pre) * sine_table[:, None, :]
    value_rows = jnp.dot(normed, value_weight, preferred_element_type=jnp.float32)
    return (rotated.reshape(row_count, kv_heads * head_size).astype(jnp.bfloat16), value_rows.astype(jnp.bfloat16))

def attend_group(query_group, grad_group, key_group, value_group, causal_mask, score_scale):
    query_wide = query_group.astype(jnp.float32)
    grad_wide = grad_group.astype(jnp.float32)
    key_wide = key_group.astype(jnp.float32)
    value_wide = value_group.astype(jnp.float32)
    scores = jnp.einsum('tgd,sd->gts', query_wide, key_wide) * score_scale
    scores = jnp.where(causal_mask[None], scores, -1e+30)
    row_max = lax.optimization_barrier(jnp.max(scores, axis=-1, keepdims=True))
    exponent = jnp.exp(scores - row_max)
    probability = exponent / lax.optimization_barrier(jnp.sum(exponent, axis=-1, keepdims=True))
    probability_b = probability.astype(jnp.bfloat16)
    prob_wide = probability_b.astype(jnp.float32)
    attended = jnp.einsum('gts,sd->tgd', prob_wide, value_wide).astype(jnp.bfloat16)
    dprob = jnp.einsum('tgd,sd->gts', grad_wide, value_wide)
    delta = lax.optimization_barrier(jnp.sum(grad_wide * attended.astype(jnp.float32), axis=-1))
    dscores = (probability * (dprob - jnp.transpose(delta)[:, :, None])).astype(jnp.bfloat16)
    dscore_wide = dscores.astype(jnp.float32)
    dquery = (jnp.einsum('gts,sd->tgd', dscore_wide, key_wide) * score_scale).astype(jnp.bfloat16)
    key_term = jnp.einsum('gts,tgd->sd', dscore_wide, query_wide) * score_scale
    value_term = jnp.einsum('gts,tgd->sd', prob_wide, grad_wide)
    return (attended, dquery, key_term, value_term)

def attend_device(queries, grads, all_keys, all_values, query_pos, key_pos, kv_heads, head_size):
    row_count = queries.shape[0]
    group_size = queries.shape[1] // (kv_heads * head_size)
    group_width = group_size * head_size
    causal_mask = key_pos[None, :] <= query_pos[:, None]
    score_scale = head_size ** (-0.5)
    outputs = []
    for head_group in range(kv_heads):
        query_group = queries[:, head_group * group_width:(head_group + 1) * group_width].reshape(row_count, group_size, head_size)
        grad_group = grads[:, head_group * group_width:(head_group + 1) * group_width].reshape(row_count, group_size, head_size)
        key_group = all_keys[:, head_group * head_size:(head_group + 1) * head_size]
        value_group = all_values[:, head_group * head_size:(head_group + 1) * head_size]
        outputs.append(attend_group(query_group, grad_group, key_group, value_group, causal_mask, score_scale))
    attended = jnp.concatenate([item[0].reshape(row_count, group_width) for item in outputs], axis=1)
    dquery = jnp.concatenate([item[1].reshape(row_count, group_width) for item in outputs], axis=1)
    key_terms = jnp.concatenate([item[2] for item in outputs], axis=1)
    value_terms = jnp.concatenate([item[3] for item in outputs], axis=1)
    return (attended, dquery, key_terms, value_terms)

def finish_backward(tokens, normed, rms_scale, key_grad, value_grad, cosine, sine_table, norm_gain, key_weight, value_weight, kv_heads, head_size):
    row_count = tokens.shape[0]
    shaped = key_grad.reshape(row_count, kv_heads, head_size)
    key_pre_grad = (shaped * cosine[:, None, :] + rotate_back(shaped * sine_table[:, None, :])).reshape(row_count, kv_heads * head_size).astype(jnp.bfloat16)
    value_pre_grad = value_grad.astype(jnp.bfloat16)
    weight_key = jnp.dot(normed.T, key_pre_grad, preferred_element_type=jnp.float32)
    weight_value = jnp.dot(normed.T, value_pre_grad, preferred_element_type=jnp.float32)
    normed_grad = jnp.dot(key_pre_grad, key_weight.T, preferred_element_type=jnp.float32) + jnp.dot(value_pre_grad, value_weight.T, preferred_element_type=jnp.float32)
    widened = tokens.astype(jnp.float32)
    gain_part = lax.optimization_barrier(jnp.sum(normed_grad * widened * rms_scale, axis=0))
    inner_mean = lax.optimization_barrier(jnp.mean(normed_grad * norm_gain * widened, axis=-1, keepdims=True))
    grad_rows = (rms_scale * norm_gain * normed_grad - widened * rms_scale ** 3 * inner_mean).astype(jnp.bfloat16)
    return (grad_rows, weight_key, weight_value, gain_part)

def reference(tokens, queries, d_attended, span_order, norm_gain, key_weight, value_weight):
    token_pos = positions(span_order, SEQ_DEV // 2)
    cosine, sine_table = rotation(token_pos, HEAD_DIM)
    kv_width = KV_HEADS * HEAD_DIM
    total_key = jnp.zeros((D, kv_width), jnp.float32)
    total_value = jnp.zeros((D, kv_width), jnp.float32)
    total_gain = jnp.zeros((D,), jnp.float32)
    attended_list, dquery_list, dtoken_list = ([], [], [])
    for sequence in range(SEQS):
        normed, rms_scale = normalize(tokens[sequence], norm_gain)
        rotated_keys, value_rows = project_keys(normed, key_weight, value_weight, cosine, sine_table, KV_HEADS, HEAD_DIM)
        seq_queries = queries[sequence]
        seq_grads = d_attended[sequence]

        def shard_step(totals, shard_index):
            first_row = shard_index * SEQ_DEV
            block_queries = lax.dynamic_slice_in_dim(seq_queries, first_row, SEQ_DEV, 0)
            block_grads = lax.dynamic_slice_in_dim(seq_grads, first_row, SEQ_DEV, 0)
            query_pos = lax.dynamic_slice_in_dim(token_pos, first_row, SEQ_DEV, 0)
            attended, dquery, key_terms, value_terms = attend_device(block_queries, block_grads, rotated_keys, value_rows, query_pos, token_pos, KV_HEADS, HEAD_DIM)
            key_round = lax.optimization_barrier(key_terms.astype(jnp.bfloat16)).astype(jnp.float32)
            value_round = lax.optimization_barrier(value_terms.astype(jnp.bfloat16)).astype(jnp.float32)
            return ((totals[0] + key_round, totals[1] + value_round), (attended, dquery))
        zeros_init = jnp.zeros((SEQ, kv_width), jnp.float32)
        sums, stacked = lax.scan(shard_step, (zeros_init, zeros_init), jnp.arange(N_CTX, dtype=jnp.int32))
        attended_list.append(stacked[0].reshape(SEQ, HEADS * HEAD_DIM))
        dquery_list.append(stacked[1].reshape(SEQ, HEADS * HEAD_DIM))
        grad_rows, weight_key, weight_value, gain_part = finish_backward(tokens[sequence], normed, rms_scale, sums[0], sums[1], cosine, sine_table, norm_gain, key_weight, value_weight, KV_HEADS, HEAD_DIM)
        dtoken_list.append(grad_rows)
        total_key = total_key + weight_key
        total_value = total_value + weight_value
        total_gain = total_gain + gain_part
    return (jnp.stack(attended_list), jnp.stack(dquery_list), jnp.stack(dtoken_list), total_key, total_value, total_gain)
```

```python
import functools
import math

import jax
import jax.numpy as jnp
from jax import lax
from jax.experimental import pallas as pl
from jax.experimental.pallas import tpu as pltpu
from jax.sharding import PartitionSpec as P

KV_HEADS = 4
HEAD_DIM = 128
ROPE_BASE = 500000.0
EPSILON = 1e-05
BF = jnp.bfloat16
F32 = jnp.float32
VM = pltpu.VMEM
MESH = pl.DeviceIdType.MESH


def flip1(a):
    return a + 1 - 2 * (a % 2)


def flip3(a):
    return 3 - a


def flip2(a):
    return (a + 2) % 4


class Here:
    def __init__(self):
        ctx = lax.axis_index("ctx")
        dp = lax.axis_index("dp")
        self.z = ctx // 8
        self.y = (ctx // 2) % 4
        self.xh = ctx % 2
        self.xl = dp // 2
        self.core = dp % 2
        self.x = self.xh * 2 + self.xl

    def at(self, z=None, y=None, x=None, core=None):
        z = self.z if z is None else z
        y = self.y if y is None else y
        core = self.core if core is None else core
        if x is None:
            xh, xl = self.xh, self.xl
        else:
            xh, xl = x // 2, x % 2
        return {"ctx": z * 8 + y * 2 + xh, "dp": xl * 2 + core}


class Net:
    def __init__(self, send_sems, recv_sems):
        self.send_sems = send_sems
        self.recv_sems = recv_sems
        self.made = []

    def start(self, src, dst, device):
        k = len(self.made)
        copy = pltpu.make_async_remote_copy(
            src_ref=src,
            dst_ref=dst,
            send_sem=self.send_sems.at[k],
            recv_sem=self.recv_sems.at[k],
            device_id=device,
            device_id_type=MESH,
        )
        copy.start()
        self.made.append(copy)
        return copy

    def finish(self):
        for copy in self.made:
            copy.wait_send()


def greet(devices):
    barrier = pltpu.get_barrier_semaphore()
    for device in devices:
        pl.semaphore_signal(barrier, inc=1, device_id=device, device_id_type=MESH)
    pl.semaphore_wait(barrier, len(devices))


def cols(index, width):
    return pl.ds(pl.multiple_of(index * width, width), width)


N_FRONT = 2 * 3 * 3 + 2 * (1 + 2 * (2 + 4)) + 1


def front_kernel(q, do, kv, nrm, qr, dr, kvr, nrm2, send_sems, recv_sems, local_sems):
    here = Here()
    z, y, xh = here.z, here.y, here.xh
    x2 = flip2(here.x)
    greet(
        [here.at(z=f(z)) for f in (flip1, flip3, flip2)]
        + [here.at(y=f(y)) for f in (flip1, flip3, flip2)]
        + [here.at(x=x2), here.at(core=1 - here.core)]
    )
    net = Net(send_sems, recv_sems)

    def along(s, value):
        return here.at(z=value) if s == 0 else here.at(y=value)

    def across(s, value):
        return here.at(y=value) if s == 0 else here.at(z=value)

    head = [z, y]
    ring = [y, z]
    local = []

    def keep(src, dst):
        copy = pltpu.make_async_copy(src, dst, local_sems.at[len(local)])
        copy.start()
        local.append(copy)

    mine = [ring[s] * 2 + xh for s in range(2)]
    kv_copies = [[], []]
    for s in range(2):
        keep(kv.at[s, :, cols(head[s], 256)], kvr.at[s, mine[s], head[s]])
    for f in (flip1, flip3, flip2):
        for s in range(2):
            to = f(head[s])
            kv_copies[s].append(
                net.start(kv.at[s, :, cols(to, 256)], kvr.at[s, mine[s], head[s]], along(s, to))
            )
    rest = []
    for f in (flip1, flip3, flip2):
        for s in range(2):
            to = f(head[s])
            for src, dst in ((q, qr), (do, dr)):
                rest.append(net.start(src.at[s, :, cols(to, 512)], dst.at[s, head[s]], along(s, to)))
    for s in range(2):
        keep(q.at[s, :, cols(head[s], 512)], qr.at[s, head[s]])
        keep(do.at[s, :, cols(head[s], 512)], dr.at[s, head[s]])
    for s in range(2):
        local[s].wait()
        for copy in kv_copies[s]:
            copy.wait_recv()

    first = [[], []]
    second = [[], []]
    last = []

    def spread(s, xh_of):
        slot = ring[s] * 2 + xh_of
        for half, f in ((0, flip1), (1, flip3)):
            block = kvr.at[s, slot, 2 * half : 2 * half + 2]
            first[s].append(net.start(block, block, across(s, f(ring[s]))))

    def spread_on(s, xh_of):
        for half, f, g in ((0, flip1, flip3), (1, flip3, flip1)):
            first[s].pop(0).wait_recv()
            for value in (ring[s], f(ring[s])):
                block = kvr.at[s, value * 2 + xh_of, 2 * half : 2 * half + 2]
                last.append(net.start(block, block, across(s, g(ring[s]))))

    swapped = []
    for s in range(2):
        block = kvr.at[s, mine[s]]
        swapped.append(net.start(block, block, here.at(x=x2)))
        spread(s, xh)
    rest.append(net.start(nrm, nrm2, here.at(core=1 - here.core)))
    for s in range(2):
        spread_on(s, xh)
    for s in range(2):
        swapped[s].wait_recv()
        spread(s, 1 - xh)
    for s in range(2):
        spread_on(s, 1 - xh)
    for copy in last + rest:
        copy.wait_recv()
    for copy in local[2:]:
        copy.wait()
    net.finish()


def front(q, do, kv, nrm):
    vm = pl.BlockSpec(memory_space=VM)
    return pl.pallas_call(
        front_kernel,
        name="front",
        out_shape=(
            jax.ShapeDtypeStruct((2, 4, 64, 512), BF),
            jax.ShapeDtypeStruct((2, 4, 64, 512), BF),
            jax.ShapeDtypeStruct((2, 8, 4, 64, 256), BF),
            jax.ShapeDtypeStruct(nrm.shape, BF),
        ),
        in_specs=[vm] * 4,
        out_specs=(vm,) * 4,
        scratch_shapes=[
            pltpu.SemaphoreType.DMA((N_FRONT,)),
            pltpu.SemaphoreType.DMA((N_FRONT,)),
            pltpu.SemaphoreType.DMA((6,)),
        ],
        compiler_params=pltpu.CompilerParams(collective_id=1, has_side_effects=True),
    )(q, do, kv, nrm)


CHUNK = 256
KEYS = 2048


def attend_kernel(
    q_ref, do_ref, kv_ref, qpos_ref, kpos_ref, att_ref, dq_ref, term_ref,
    score, prob, key_t, value_t, acc_k, acc_v,
):
    block = pl.program_id(1)
    chunks = KEYS // CHUNK
    scale = HEAD_DIM ** (-0.5)
    to_two = scale * math.log2(math.e)

    @pl.when(block == 0)
    def _():
        key_t[...] = kv_ref[0, :, :128].T
        value_t[...] = kv_ref[0, :, 128:].T
        acc_k[...] = jnp.zeros_like(acc_k)
        acc_v[...] = jnp.zeros_like(acc_v)

    q = jnp.concatenate([q_ref[0, 0, :, h * 128 : (h + 1) * 128] for h in range(4)], axis=0)
    do = jnp.concatenate([do_ref[0, 0, :, h * 128 : (h + 1) * 128] for h in range(4)], axis=0)
    q_t = q.T
    do_t = do.T
    q_pos = qpos_ref[0, 0]

    def rows(c):
        return pl.ds(pl.multiple_of(c * CHUNK, CHUNK), CHUNK)

    def scores_of(c, top):
        s = jnp.dot(kv_ref[0, rows(c), :128], q_t, preferred_element_type=F32)
        k_pos = kpos_ref[0, rows(c), :]
        k_pos = jnp.concatenate([k_pos, k_pos], axis=1)
        s = jnp.where(k_pos <= q_pos, s, -1e30)
        score[rows(c), :] = s
        return jnp.maximum(top, jnp.max(s.reshape(CHUNK // 8, 8, 256), axis=0))

    top = lax.fori_loop(0, chunks, scores_of, jnp.full((8, 256), -1e30, F32), unroll=True)
    top = jnp.max(top, axis=0, keepdims=True)

    def exps_of(c, total):
        e = jnp.exp2((score[rows(c), :] - top) * to_two)
        score[rows(c), :] = e
        return total + jnp.sum(e.reshape(CHUNK // 8, 8, 256), axis=0)

    total = lax.fori_loop(0, chunks, exps_of, jnp.zeros((8, 256), F32), unroll=True)
    inverse = 1.0 / jnp.sum(total, axis=0, keepdims=True)

    def attended_of(c, out):
        p = (score[rows(c), :] * inverse).astype(BF)
        prob[rows(c), :] = p
        return out + jnp.dot(value_t[:, rows(c)], p, preferred_element_type=F32)

    out_t = lax.fori_loop(0, chunks, attended_of, jnp.zeros((128, 256), F32), unroll=True)
    out_t = out_t.astype(BF)
    delta = jnp.sum(out_t.astype(F32) * do_t.astype(F32), axis=0, keepdims=True)

    def grads_of(c, dq_t):
        dp = jnp.dot(kv_ref[0, rows(c), 128:], do_t, preferred_element_type=F32)
        ds = (score[rows(c), :] * inverse * (dp - delta)).astype(BF)
        acc_k[rows(c), :] += jnp.dot(ds, q, preferred_element_type=F32)
        acc_v[rows(c), :] += jnp.dot(prob[rows(c), :], do, preferred_element_type=F32)
        return dq_t + jnp.dot(key_t[:, rows(c)], ds, preferred_element_type=F32)

    dq_t = lax.fori_loop(0, chunks, grads_of, jnp.zeros((128, 256), F32), unroll=True)
    out = out_t.T
    dq = (dq_t * scale).astype(BF).T
    for h in range(4):
        att_ref[0, 0, :, h * 128 : (h + 1) * 128] = out[h * 64 : (h + 1) * 64]
        dq_ref[0, 0, :, h * 128 : (h + 1) * 128] = dq[h * 64 : (h + 1) * 64]

    @pl.when(block == 3)
    def _():
        term_ref[0, :, :128] = (acc_k[...] * scale).astype(BF)
        term_ref[0, :, 128:] = acc_v[...].astype(BF)


def attend(qr, dr, kvr, q_pos, k_pos):
    rows = pl.BlockSpec((1, 1, 64, 512), lambda s, b: (s, b, 0, 0))
    whole = pl.BlockSpec((1, KEYS, 256), lambda s, b: (s, 0, 0))
    return pl.pallas_call(
        attend_kernel,
        name="attend",
        grid=(2, 4),
        out_shape=(
            jax.ShapeDtypeStruct((2, 4, 64, 512), BF),
            jax.ShapeDtypeStruct((2, 4, 64, 512), BF),
            jax.ShapeDtypeStruct((2, KEYS, 256), BF),
        ),
        in_specs=[
            rows,
            rows,
            whole,
            pl.BlockSpec((1, 1, 1, 256), lambda s, b: (s, b, 0, 0)),
            pl.BlockSpec((1, KEYS, 128), lambda s, b: (s, 0, 0)),
        ],
        out_specs=(rows, rows, whole),
        scratch_shapes=[
            VM((KEYS, 256), F32),
            VM((KEYS, 256), BF),
            VM((128, KEYS), BF),
            VM((128, KEYS), BF),
            VM((KEYS, 128), F32),
            VM((KEYS, 128), F32),
        ],
        compiler_params=pltpu.CompilerParams(
            dimension_semantics=("arbitrary", "arbitrary"), vmem_limit_bytes=48 * 2**20
        ),
        cost_estimate=pl.CostEstimate(
            flops=6_500_000_000, bytes_accessed=12_000_000, transcendentals=4_200_000
        ),
    )(qr, dr, kvr, q_pos, k_pos)


N_BACK = 2 * (2 * 3 + 4 + 2 + 1 + 3)


def back_kernel(
    att, dq, term, att_out, dq_out, dkv_out,
    got1, sum1, got2, part, got3, final, send_sems, recv_sems, local_sems,
):
    here = Here()
    z, y, xh = here.z, here.y, here.xh
    x2 = flip2(here.x)
    greet(
        [here.at(z=f(z)) for f in (flip1, flip3, flip2)]
        + [here.at(y=f(y)) for f in (flip1, flip3, flip2)]
        + [here.at(x=x2)]
    )
    net = Net(send_sems, recv_sems)

    def along(s, value):
        return here.at(z=value) if s == 0 else here.at(y=value)

    def across(s, value):
        return here.at(y=value) if s == 0 else here.at(z=value)

    head = [z, y]
    ring = [y, z]
    flips = ((flip3, flip1), (flip1, flip3))

    def slots(value):
        return pl.ds(value * 2, 2)

    one = {}
    for j in (1, 0):
        for s in range(2):
            for half in range(2):
                f, g = flips[half]
                target = f(ring[s])
                slot = target if j == 0 else g(target)
                one[s, half, j] = net.start(
                    term.at[s, slots(slot), 2 * half : 2 * half + 2],
                    got1.at[s, half, j],
                    across(s, target),
                )
    rest = []
    local = []
    for f in (flip1, flip3, flip2):
        for s in range(2):
            to = f(head[s])
            for src, dst in ((att, att_out), (dq, dq_out)):
                rest.append(net.start(src.at[s, to], dst.at[s, :, cols(head[s], 512)], along(s, to)))
    for s in range(2):
        for src, dst in ((att, att_out), (dq, dq_out)):
            copy = pltpu.make_async_copy(
                src.at[s, head[s]], dst.at[s, :, cols(head[s], 512)], local_sems.at[len(local)]
            )
            copy.start()
            local.append(copy)

    two = {}
    for s in range(2):
        for half in range(2):
            f, g = flips[half]
            one[s, half, 1].wait_recv()
            sum1[s, half] = (
                term[s, slots(g(ring[s])), 2 * half : 2 * half + 2].astype(F32)
                + got1[s, half, 1].astype(F32)
            ).astype(BF)
            two[s, half] = net.start(sum1.at[s, half], got2.at[s, half], across(s, g(ring[s])))
    three = []
    for s in range(2):
        for half in range(2):
            one[s, half, 0].wait_recv()
            two[s, half].wait_recv()
            part[s, :, 2 * half : 2 * half + 2] = (
                term[s, slots(ring[s]), 2 * half : 2 * half + 2].astype(F32)
                + got1[s, half, 0].astype(F32)
                + got2[s, half].astype(F32)
            ).astype(BF)
        three.append(net.start(part.at[s, 1 - xh], got3.at[s], here.at(x=x2)))
    for s in range(2):
        three[s].wait_recv()
        final[s] = (part[s, xh].astype(F32) + got3[s].astype(F32)).astype(BF)
        for f in (flip1, flip3, flip2):
            to = f(head[s])
            rest.append(net.start(final.at[s, to], dkv_out.at[s, :, cols(head[s], 256)], along(s, to)))
        copy = pltpu.make_async_copy(
            final.at[s, head[s]], dkv_out.at[s, :, cols(head[s], 256)], local_sems.at[len(local)]
        )
        copy.start()
        local.append(copy)
    for copy in rest:
        copy.wait_recv()
    for copy in local:
        copy.wait()
    net.finish()


def back(att, dq, term):
    vm = pl.BlockSpec(memory_space=VM)
    return pl.pallas_call(
        back_kernel,
        name="back",
        out_shape=(
            jax.ShapeDtypeStruct((2, 64, 2048), BF),
            jax.ShapeDtypeStruct((2, 64, 2048), BF),
            jax.ShapeDtypeStruct((2, 64, 1024), BF),
        ),
        in_specs=[vm] * 3,
        out_specs=(vm,) * 3,
        scratch_shapes=[
            VM((2, 2, 2, 2, 2, 64, 256), BF),
            VM((2, 2, 2, 2, 64, 256), BF),
            VM((2, 2, 2, 2, 64, 256), BF),
            VM((2, 2, 4, 64, 256), BF),
            VM((2, 4, 64, 256), BF),
            VM((2, 4, 64, 256), BF),
            pltpu.SemaphoreType.DMA((N_BACK,)),
            pltpu.SemaphoreType.DMA((N_BACK,)),
            pltpu.SemaphoreType.DMA((6,)),
        ],
        compiler_params=pltpu.CompilerParams(collective_id=2, has_side_effects=True),
    )(att, dq, term)


def outer_kernel(n0_ref, n1_ref, g0_ref, g1_ref, out_ref):
    n = jnp.concatenate([n0_ref[...], n1_ref[...]], axis=0)
    g = jnp.concatenate([g0_ref[...], g1_ref[...]], axis=0)
    w = lax.dot_general(n, g, (((0,), (0,)), ((), ())), preferred_element_type=F32).astype(BF)
    for x in range(4):
        for u in range(4):
            at = x * 64 + u * 16
            out_ref[u, 0, x] = w[at : at + 16]


def outer(n0, n1, g0, g1):
    n_spec = pl.BlockSpec((128, 256), lambda i: (0, i))
    g_spec = pl.BlockSpec((128, 512), lambda i: (0, 0))
    return pl.pallas_call(
        outer_kernel,
        name="outer",
        grid=(16,),
        out_shape=jax.ShapeDtypeStruct((4, 16, 4, 16, 512), BF),
        in_specs=[n_spec, n_spec, g_spec, g_spec],
        out_specs=pl.BlockSpec((4, 1, 4, 16, 512), lambda i: (0, i, 0, 0, 0)),
        compiler_params=pltpu.CompilerParams(dimension_semantics=("arbitrary",)),
        cost_estimate=pl.CostEstimate(
            flops=1_080_000_000, bytes_accessed=6_500_000, transcendentals=0
        ),
    )(n0, n1, g0, g1)


PARTS = (
    (0, 0, 128, "zyx", True),
    (1, 0, 128, "yxz", True),
    (2, 0, 256, "xzy", True),
    (0, 128, 384, "zyx", False),
    (1, 128, 384, "yxz", False),
    (2, 256, 256, "xzy", False),
    (3, 0, 256, "zyx", True),
    (3, 256, 256, "yxz", True),
)
N_SUM = 9 * len(PARTS) + 8 + 1


def sum_kernel(
    g, gain, out, gain_out,
    r0, s0, r1, s1, r2, s2, r3, s3, r4, s4, r5, full, gain_got, gain_sent, send_sems, recv_sems,
):
    here = Here()
    place = {"z": here.z, "y": here.y, "x": here.x}
    greet(
        [here.at(**{a: f(place[a])}) for a in "zyx" for f in (flip1, flip3)]
        + [here.at(core=1 - here.core)]
    )
    net = Net(send_sems, recv_sems)

    def device(axis, value):
        return here.at(**{axis: value})

    plans = []
    for u, lo, width, order, up in PARTS:
        f, f2 = (flip1, flip3) if up else (flip3, flip1)
        a0, a1, a2 = order
        left = [a for a in "zyx" if a != a0]
        plans.append((u, pl.ds(lo, width), f, f2, a0, a1, a2, left.index(a1) == 0))

    def slab(ref, u, axis, value, lanes):
        if axis == "z":
            return ref.at[u, value, :, :, :, lanes]
        if axis == "y":
            return ref.at[u, :, value, :, :, lanes]
        return ref.at[u, :, :, value, :, lanes]

    def slab1(u, value, lanes, leading):
        return s1.at[u, value, :, :, lanes] if leading else s1.at[u, :, value, :, lanes]

    def wide(ref):
        return ref[...].astype(F32)

    waits = {}

    zf, yf, xf = place["z"], place["y"], place["x"]
    gain_routes = (
        [device("z", flip3(zf))]
        + [device("y", flip1(yf)), device("y", flip3(yf)), device("x", flip1(xf)), device("x", flip3(xf))]
        + [here.at(core=1 - here.core)]
    )
    gain_now = []

    def gain_step(step):
        if step == 0:
            gain_now.append(
                [
                    net.start(gain.at[flip1(zf)], gain_got.at[0], device("z", flip1(zf))),
                    net.start(gain.at[flip2(zf)], gain_got.at[1], device("z", flip1(zf))),
                ]
            )
            return
        for copy in gain_now[-1]:
            copy.wait_recv()
        if step == 1:
            gain_sent[0] = gain[flip3(zf)] + gain_got[1]
            gain_sent[1] = gain[zf] + gain_got[0]
            gain_now.append([net.start(gain_sent.at[0], gain_got.at[2], gain_routes[0])])
            return
        if step == 2:
            gain_sent[2] = gain_sent[1] + gain_got[2]
        else:
            gain_sent[step] = gain_sent[step - 1] + gain_got[step]
        if step < 7:
            gain_now.append(
                [net.start(gain_sent.at[step], gain_got.at[step + 1], gain_routes[step - 1])]
            )

    for step in range(6):
        for p, (u, lanes, f, f2, a0, a1, a2, leading) in enumerate(plans):
            m0, m1, m2 = place[a0], place[a1], place[a2]
            if step == 0:
                to = device(a0, f(m0))
                waits[p, 0, 1] = net.start(
                    slab(g, u, a0, flip2(m0), lanes), r0.at[u, 1, :, :, :, lanes], to
                )
                waits[p, 0, 0] = net.start(
                    slab(g, u, a0, f(m0), lanes), r0.at[u, 0, :, :, :, lanes], to
                )
            elif step == 1:
                waits[p, 0, 1].wait_recv()
                s0[u, :, :, :, lanes] = (
                    wide(slab(g, u, a0, f2(m0), lanes)) + r0[u, 1, :, :, :, lanes].astype(F32)
                ).astype(BF)
                waits[p, 1] = net.start(
                    s0.at[u, :, :, :, lanes], r1.at[u, :, :, :, lanes], device(a0, f2(m0))
                )
            elif step == 2:
                waits[p, 0, 0].wait_recv()
                waits[p, 1].wait_recv()
                s1[u, :, :, :, lanes] = (
                    wide(slab(g, u, a0, m0, lanes))
                    + r0[u, 0, :, :, :, lanes].astype(F32)
                    + r1[u, :, :, :, lanes].astype(F32)
                ).astype(BF)
                to = device(a1, f(m1))
                waits[p, 2, 1] = net.start(
                    slab1(u, flip2(m1), lanes, leading), r2.at[u, 1, :, :, lanes], to
                )
                waits[p, 2, 0] = net.start(
                    slab1(u, f(m1), lanes, leading), r2.at[u, 0, :, :, lanes], to
                )
            elif step == 3:
                waits[p, 2, 1].wait_recv()
                s2[u, :, :, lanes] = (
                    wide(slab1(u, f2(m1), lanes, leading)) + r2[u, 1, :, :, lanes].astype(F32)
                ).astype(BF)
                waits[p, 3] = net.start(
                    s2.at[u, :, :, lanes], r3.at[u, :, :, lanes], device(a1, f2(m1))
                )
            elif step == 4:
                waits[p, 2, 0].wait_recv()
                waits[p, 3].wait_recv()
                s3[u, :, :, lanes] = (
                    wide(slab1(u, m1, lanes, leading))
                    + r2[u, 0, :, :, lanes].astype(F32)
                    + r3[u, :, :, lanes].astype(F32)
                ).astype(BF)
                to = device(a2, f(m2))
                waits[p, 4, 1] = net.start(
                    s3.at[u, flip2(m2), :, lanes], r4.at[u, 1, :, lanes], to
                )
                waits[p, 4, 0] = net.start(s3.at[u, f(m2), :, lanes], r4.at[u, 0, :, lanes], to)
            else:
                waits[p, 4, 1].wait_recv()
                s4[u, :, lanes] = (
                    s3[u, f2(m2), :, lanes].astype(F32) + r4[u, 1, :, lanes].astype(F32)
                ).astype(BF)
                waits[p, 5] = net.start(
                    s4.at[u, :, lanes], r5.at[u, :, lanes], device(a2, f2(m2))
                )
        gain_step(step)
    for p, (u, lanes, f, f2, a0, a1, a2, leading) in enumerate(plans):
        waits[p, 4, 0].wait_recv()
        waits[p, 5].wait_recv()
        full[u // 2, u % 2, :, lanes] = (
            s3[u, place[a2], :, lanes].astype(F32)
            + r4[u, 0, :, lanes].astype(F32)
            + r5[u, :, lanes].astype(F32)
        )
    gain_step(6)
    swap = net.start(full.at[1 - here.core], out.at[here.core], here.at(core=1 - here.core))
    out[here.core] = full[here.core]
    gain_step(7)
    gain_out[...] = gain_sent[7]
    swap.wait_recv()
    net.finish()


def sum_everywhere(g, gain):
    vm = pl.BlockSpec(memory_space=VM)
    tail = (16, 512)
    return pl.pallas_call(
        sum_kernel,
        name="sum_everywhere",
        out_shape=(
            jax.ShapeDtypeStruct((2, 2, *tail), F32),
            jax.ShapeDtypeStruct((8, 128), F32),
        ),
        in_specs=[vm] * 2,
        out_specs=(vm,) * 2,
        scratch_shapes=[
            VM((4, 2, 4, 4, *tail), BF),
            VM((4, 4, 4, *tail), BF),
            VM((4, 4, 4, *tail), BF),
            VM((4, 4, 4, *tail), BF),
            VM((4, 2, 4, *tail), BF),
            VM((4, 4, *tail), BF),
            VM((4, 4, *tail), BF),
            VM((4, 4, *tail), BF),
            VM((4, 2, *tail), BF),
            VM((4, *tail), BF),
            VM((4, *tail), BF),
            VM((2, 2, *tail), F32),
            VM((8, 8, 128), F32),
            VM((8, 8, 128), F32),
            pltpu.SemaphoreType.DMA((N_SUM,)),
            pltpu.SemaphoreType.DMA((N_SUM,)),
        ],
        compiler_params=pltpu.CompilerParams(collective_id=3, has_side_effects=True),
    )(g, gain)


def rotation(token_pos, head_size):
    half_dim = head_size // 2
    frequency = ROPE_BASE ** (-2.0 * jnp.arange(half_dim, dtype=F32) / head_size)
    angles = token_pos.astype(F32)[:, None] * frequency[None, :]
    angles = jnp.concatenate([angles, angles], axis=1)
    return (jnp.cos(angles), jnp.sin(angles))


def rotate_half(values):
    half_dim = values.shape[-1] // 2
    return jnp.concatenate([-values[..., half_dim:], values[..., :half_dim]], axis=-1)


def rotate_back(values):
    half_dim = values.shape[-1] // 2
    return jnp.concatenate([values[..., half_dim:], -values[..., :half_dim]], axis=-1)


def body(tokens, queries, d_attended, span_order, norm_gain, key_weight, value_weight):
    seqs, rows, width = tokens.shape
    count = seqs * rows
    ctx = lax.axis_index("ctx")
    core = lax.axis_index("dp") % 2
    z, y, xh = ctx // 8, (ctx // 2) % 4, ctx % 2
    offsets = jnp.arange(rows // 2, dtype=jnp.int32)
    token_pos = (span_order[:, None] * (rows // 2) + offsets[None, :]).reshape(-1)
    own_pos = lax.dynamic_slice_in_dim(token_pos, ctx * rows, rows, 0)
    cosine, sine = rotation(own_pos, HEAD_DIM)
    cosine = jnp.tile(cosine, (seqs, 1))[:, None, :]
    sine = jnp.tile(sine, (seqs, 1))[:, None, :]

    placed = token_pos.reshape(4, 4, 2, rows)
    q_pos = jnp.stack([placed[:, y, xh], placed[z, :, xh]])
    q_pos = jnp.tile(q_pos, (1, 1, 4))[:, :, None, :]
    k_pos = jnp.stack(
        [placed.transpose(1, 2, 0, 3).reshape(-1), placed.transpose(0, 2, 1, 3).reshape(-1)]
    )
    k_pos = jnp.broadcast_to(k_pos[:, :, None], (*k_pos.shape, 128))

    flat = tokens.reshape(count, width)
    wide = flat.astype(F32)
    rms = lax.rsqrt(jnp.mean(wide * wide, axis=-1, keepdims=True) + EPSILON)
    normed = (wide * rms * norm_gain).astype(BF)
    key_pre = jnp.dot(normed, key_weight, preferred_element_type=F32).reshape(count, KV_HEADS, -1)
    keys = (key_pre * cosine + rotate_half(key_pre) * sine).astype(BF)
    values = jnp.dot(normed, value_weight, preferred_element_type=F32).astype(BF)
    kv = jnp.stack([keys, values.reshape(count, KV_HEADS, HEAD_DIM)], axis=2)
    kv = kv.reshape(seqs, rows, 2 * KV_HEADS * HEAD_DIM)

    qr, dr, kvr, other = front(queries, d_attended, kv, normed)
    att, dq, term = attend(qr, dr, kvr.reshape(seqs, -1, 256), q_pos, k_pos)
    attended, grad_queries, dkv = back(att, dq, term.reshape(seqs, 8, 4, rows, 256))

    dkv = dkv.reshape(count, KV_HEADS, 2, HEAD_DIM).astype(F32)
    shaped = dkv[:, :, 0]
    key_grad = (shaped * cosine + rotate_back(shaped * sine)).reshape(count, -1).astype(BF)
    value_grad = dkv[:, :, 1].reshape(count, -1).astype(BF)
    own = jnp.where(core == 0, key_grad, value_grad)
    sent = jnp.where(core == 0, value_grad, key_grad)
    got = lax.ppermute(sent, "dp", [(0, 1), (1, 0), (2, 3), (3, 2)])
    normed_grad = jnp.dot(key_grad, key_weight.T, preferred_element_type=F32) + jnp.dot(
        value_grad, value_weight.T, preferred_element_type=F32
    )
    gain_part = jnp.sum(normed_grad * wide * rms, axis=0)
    inner = jnp.mean(normed_grad * norm_gain * wide, axis=-1, keepdims=True)
    grad_rows = (rms * norm_gain * normed_grad - wide * rms**3 * inner).astype(BF)

    g = outer(normed, other, own, got).reshape(4, 4, 4, 4, 16, 512)
    weights, gain = sum_everywhere(g, gain_part.reshape(4, 8, 128))
    weights = weights.reshape(2, 32, 512)
    gain = lax.dynamic_slice(gain, (ctx % 8, lax.axis_index("dp") * 32), (1, 32))
    return (
        attended,
        grad_queries,
        grad_rows.reshape(seqs, rows, width),
        weights[0],
        weights[1],
        gain.reshape(32),
    )


def solution(mesh):
    placed = (P("dp", "ctx", None), P("dp", "ctx", None), P("dp", "ctx", None), P(), P(), P(), P())
    return jax.shard_map(
        body,
        mesh=mesh,
        in_specs=placed,
        out_specs=(
            P("dp", "ctx", None),
            P("dp", "ctx", None),
            P("dp", "ctx", None),
            P(("ctx", "dp"), None),
            P(("ctx", "dp"), None),
            P(("ctx", "dp")),
        ),
        check_vma=False,
    )
```

```python
import functools
import math

import jax
import jax.numpy as jnp
from jax import lax
from jax.experimental import pallas as pl
from jax.experimental.pallas import tpu as pltpu
from jax.sharding import PartitionSpec as P

KV_HEADS = 4
HEAD_DIM = 128
ROPE_BASE = 500000.0
EPSILON = 1e-05
BF = jnp.bfloat16
F32 = jnp.float32
VM = pltpu.VMEM
MESH = pl.DeviceIdType.MESH


def flip1(a):
    return a + 1 - 2 * (a % 2)


def flip3(a):
    return 3 - a


def flip2(a):
    return (a + 2) % 4


class Here:
    def __init__(self):
        ctx = lax.axis_index("ctx")
        dp = lax.axis_index("dp")
        self.z = ctx // 8
        self.y = (ctx // 2) % 4
        self.xh = ctx % 2
        self.xl = dp // 2
        self.core = dp % 2
        self.x = self.xh * 2 + self.xl

    def at(self, z=None, y=None, x=None, core=None):
        z = self.z if z is None else z
        y = self.y if y is None else y
        core = self.core if core is None else core
        if x is None:
            xh, xl = self.xh, self.xl
        else:
            xh, xl = x // 2, x % 2
        return {"ctx": z * 8 + y * 2 + xh, "dp": xl * 2 + core}


class Net:
    def __init__(self, send_sems, recv_sems):
        self.send_sems = send_sems
        self.recv_sems = recv_sems
        self.made = []

    def start(self, src, dst, device):
        k = len(self.made)
        copy = pltpu.make_async_remote_copy(
            src_ref=src,
            dst_ref=dst,
            send_sem=self.send_sems.at[k],
            recv_sem=self.recv_sems.at[k],
            device_id=device,
            device_id_type=MESH,
        )
        copy.start()
        self.made.append(copy)
        return copy

    def finish(self):
        for copy in self.made:
            copy.wait_send()


def greet(devices):
    barrier = pltpu.get_barrier_semaphore()
    for device in devices:
        pl.semaphore_signal(barrier, inc=1, device_id=device, device_id_type=MESH)
    pl.semaphore_wait(barrier, len(devices))


def cols(index, width):
    return pl.ds(pl.multiple_of(index * width, width), width)


N_FRONT = 2 * 3 * 3 + 2 * (1 + 2 * (2 + 4)) + 1
PIECES = 8


def front_kernel(
    q, do, tokens, gain, key_w, value_w, cos, sin,
    qr, dr, kvr, norm_t, rms_out,
    kw, vw, normed, acc, kv, send_sems, recv_sems, local_sems, weight_sems,
):
    here = Here()
    z, y, xh = here.z, here.y, here.xh
    x2 = flip2(here.x)
    piece = 4096 // PIECES
    loads = []
    for c in range(PIECES):
        for w, (src, dst) in enumerate(((key_w, kw), (value_w, vw))):
            at = pl.ds(c * piece, piece)
            copy = pltpu.make_async_copy(src.at[at], dst.at[at], weight_sems.at[2 * c + w])
            copy.start()
            loads.append(copy)
    greet(
        [here.at(z=f(z)) for f in (flip1, flip3, flip2)]
        + [here.at(y=f(y)) for f in (flip1, flip3, flip2)]
        + [here.at(x=x2), here.at(core=1 - here.core)]
    )
    net = Net(send_sems, recv_sems)

    def along(s, value):
        return here.at(z=value) if s == 0 else here.at(y=value)

    def across(s, value):
        return here.at(y=value) if s == 0 else here.at(z=value)

    head = [z, y]
    ring = [y, z]
    local = []

    def keep(src, dst):
        copy = pltpu.make_async_copy(src, dst, local_sems.at[len(local)])
        copy.start()
        local.append(copy)

    rest = []
    for f in (flip1, flip3, flip2):
        for s in range(2):
            to = f(head[s])
            for src, dst in ((q, qr), (do, dr)):
                rest.append(net.start(src.at[s, :, cols(to, 512)], dst.at[s, head[s]], along(s, to)))
    for s in range(2):
        keep(q.at[s, :, cols(head[s], 512)], qr.at[s, head[s]])
        keep(do.at[s, :, cols(head[s], 512)], dr.at[s, head[s]])

    squares = jnp.zeros((128, 128), F32)
    for c in range(32):
        t = tokens[:, c * 128 : (c + 1) * 128].astype(F32)
        squares = squares + t * t
    rms = lax.rsqrt(jnp.sum(squares, axis=1, keepdims=True) / 4096.0 + EPSILON)
    rms_out[...] = jnp.broadcast_to(rms, (128, 128))
    for c in range(PIECES):
        at = slice(c * piece, (c + 1) * piece)
        normed[:, at] = (tokens[:, at].astype(F32) * rms * gain[:, at]).astype(BF)
    for c in range(PIECES):
        at = slice(c * piece, (c + 1) * piece)
        n = normed[:, at]
        for w, ref in enumerate((kw, vw)):
            loads[2 * c + w].wait()
            term = jnp.dot(n, ref[at, :], preferred_element_type=F32)
            if c == 0:
                acc[w] = term
            else:
                acc[w] += term
    both_cos = jnp.concatenate([cos[...], cos[...]], axis=0)
    both_sin = jnp.concatenate([sin[...], sin[...]], axis=0)
    for h in range(KV_HEADS):
        at = slice(h * 128, (h + 1) * 128)
        u = acc[0, :, at]
        k = (u * both_cos + pltpu.roll(u, 64, 1) * both_sin).astype(BF)
        v = acc[1, :, at].astype(BF)
        for s in range(2):
            kv[s, :, h * 256 : h * 256 + 128] = k[s * 64 : (s + 1) * 64]
            kv[s, :, h * 256 + 128 : (h + 1) * 256] = v[s * 64 : (s + 1) * 64]

    mine = [ring[s] * 2 + xh for s in range(2)]
    kv_copies = [[], []]
    for f in (flip1, flip3, flip2):
        for s in range(2):
            to = f(head[s])
            kv_copies[s].append(
                net.start(kv.at[s, :, cols(to, 256)], kvr.at[s, mine[s], head[s]], along(s, to))
            )
    for s in range(2):
        keep(kv.at[s, :, cols(head[s], 256)], kvr.at[s, mine[s], head[s]])
    for c in range(32):
        at = slice(c * 128, (c + 1) * 128)
        norm_t[0, at, :] = normed[:, at].T
    rest.append(net.start(norm_t.at[0], norm_t.at[1], here.at(core=1 - here.core)))
    for s in range(2):
        local[4 + s].wait()
        for copy in kv_copies[s]:
            copy.wait_recv()

    first = [[], []]
    last = []

    def spread(s, xh_of):
        slot = ring[s] * 2 + xh_of
        for half, f in ((0, flip1), (1, flip3)):
            block = kvr.at[s, slot, 2 * half : 2 * half + 2]
            first[s].append(net.start(block, block, across(s, f(ring[s]))))

    def spread_on(s, xh_of):
        for half, f, g in ((0, flip1, flip3), (1, flip3, flip1)):
            first[s].pop(0).wait_recv()
            for value in (ring[s], f(ring[s])):
                block = kvr.at[s, value * 2 + xh_of, 2 * half : 2 * half + 2]
                last.append(net.start(block, block, across(s, g(ring[s]))))

    swapped = []
    for s in range(2):
        block = kvr.at[s, mine[s]]
        swapped.append(net.start(block, block, here.at(x=x2)))
        spread(s, xh)
    for s in range(2):
        spread_on(s, xh)
    for s in range(2):
        swapped[s].wait_recv()
        spread(s, 1 - xh)
    for s in range(2):
        spread_on(s, 1 - xh)
    for copy in last + rest:
        copy.wait_recv()
    for copy in local[:4]:
        copy.wait()
    net.finish()


def front(q, do, tokens, gain, key_w, value_w, cos, sin):
    vm = pl.BlockSpec(memory_space=VM)
    any_ = pl.BlockSpec(memory_space=pl.ANY)
    return pl.pallas_call(
        front_kernel,
        name="front",
        out_shape=(
            jax.ShapeDtypeStruct((2, 4, 64, 512), BF),
            jax.ShapeDtypeStruct((2, 4, 64, 512), BF),
            jax.ShapeDtypeStruct((2, 8, 4, 64, 256), BF),
            jax.ShapeDtypeStruct((2, 4096, 128), BF),
            jax.ShapeDtypeStruct((128, 128), F32),
        ),
        in_specs=[any_, any_, vm, vm, any_, any_, vm, vm],
        out_specs=(vm,) * 5,
        scratch_shapes=[
            VM((4096, 512), BF),
            VM((4096, 512), BF),
            VM((128, 4096), BF),
            VM((2, 128, 512), F32),
            VM((2, 64, 1024), BF),
            pltpu.SemaphoreType.DMA((N_FRONT,)),
            pltpu.SemaphoreType.DMA((N_FRONT,)),
            pltpu.SemaphoreType.DMA((6,)),
            pltpu.SemaphoreType.DMA((2 * PIECES,)),
        ],
        compiler_params=pltpu.CompilerParams(
            collective_id=1, has_side_effects=True, vmem_limit_bytes=56 * 2**20
        ),
    )(q, do, tokens, gain, key_w, value_w, cos, sin)


CHUNK = 256
KEYS = 2048


def attend_kernel(
    q_ref, do_ref, kv_ref, qpos_ref, kpos_ref, att_ref, dq_ref, term_ref,
    score, prob, key_t, value_t, acc_k, acc_v,
):
    block = pl.program_id(1)
    chunks = KEYS // CHUNK
    scale = HEAD_DIM ** (-0.5)
    to_two = scale * math.log2(math.e)

    @pl.when(block == 0)
    def _():
        key_t[...] = kv_ref[0, :, :128].T
        value_t[...] = kv_ref[0, :, 128:].T
        acc_k[...] = jnp.zeros_like(acc_k)
        acc_v[...] = jnp.zeros_like(acc_v)

    q = jnp.concatenate([q_ref[0, 0, :, h * 128 : (h + 1) * 128] for h in range(4)], axis=0)
    do = jnp.concatenate([do_ref[0, 0, :, h * 128 : (h + 1) * 128] for h in range(4)], axis=0)
    q_t = q.T
    do_t = do.T
    q_pos = qpos_ref[0, 0]

    def rows(c):
        return pl.ds(pl.multiple_of(c * CHUNK, CHUNK), CHUNK)

    def scores_of(c, top):
        s = jnp.dot(kv_ref[0, rows(c), :128], q_t, preferred_element_type=F32)
        k_pos = kpos_ref[0, rows(c), :]
        k_pos = jnp.concatenate([k_pos, k_pos], axis=1)
        s = jnp.where(k_pos <= q_pos, s, -1e30)
        score[rows(c), :] = s
        return jnp.maximum(top, jnp.max(s.reshape(CHUNK // 8, 8, 256), axis=0))

    top = lax.fori_loop(0, chunks, scores_of, jnp.full((8, 256), -1e30, F32), unroll=True)
    top = jnp.max(top, axis=0, keepdims=True)

    def exps_of(c, total):
        e = jnp.exp2((score[rows(c), :] - top) * to_two)
        score[rows(c), :] = e
        return total + jnp.sum(e.reshape(CHUNK // 8, 8, 256), axis=0)

    total = lax.fori_loop(0, chunks, exps_of, jnp.zeros((8, 256), F32), unroll=True)
    inverse = 1.0 / jnp.sum(total, axis=0, keepdims=True)

    def attended_of(c, out):
        p = (score[rows(c), :] * inverse).astype(BF)
        prob[rows(c), :] = p
        return out + jnp.dot(value_t[:, rows(c)], p, preferred_element_type=F32)

    out_t = lax.fori_loop(0, chunks, attended_of, jnp.zeros((128, 256), F32), unroll=True)
    out_t = out_t.astype(BF)
    delta = jnp.sum(out_t.astype(F32) * do_t.astype(F32), axis=0, keepdims=True)

    def grads_of(c, dq_t):
        dp = jnp.dot(kv_ref[0, rows(c), 128:], do_t, preferred_element_type=F32)
        ds = (score[rows(c), :] * inverse * (dp - delta)).astype(BF)
        acc_k[rows(c), :] += jnp.dot(ds, q, preferred_element_type=F32)
        acc_v[rows(c), :] += jnp.dot(prob[rows(c), :], do, preferred_element_type=F32)
        return dq_t + jnp.dot(key_t[:, rows(c)], ds, preferred_element_type=F32)

    dq_t = lax.fori_loop(0, chunks, grads_of, jnp.zeros((128, 256), F32), unroll=True)
    out = out_t.T
    dq = (dq_t * scale).astype(BF).T
    for h in range(4):
        att_ref[0, 0, :, h * 128 : (h + 1) * 128] = out[h * 64 : (h + 1) * 64]
        dq_ref[0, 0, :, h * 128 : (h + 1) * 128] = dq[h * 64 : (h + 1) * 64]

    @pl.when(block == 3)
    def _():
        term_ref[0, :, :128] = (acc_k[...] * scale).astype(BF)
        term_ref[0, :, 128:] = acc_v[...].astype(BF)


def attend(qr, dr, kvr, q_pos, k_pos):
    rows = pl.BlockSpec((1, 1, 64, 512), lambda s, b: (s, b, 0, 0))
    whole = pl.BlockSpec((1, KEYS, 256), lambda s, b: (s, 0, 0))
    return pl.pallas_call(
        attend_kernel,
        name="attend",
        grid=(2, 4),
        out_shape=(
            jax.ShapeDtypeStruct((2, 4, 64, 512), BF),
            jax.ShapeDtypeStruct((2, 4, 64, 512), BF),
            jax.ShapeDtypeStruct((2, KEYS, 256), BF),
        ),
        in_specs=[
            rows,
            rows,
            whole,
            pl.BlockSpec((1, 1, 1, 256), lambda s, b: (s, b, 0, 0)),
            pl.BlockSpec((1, KEYS, 128), lambda s, b: (s, 0, 0)),
        ],
        out_specs=(rows, rows, whole),
        scratch_shapes=[
            VM((KEYS, 256), F32),
            VM((KEYS, 256), BF),
            VM((128, KEYS), BF),
            VM((128, KEYS), BF),
            VM((KEYS, 128), F32),
            VM((KEYS, 128), F32),
        ],
        compiler_params=pltpu.CompilerParams(
            dimension_semantics=("arbitrary", "arbitrary"), vmem_limit_bytes=48 * 2**20
        ),
        cost_estimate=pl.CostEstimate(
            flops=6_500_000_000, bytes_accessed=12_000_000, transcendentals=4_200_000
        ),
    )(qr, dr, kvr, q_pos, k_pos)


PARTS = (
    (0, 0, 128, "zyx", True),
    (1, 0, 128, "yxz", True),
    (2, 0, 256, "xzy", True),
    (0, 128, 384, "zyx", False),
    (1, 128, 384, "yxz", False),
    (2, 256, 256, "xzy", False),
    (3, 0, 256, "zyx", True),
    (3, 256, 256, "yxz", True),
)
N_BACK = 2 * (2 * 3 + 4 + 2 + 1 + 3)
N_SUM = 9 * len(PARTS) + 8 + 1
N_TAIL = N_BACK + N_SUM + 1


def tail_kernel(
    att, dq, term_hbm, tokens_hbm, norm_hbm, rms_in, norm_gain, key_w, value_w, cos, sin,
    att_out, dq_out, rows_out, out, gain_out,
    term, tokens, norm_t, kw, vw, got1, sum1, got2, part, got3, final, dkv_out,
    grads, got_grad, big, wide_grad, gain,
    r0, s0, r1, s1, r2, s2, r3, s3, r4, s4, r5, full, gain_got, gain_sent,
    send_sems, recv_sems, local_sems, load_sems,
):
    here = Here()
    place = {"z": here.z, "y": here.y, "x": here.x}
    z, y, xh = here.z, here.y, here.xh
    x2 = flip2(here.x)
    greet(
        [here.at(**{a: f(place[a])}) for a in "zy" for f in (flip1, flip3, flip2)]
        + [here.at(x=f(here.x)) for f in (flip1, flip3, flip2)]
        + [here.at(core=1 - here.core)]
    )
    net = Net(send_sems, recv_sems)
    loads = []
    for k, (src, dst) in enumerate(
        ((term_hbm, term), (norm_hbm, norm_t), (tokens_hbm, tokens), (key_w, kw), (value_w, vw))
    ):
        loads.append(pltpu.make_async_copy(src, dst, load_sems.at[k]))

    def along(s, value):
        return here.at(z=value) if s == 0 else here.at(y=value)

    def across(s, value):
        return here.at(y=value) if s == 0 else here.at(z=value)

    head = [z, y]
    ring = [y, z]
    flips = ((flip3, flip1), (flip1, flip3))

    def slots(value):
        return pl.ds(value * 2, 2)

    one = {}
    for j in (1, 0):
        for s in range(2):
            for half in range(2):
                f, g = flips[half]
                target = f(ring[s])
                slot = target if j == 0 else g(target)
                one[s, half, j] = net.start(
                    term_hbm.at[s, slots(slot), 2 * half : 2 * half + 2],
                    got1.at[s, half, j],
                    across(s, target),
                )
    for copy in loads:
        copy.start()
    rest = []
    local = []
    for f in (flip1, flip3, flip2):
        for s in range(2):
            to = f(head[s])
            for src, dst in ((att, att_out), (dq, dq_out)):
                rest.append(net.start(src.at[s, to], dst.at[s, :, cols(head[s], 512)], along(s, to)))
    for s in range(2):
        for src, dst in ((att, att_out), (dq, dq_out)):
            copy = pltpu.make_async_copy(
                src.at[s, head[s]], dst.at[s, :, cols(head[s], 512)], local_sems.at[len(local)]
            )
            copy.start()
            local.append(copy)

    loads[0].wait()
    two = {}
    for s in range(2):
        for half in range(2):
            f, g = flips[half]
            one[s, half, 1].wait_recv()
            sum1[s, half] = (
                term[s, slots(g(ring[s])), 2 * half : 2 * half + 2].astype(F32)
                + got1[s, half, 1].astype(F32)
            ).astype(BF)
            two[s, half] = net.start(sum1.at[s, half], got2.at[s, half], across(s, g(ring[s])))
    three = []
    for s in range(2):
        for half in range(2):
            one[s, half, 0].wait_recv()
            two[s, half].wait_recv()
            part[s, :, 2 * half : 2 * half + 2] = (
                term[s, slots(ring[s]), 2 * half : 2 * half + 2].astype(F32)
                + got1[s, half, 0].astype(F32)
                + got2[s, half].astype(F32)
            ).astype(BF)
        three.append(net.start(part.at[s, 1 - xh], got3.at[s], here.at(x=x2)))
    four = []
    for s in range(2):
        three[s].wait_recv()
        final[s] = (part[s, xh].astype(F32) + got3[s].astype(F32)).astype(BF)
        for f in (flip1, flip3, flip2):
            to = f(head[s])
            four.append(net.start(final.at[s, to], dkv_out.at[s, :, cols(head[s], 256)], along(s, to)))
        copy = pltpu.make_async_copy(
            final.at[s, head[s]], dkv_out.at[s, :, cols(head[s], 256)], local_sems.at[len(local)]
        )
        copy.start()
        local.append(copy)
    for copy in four:
        copy.wait_recv()
    for copy in local[4:]:
        copy.wait()

    both_cos = jnp.concatenate([cos[...], cos[...]], axis=0)
    both_sin = jnp.concatenate([sin[...], sin[...]], axis=0)
    for h in range(KV_HEADS):
        at = slice(h * 128, (h + 1) * 128)
        u = jnp.concatenate([dkv_out[s, :, h * 256 : h * 256 + 128] for s in range(2)], axis=0)
        v = jnp.concatenate([dkv_out[s, :, h * 256 + 128 : (h + 1) * 256] for s in range(2)], axis=0)
        u = u.astype(F32)
        grads[0, :, at] = (u * both_cos - pltpu.roll(u, 64, 1) * both_sin).astype(BF)
        grads[1, :, at] = v
    swap_grad = net.start(grads.at[1 - here.core], got_grad, here.at(core=1 - here.core))
    loads[1].wait()
    swap_grad.wait_recv()
    pair = jnp.concatenate([grads[here.core], got_grad[...]], axis=0)

    @pl.loop(0, 16)
    def _(i):
        at = pl.ds(pl.multiple_of(i * 256, 256), 256)
        n = jnp.concatenate([norm_t[0, at, :], norm_t[1, at, :]], axis=1)
        w = jnp.dot(n, pair, preferred_element_type=F32).astype(BF)
        for x in range(4):
            for u in range(4):
                row = x * 64 + u * 16
                big[u, i // 4, i % 4, x] = w[row : row + 16]

    def backward_rows():
        for copy in loads[2:]:
            copy.wait()
        rms = rms_in[:, :1]
        key_grad, value_grad = grads[0], grads[1]
        nt = (((1,), (1,)), ((), ()))
        inner = jnp.zeros((128, 128), F32)
        for c in range(16):
            at = slice(c * 256, (c + 1) * 256)
            ng = lax.dot_general(key_grad, kw[at, :], nt, preferred_element_type=F32)
            ng = ng + lax.dot_general(value_grad, vw[at, :], nt, preferred_element_type=F32)
            t = tokens[:, at].astype(F32)
            wide_grad[:, at] = ng
            across_rows = jnp.sum(ng * t * rms, axis=0, keepdims=True)
            weighted = ng * norm_gain[:, at] * t
            inner = inner + weighted[:, :128] + weighted[:, 128:]
            for k in range(2):
                row = c * 2 + k
                gain[row // 8, row % 8 : row % 8 + 1, :] = across_rows[:, k * 128 : (k + 1) * 128]
        mean = jnp.sum(inner, axis=1, keepdims=True) / 4096.0
        cube = rms**3 * mean
        for c in range(16):
            at = slice(c * 256, (c + 1) * 256)
            rows_out[:, at] = (
                rms * norm_gain[:, at] * wide_grad[:, at] - tokens[:, at].astype(F32) * cube
            ).astype(BF)

    def device(axis, value):
        return here.at(**{axis: value})

    plans = []
    for u, lo, width, order, up in PARTS:
        f, f2 = (flip1, flip3) if up else (flip3, flip1)
        a0, a1, a2 = order
        left = [a for a in "zyx" if a != a0]
        plans.append((u, pl.ds(lo, width), f, f2, a0, a1, a2, left.index(a1) == 0))

    def slab(ref, u, axis, value, lanes):
        if axis == "z":
            return ref.at[u, value, :, :, :, lanes]
        if axis == "y":
            return ref.at[u, :, value, :, :, lanes]
        return ref.at[u, :, :, value, :, lanes]

    def slab1(u, value, lanes, leading):
        return s1.at[u, value, :, :, lanes] if leading else s1.at[u, :, value, :, lanes]

    def wide(ref):
        return ref[...].astype(F32)

    waits = {}

    zf, yf, xf = place["z"], place["y"], place["x"]
    gain_routes = (
        [device("z", flip3(zf))]
        + [device("y", flip1(yf)), device("y", flip3(yf)), device("x", flip1(xf)), device("x", flip3(xf))]
        + [here.at(core=1 - here.core)]
    )
    gain_now = []

    def gain_step(step):
        if step == 0:
            gain_now.append(
                [
                    net.start(gain.at[flip1(zf)], gain_got.at[0], device("z", flip1(zf))),
                    net.start(gain.at[flip2(zf)], gain_got.at[1], device("z", flip1(zf))),
                ]
            )
            return
        for copy in gain_now[-1]:
            copy.wait_recv()
        if step == 1:
            gain_sent[0] = gain[flip3(zf)] + gain_got[1]
            gain_sent[1] = gain[zf] + gain_got[0]
            gain_now.append([net.start(gain_sent.at[0], gain_got.at[2], gain_routes[0])])
            return
        if step == 2:
            gain_sent[2] = gain_sent[1] + gain_got[2]
        else:
            gain_sent[step] = gain_sent[step - 1] + gain_got[step]
        if step < 7:
            gain_now.append(
                [net.start(gain_sent.at[step], gain_got.at[step + 1], gain_routes[step - 1])]
            )

    for step in range(6):
        for p, (u, lanes, f, f2, a0, a1, a2, leading) in enumerate(plans):
            m0, m1, m2 = place[a0], place[a1], place[a2]
            if step == 0:
                to = device(a0, f(m0))
                waits[p, 0, 1] = net.start(
                    slab(big, u, a0, flip2(m0), lanes), r0.at[u, 1, :, :, :, lanes], to
                )
                waits[p, 0, 0] = net.start(
                    slab(big, u, a0, f(m0), lanes), r0.at[u, 0, :, :, :, lanes], to
                )
            elif step == 1:
                waits[p, 0, 1].wait_recv()
                s0[u, :, :, :, lanes] = (
                    wide(slab(big, u, a0, f2(m0), lanes)) + r0[u, 1, :, :, :, lanes].astype(F32)
                ).astype(BF)
                waits[p, 1] = net.start(
                    s0.at[u, :, :, :, lanes], r1.at[u, :, :, :, lanes], device(a0, f2(m0))
                )
            elif step == 2:
                waits[p, 0, 0].wait_recv()
                waits[p, 1].wait_recv()
                s1[u, :, :, :, lanes] = (
                    wide(slab(big, u, a0, m0, lanes))
                    + r0[u, 0, :, :, :, lanes].astype(F32)
                    + r1[u, :, :, :, lanes].astype(F32)
                ).astype(BF)
                to = device(a1, f(m1))
                waits[p, 2, 1] = net.start(
                    slab1(u, flip2(m1), lanes, leading), r2.at[u, 1, :, :, lanes], to
                )
                waits[p, 2, 0] = net.start(
                    slab1(u, f(m1), lanes, leading), r2.at[u, 0, :, :, lanes], to
                )
            elif step == 3:
                waits[p, 2, 1].wait_recv()
                s2[u, :, :, lanes] = (
                    wide(slab1(u, f2(m1), lanes, leading)) + r2[u, 1, :, :, lanes].astype(F32)
                ).astype(BF)
                waits[p, 3] = net.start(
                    s2.at[u, :, :, lanes], r3.at[u, :, :, lanes], device(a1, f2(m1))
                )
            elif step == 4:
                waits[p, 2, 0].wait_recv()
                waits[p, 3].wait_recv()
                s3[u, :, :, lanes] = (
                    wide(slab1(u, m1, lanes, leading))
                    + r2[u, 0, :, :, lanes].astype(F32)
                    + r3[u, :, :, lanes].astype(F32)
                ).astype(BF)
                to = device(a2, f(m2))
                waits[p, 4, 1] = net.start(
                    s3.at[u, flip2(m2), :, lanes], r4.at[u, 1, :, lanes], to
                )
                waits[p, 4, 0] = net.start(s3.at[u, f(m2), :, lanes], r4.at[u, 0, :, lanes], to)
            else:
                waits[p, 4, 1].wait_recv()
                s4[u, :, lanes] = (
                    s3[u, f2(m2), :, lanes].astype(F32) + r4[u, 1, :, lanes].astype(F32)
                ).astype(BF)
                waits[p, 5] = net.start(
                    s4.at[u, :, lanes], r5.at[u, :, lanes], device(a2, f2(m2))
                )
        if step == 0:
            backward_rows()
        gain_step(step)
    for p, (u, lanes, f, f2, a0, a1, a2, leading) in enumerate(plans):
        waits[p, 4, 0].wait_recv()
        waits[p, 5].wait_recv()
        full[u // 2, u % 2, :, lanes] = (
            s3[u, place[a2], :, lanes].astype(F32)
            + r4[u, 0, :, lanes].astype(F32)
            + r5[u, :, lanes].astype(F32)
        )
    gain_step(6)
    swap = net.start(full.at[1 - here.core], out.at[here.core], here.at(core=1 - here.core))
    out[here.core] = full[here.core]
    gain_step(7)
    gain_out[...] = gain_sent[7]
    swap.wait_recv()
    for copy in rest:
        copy.wait_recv()
    for copy in local[:4]:
        copy.wait()
    net.finish()


def tail(att, dq, term, tokens, norm_t, rms, norm_gain, key_w, value_w, cos, sin):
    vm = pl.BlockSpec(memory_space=VM)
    any_ = pl.BlockSpec(memory_space=pl.ANY)
    end = (16, 512)
    return pl.pallas_call(
        tail_kernel,
        name="tail",
        out_shape=(
            jax.ShapeDtypeStruct((2, 64, 2048), BF),
            jax.ShapeDtypeStruct((2, 64, 2048), BF),
            jax.ShapeDtypeStruct((128, 4096), BF),
            jax.ShapeDtypeStruct((2, 2, *end), F32),
            jax.ShapeDtypeStruct((8, 128), F32),
        ),
        in_specs=[any_] * 5 + [vm] * 2 + [any_] * 2 + [vm] * 2,
        out_specs=(vm,) * 5,
        scratch_shapes=[
            VM((2, 8, 4, 64, 256), BF),
            VM((128, 4096), BF),
            VM((2, 4096, 128), BF),
            VM((4096, 512), BF),
            VM((4096, 512), BF),
            VM((2, 2, 2, 2, 2, 64, 256), BF),
            VM((2, 2, 2, 2, 64, 256), BF),
            VM((2, 2, 2, 2, 64, 256), BF),
            VM((2, 2, 4, 64, 256), BF),
            VM((2, 4, 64, 256), BF),
            VM((2, 4, 64, 256), BF),
            VM((2, 64, 1024), BF),
            VM((2, 128, 512), BF),
            VM((128, 512), BF),
            VM((4, 4, 4, 4, *end), BF),
            VM((128, 4096), F32),
            VM((4, 8, 128), F32),
            VM((4, 2, 4, 4, *end), BF),
            VM((4, 4, 4, *end), BF),
            VM((4, 4, 4, *end), BF),
            VM((4, 4, 4, *end), BF),
            VM((4, 2, 4, *end), BF),
            VM((4, 4, *end), BF),
            VM((4, 4, *end), BF),
            VM((4, 4, *end), BF),
            VM((4, 2, *end), BF),
            VM((4, *end), BF),
            VM((4, *end), BF),
            VM((2, 2, *end), F32),
            VM((8, 8, 128), F32),
            VM((8, 8, 128), F32),
            pltpu.SemaphoreType.DMA((N_TAIL,)),
            pltpu.SemaphoreType.DMA((N_TAIL,)),
            pltpu.SemaphoreType.DMA((6,)),
            pltpu.SemaphoreType.DMA((5,)),
        ],
        compiler_params=pltpu.CompilerParams(
            collective_id=2, has_side_effects=True, vmem_limit_bytes=60 * 2**20
        ),
    )(att, dq, term, tokens, norm_t, rms, norm_gain, key_w, value_w, cos, sin)


def rotation(token_pos, head_size):
    half_dim = head_size // 2
    frequency = ROPE_BASE ** (-2.0 * jnp.arange(half_dim, dtype=F32) / head_size)
    angles = token_pos.astype(F32)[:, None] * frequency[None, :]
    angles = jnp.concatenate([angles, angles], axis=1)
    return (jnp.cos(angles), jnp.sin(angles))


def body(tokens, queries, d_attended, span_order, norm_gain, key_weight, value_weight):
    seqs, rows, width = tokens.shape
    count = seqs * rows
    ctx = lax.axis_index("ctx")
    z, y, xh = ctx // 8, (ctx // 2) % 4, ctx % 2
    offsets = jnp.arange(rows // 2, dtype=jnp.int32)
    token_pos = (span_order[:, None] * (rows // 2) + offsets[None, :]).reshape(-1)
    own_pos = lax.dynamic_slice_in_dim(token_pos, ctx * rows, rows, 0)
    cosine, sine = rotation(own_pos, HEAD_DIM)
    sine = jnp.concatenate([-sine[:, : HEAD_DIM // 2], sine[:, HEAD_DIM // 2 :]], axis=1)

    placed = token_pos.reshape(4, 4, 2, rows)
    q_pos = jnp.stack([placed[:, y, xh], placed[z, :, xh]])
    q_pos = jnp.tile(q_pos, (1, 1, 4))[:, :, None, :]
    k_pos = jnp.stack(
        [placed.transpose(1, 2, 0, 3).reshape(-1), placed.transpose(0, 2, 1, 3).reshape(-1)]
    )
    k_pos = jnp.broadcast_to(k_pos[:, :, None], (*k_pos.shape, 128))

    flat = tokens.reshape(count, width)
    gain_row = norm_gain.reshape(1, width)
    qr, dr, kvr, norm_t, rms = front(
        queries, d_attended, flat, gain_row, key_weight, value_weight, cosine, sine
    )
    att, dq, term = attend(qr, dr, kvr.reshape(seqs, -1, 256), q_pos, k_pos)
    attended, grad_queries, grad_rows, weights, gain = tail(
        att, dq, term.reshape(seqs, 8, 4, rows, 256), flat, norm_t, rms, gain_row,
        key_weight, value_weight, cosine, sine,
    )
    weights = weights.reshape(2, 32, 512)
    gain = lax.dynamic_slice(gain, (ctx % 8, lax.axis_index("dp") * 32), (1, 32))
    return (
        attended,
        grad_queries,
        grad_rows.reshape(seqs, rows, width),
        weights[0],
        weights[1],
        gain.reshape(32),
    )


def solution(mesh):
    placed = (P("dp", "ctx", None), P("dp", "ctx", None), P("dp", "ctx", None), P(), P(), P(), P())
    return jax.shard_map(
        body,
        mesh=mesh,
        in_specs=placed,
        out_specs=(
            P("dp", "ctx", None),
            P("dp", "ctx", None),
            P("dp", "ctx", None),
            P(("ctx", "dp"), None),
            P(("ctx", "dp"), None),
            P(("ctx", "dp")),
        ),
        check_vma=False,
    )
```

```python
import functools
import math

import jax
import jax.numpy as jnp
from jax import lax
from jax.experimental import pallas as pl
from jax.experimental.pallas import tpu as pltpu
from jax.sharding import PartitionSpec as P

KV_HEADS = 4
HEAD_DIM = 128
ROPE_BASE = 500000.0
EPSILON = 1e-05
BF = jnp.bfloat16
F32 = jnp.float32
VM = pltpu.VMEM
MESH = pl.DeviceIdType.MESH


def flip1(a):
    return a + 1 - 2 * (a % 2)


def flip3(a):
    return 3 - a


def flip2(a):
    return (a + 2) % 4


class Here:
    def __init__(self):
        ctx = lax.axis_index("ctx")
        dp = lax.axis_index("dp")
        self.z = ctx // 8
        self.y = (ctx // 2) % 4
        self.xh = ctx % 2
        self.xl = dp // 2
        self.core = dp % 2
        self.x = self.xh * 2 + self.xl

    def at(self, z=None, y=None, x=None, core=None):
        z = self.z if z is None else z
        y = self.y if y is None else y
        core = self.core if core is None else core
        if x is None:
            xh, xl = self.xh, self.xl
        else:
            xh, xl = x // 2, x % 2
        return {"ctx": z * 8 + y * 2 + xh, "dp": xl * 2 + core}


class Net:
    def __init__(self, send_sems, recv_sems):
        self.send_sems = send_sems
        self.recv_sems = recv_sems
        self.made = []

    def start(self, src, dst, device):
        k = len(self.made)
        copy = pltpu.make_async_remote_copy(
            src_ref=src,
            dst_ref=dst,
            send_sem=self.send_sems.at[k],
            recv_sem=self.recv_sems.at[k],
            device_id=device,
            device_id_type=MESH,
        )
        copy.start()
        self.made.append(copy)
        return copy

    def finish(self):
        for copy in self.made:
            copy.wait_send()


def greet(devices):
    barrier = pltpu.get_barrier_semaphore()
    for device in devices:
        pl.semaphore_signal(barrier, inc=1, device_id=device, device_id_type=MESH)
    pl.semaphore_wait(barrier, len(devices))


def cols(index, width):
    return pl.ds(pl.multiple_of(index * width, width), width)


N_FRONT = 2 * 3 * 3 + 2 * (2 + 2 * (2 + 4)) + 1
PIECES = 8


def front_kernel(
    q, do, tokens, gain, key_w, value_w, cos, sin,
    qr, dr, kvr, norm_t, rms_out,
    kw, vw, normed, acc, kv, send_sems, recv_sems, local_sems, weight_sems,
):
    here = Here()
    z, y, xh = here.z, here.y, here.xh
    x2 = flip2(here.x)
    piece = 4096 // PIECES
    loads = []
    for c in range(PIECES):
        for w, (src, dst) in enumerate(((key_w, kw), (value_w, vw))):
            at = pl.ds(c * piece, piece)
            copy = pltpu.make_async_copy(src.at[at], dst.at[at], weight_sems.at[2 * c + w])
            copy.start()
            loads.append(copy)
    greet(
        [here.at(z=f(z)) for f in (flip1, flip3, flip2)]
        + [here.at(y=f(y)) for f in (flip1, flip3, flip2)]
        + [here.at(x=x2), here.at(core=1 - here.core)]
    )
    net = Net(send_sems, recv_sems)

    def along(s, value):
        return here.at(z=value) if s == 0 else here.at(y=value)

    def across(s, value):
        return here.at(y=value) if s == 0 else here.at(z=value)

    head = [z, y]
    ring = [y, z]
    local = []

    def keep(src, dst):
        copy = pltpu.make_async_copy(src, dst, local_sems.at[len(local)])
        copy.start()
        local.append(copy)

    rest = []
    for f in (flip1, flip3, flip2):
        for s in range(2):
            to = f(head[s])
            for src, dst in ((q, qr), (do, dr)):
                rest.append(net.start(src.at[s, :, cols(to, 512)], dst.at[s, head[s]], along(s, to)))
    for s in range(2):
        keep(q.at[s, :, cols(head[s], 512)], qr.at[s, head[s]])
        keep(do.at[s, :, cols(head[s], 512)], dr.at[s, head[s]])

    squares = jnp.zeros((128, 128), F32)
    for c in range(32):
        t = tokens[:, c * 128 : (c + 1) * 128].astype(F32)
        squares = squares + t * t
    rms = lax.rsqrt(jnp.sum(squares, axis=1, keepdims=True) / 4096.0 + EPSILON)
    rms_out[...] = jnp.broadcast_to(rms, (128, 128))
    for c in range(PIECES):
        at = slice(c * piece, (c + 1) * piece)
        normed[:, at] = (tokens[:, at].astype(F32) * rms * gain[:, at]).astype(BF)
    for c in range(PIECES):
        at = slice(c * piece, (c + 1) * piece)
        n = normed[:, at]
        for w, ref in enumerate((kw, vw)):
            loads[2 * c + w].wait()
            term = jnp.dot(n, ref[at, :], preferred_element_type=F32)
            if c == 0:
                acc[w] = term
            else:
                acc[w] += term
    both_cos = jnp.concatenate([cos[...], cos[...]], axis=0)
    both_sin = jnp.concatenate([sin[...], sin[...]], axis=0)
    for h in range(KV_HEADS):
        at = slice(h * 128, (h + 1) * 128)
        u = acc[0, :, at]
        k = (u * both_cos + pltpu.roll(u, 64, 1) * both_sin).astype(BF)
        v = acc[1, :, at].astype(BF)
        for s in range(2):
            kv[s, :, h * 256 : h * 256 + 128] = k[s * 64 : (s + 1) * 64]
            kv[s, :, h * 256 + 128 : (h + 1) * 256] = v[s * 64 : (s + 1) * 64]

    mine = [ring[s] * 2 + xh for s in range(2)]
    kv_copies = [[], []]
    for f in (flip1, flip3, flip2):
        for s in range(2):
            to = f(head[s])
            kv_copies[s].append(
                net.start(kv.at[s, :, cols(to, 256)], kvr.at[s, mine[s], head[s]], along(s, to))
            )
    for s in range(2):
        keep(kv.at[s, :, cols(head[s], 256)], kvr.at[s, mine[s], head[s]])
    for c in range(32):
        at = slice(c * 128, (c + 1) * 128)
        norm_t[0, at, :] = normed[:, at].T
    rest.append(net.start(norm_t.at[0], norm_t.at[1], here.at(core=1 - here.core)))
    for s in range(2):
        local[4 + s].wait()
        for copy in kv_copies[s]:
            copy.wait_recv()

    first = [[], []]
    last = []

    def spread(s, xh_of, half):
        f = (flip1, flip3)[half]
        block = kvr.at[s, ring[s] * 2 + xh_of, 2 * half : 2 * half + 2]
        first[s].append(net.start(block, block, across(s, f(ring[s]))))

    def spread_on(s, xh_of):
        for half, f, g in ((0, flip1, flip3), (1, flip3, flip1)):
            first[s].pop(0).wait_recv()
            for value in (ring[s], f(ring[s])):
                block = kvr.at[s, value * 2 + xh_of, 2 * half : 2 * half + 2]
                last.append(net.start(block, block, across(s, g(ring[s]))))

    swapped = {}
    for half in range(2):
        for s in range(2):
            block = kvr.at[s, mine[s], 2 * half : 2 * half + 2]
            swapped[s, half] = net.start(block, block, here.at(x=x2))
    for half in range(2):
        for s in range(2):
            spread(s, xh, half)
    for s in range(2):
        spread_on(s, xh)
    for half in range(2):
        for s in range(2):
            swapped[s, half].wait_recv()
            spread(s, 1 - xh, half)
    for s in range(2):
        spread_on(s, 1 - xh)
    for copy in last + rest:
        copy.wait_recv()
    for copy in local[:4]:
        copy.wait()
    net.finish()


def front(q, do, tokens, gain, key_w, value_w, cos, sin):
    vm = pl.BlockSpec(memory_space=VM)
    any_ = pl.BlockSpec(memory_space=pl.ANY)
    return pl.pallas_call(
        front_kernel,
        name="front",
        out_shape=(
            jax.ShapeDtypeStruct((2, 4, 64, 512), BF),
            jax.ShapeDtypeStruct((2, 4, 64, 512), BF),
            jax.ShapeDtypeStruct((2, 8, 4, 64, 256), BF),
            jax.ShapeDtypeStruct((2, 4096, 128), BF),
            jax.ShapeDtypeStruct((128, 128), F32),
        ),
        in_specs=[any_, any_, vm, vm, any_, any_, vm, vm],
        out_specs=(vm,) * 5,
        scratch_shapes=[
            VM((4096, 512), BF),
            VM((4096, 512), BF),
            VM((128, 4096), BF),
            VM((2, 128, 512), F32),
            VM((2, 64, 1024), BF),
            pltpu.SemaphoreType.DMA((N_FRONT,)),
            pltpu.SemaphoreType.DMA((N_FRONT,)),
            pltpu.SemaphoreType.DMA((6,)),
            pltpu.SemaphoreType.DMA((2 * PIECES,)),
        ],
        compiler_params=pltpu.CompilerParams(
            collective_id=1, has_side_effects=True, vmem_limit_bytes=60 * 1024 * 1024
        ),
    )(q, do, tokens, gain, key_w, value_w, cos, sin)


CHUNK = 256
KEYS = 2048


def attend_kernel(
    spans, q_ref, do_ref, kv_ref, att_ref, dq_ref, term_ref,
    score, prob, kv_s, key_t, value_t, acc_k, acc_v, picked,
):
    seq = pl.program_id(0)
    pair = pl.program_id(1)
    chunks = KEYS // CHUNK
    scale = HEAD_DIM ** (-0.5)
    to_two = scale * math.log2(math.e)

    def key_span(i):
        a, xh, b, half = i // 16, (i // 8) % 2, (i // 2) % 4, i % 2
        along_z = ((b * 4 + a) * 2 + xh) * 2 + half
        along_y = ((a * 4 + b) * 2 + xh) * 2 + half
        return spans[jnp.where(seq == 0, along_z, along_y)]

    def span_rows(span):
        return pl.ds(pl.multiple_of(span * 32, 32), 32)

    @pl.when(pair == 0)
    def _():
        for i in range(64):
            kv_s[span_rows(key_span(i)), :] = kv_ref[0, i * 32 : (i + 1) * 32, :]

        key_t[...] = kv_s[:, :128].T
        value_t[...] = kv_s[:, 128:].T
        acc_k[...] = jnp.zeros_like(acc_k)
        acc_v[...] = jnp.zeros_like(acc_v)
        here = Here()
        start = jnp.where(seq == 0, here.y * 4, here.z * 16) + here.xh * 2
        stride = jnp.where(seq == 0, 16, 4)
        own = [spans[start + stride * (i // 2) + i % 2] for i in range(8)]
        for i in range(8):
            rank = jnp.int32(0)
            for j in range(8):
                if j != i:
                    rank = rank + (own[j] < own[i]).astype(jnp.int32)
            picked[rank] = i
            picked[8 + rank] = own[i]

    first, second = picked[2 * pair], picked[2 * pair + 1]
    low, high = picked[8 + 2 * pair], picked[8 + 2 * pair + 1]

    def stack(ref):
        a, b = ref[0, first], ref[0, second]
        return jnp.concatenate(
            [r[:, h * 128 : (h + 1) * 128] for h in range(4) for r in (a, b)], axis=0
        )

    q = stack(q_ref)
    do = stack(do_ref)
    q_t = q.T
    do_t = do.T
    lane = lax.broadcasted_iota(jnp.int32, (1, 256), 1)
    q_pos = lane % 32 + 32 * jnp.where(lane % 64 < 32, low, high)

    def run(count):
        key_at = lax.broadcasted_iota(jnp.int32, (CHUNK, 256), 0)
        top = jnp.full((8, 256), -1e30, F32)
        for c in range(count):
            rows = slice(c * CHUNK, (c + 1) * CHUNK)
            s = jnp.dot(kv_s[rows, :128], q_t, preferred_element_type=F32)
            s = jnp.where(key_at <= q_pos - c * CHUNK, s, -1e30)
            score[rows, :] = s
            top = jnp.maximum(top, jnp.max(s.reshape(CHUNK // 8, 8, 256), axis=0))
        top = jnp.max(top, axis=0, keepdims=True)
        total = jnp.zeros((8, 256), F32)
        for c in range(count):
            rows = slice(c * CHUNK, (c + 1) * CHUNK)
            e = jnp.exp2((score[rows, :] - top) * to_two)
            score[rows, :] = e
            total = total + jnp.sum(e.reshape(CHUNK // 8, 8, 256), axis=0)
        inverse = 1.0 / jnp.sum(total, axis=0, keepdims=True)
        out_t = jnp.zeros((128, 256), F32)
        for c in range(count):
            rows = slice(c * CHUNK, (c + 1) * CHUNK)
            p = (score[rows, :] * inverse).astype(BF)
            prob[rows, :] = p
            out_t = out_t + jnp.dot(value_t[:, rows], p, preferred_element_type=F32)
        out_t = out_t.astype(BF)
        delta = jnp.sum(out_t.astype(F32) * do_t.astype(F32), axis=0, keepdims=True)
        dq_t = jnp.zeros((128, 256), F32)
        for c in range(count):
            rows = slice(c * CHUNK, (c + 1) * CHUNK)
            dp = jnp.dot(kv_s[rows, 128:], do_t, preferred_element_type=F32)
            ds = (score[rows, :] * inverse * (dp - delta)).astype(BF)
            acc_k[rows, :] += jnp.dot(ds, q, preferred_element_type=F32)
            acc_v[rows, :] += jnp.dot(prob[rows, :], do, preferred_element_type=F32)
            dq_t = dq_t + jnp.dot(key_t[:, rows], ds, preferred_element_type=F32)
        out = out_t.T
        dq = (dq_t * scale).astype(BF).T
        for h in range(4):
            for k, span in enumerate((first, second)):
                at = slice(h * 64 + k * 32, h * 64 + k * 32 + 32)
                att_ref[0, span, :, h * 128 : (h + 1) * 128] = out[at]
                dq_ref[0, span, :, h * 128 : (h + 1) * 128] = dq[at]

    need = lax.shift_right_logical(high, 3) + 1
    for count in range(1, chunks + 1):
        pl.when(need == count)(functools.partial(run, count))

    @pl.when(pair == 3)
    def _():
        for i in range(64):
            rows = span_rows(key_span(i))
            term_ref[0, i * 32 : (i + 1) * 32, :128] = (acc_k[rows, :] * scale).astype(BF)
            term_ref[0, i * 32 : (i + 1) * 32, 128:] = acc_v[rows, :].astype(BF)


def attend(spans, qr, dr, kvr):
    rows = pl.BlockSpec((1, 8, 32, 512), lambda s, b: (s, 0, 0, 0))
    whole = pl.BlockSpec((1, KEYS, 256), lambda s, b: (s, 0, 0))
    return pl.pallas_call(
        attend_kernel,
        name="attend",
        grid=(2, 4),
        out_shape=(
            jax.ShapeDtypeStruct((2, 8, 32, 512), BF),
            jax.ShapeDtypeStruct((2, 8, 32, 512), BF),
            jax.ShapeDtypeStruct((2, KEYS, 256), BF),
        ),
        in_specs=[pl.BlockSpec(memory_space=pltpu.SMEM), rows, rows, whole],
        out_specs=(rows, rows, whole),
        scratch_shapes=[
            VM((KEYS, 256), F32),
            VM((KEYS, 256), BF),
            VM((KEYS, 256), BF),
            VM((128, KEYS), BF),
            VM((128, KEYS), BF),
            VM((KEYS, 128), F32),
            VM((KEYS, 128), F32),
            pltpu.SMEM((16,), jnp.int32),
        ],
        compiler_params=pltpu.CompilerParams(
            dimension_semantics=("arbitrary", "arbitrary"), vmem_limit_bytes=60 * 1024 * 1024
        ),
        cost_estimate=pl.CostEstimate(
            flops=6_500_000_000, bytes_accessed=8_000_000, transcendentals=4_200_000
        ),
    )(spans, qr, dr, kvr)


def finish_kernel(
    att, dq, rows, weights, gain, att_to, dq_to, rows_to, keys_to, values_to, gain_to,
    att_v, dq_v, rows_v, weights_v, gain_v, sems,
):
    here = Here()
    loads = []
    for k, (src, dst) in enumerate(
        ((gain, gain_v), (att, att_v), (dq, dq_v), (rows, rows_v), (weights, weights_v))
    ):
        copy = pltpu.make_async_copy(src, dst, sems.at[k])
        copy.start()
        loads.append(copy)
    loads[0].wait()
    row = gain_v[pl.ds(here.y * 2 + here.xh, 1), :]
    dp = here.xl * 2 + here.core
    gain_to[...] = pltpu.roll(row, (128 - dp * 32) % 128, 1)[:, :32]
    stores = []
    for k, (load, src, dst) in enumerate(
        (
            (loads[1], att_v, att_to),
            (loads[2], dq_v, dq_to),
            (loads[3], rows_v, rows_to),
            (loads[4], weights_v.at[0], keys_to),
            (None, weights_v.at[1], values_to),
        )
    ):
        if load is not None:
            load.wait()
        copy = pltpu.make_async_copy(src, dst, sems.at[5 + k])
        copy.start()
        stores.append(copy)
    for copy in stores:
        copy.wait()


def finish(att, dq, rows, weights, gain):
    any_ = pl.BlockSpec(memory_space=pl.ANY)
    return pl.pallas_call(
        finish_kernel,
        name="finish",
        out_shape=(
            jax.ShapeDtypeStruct((2, 64, 2048), BF),
            jax.ShapeDtypeStruct((2, 64, 2048), BF),
            jax.ShapeDtypeStruct((128, 4096), BF),
            jax.ShapeDtypeStruct((32, 512), F32),
            jax.ShapeDtypeStruct((32, 512), F32),
            jax.ShapeDtypeStruct((1, 32), F32),
        ),
        in_specs=[any_] * 5,
        out_specs=(any_,) * 5 + (pl.BlockSpec(memory_space=VM),),
        scratch_shapes=[
            VM((2, 64, 2048), BF),
            VM((2, 64, 2048), BF),
            VM((128, 4096), BF),
            VM((2, 32, 512), F32),
            VM((8, 128), F32),
            pltpu.SemaphoreType.DMA((10,)),
        ],
        compiler_params=pltpu.CompilerParams(vmem_limit_bytes=60 * 1024 * 1024),
    )(att, dq, rows, weights, gain)


PARTS = (
    (0, 0, 128, "zyx", True),
    (1, 0, 128, "yxz", True),
    (2, 0, 256, "xzy", True),
    (0, 128, 384, "zyx", False),
    (1, 128, 384, "yxz", False),
    (2, 256, 256, "xzy", False),
    (3, 0, 256, "zyx", True),
    (3, 256, 256, "yxz", True),
)
N_BACK = 2 * (2 * 3 + 4 + 2 + 2 + 3)
N_SUM = 9 * len(PARTS) + 8 + 1
N_TAIL = N_BACK + N_SUM + 1


def tail_kernel(
    att, dq, term_hbm, tokens_hbm, norm_hbm, rms_in, norm_gain, key_w, value_w, cos, sin,
    att_out, dq_out, rows_out, out, gain_out,
    term, tokens, norm_t, kw, vw, got1, sum1, got2, part, got3, final, whole, grad_rows,
    grads, got_grad, big, wide_grad, gain,
    r0, s0, r1, s1, r2, s2, r3, s3, r4, s4, r5, full, gain_got, gain_sent,
    send_sems, recv_sems, local_sems, load_sems,
):
    here = Here()
    place = {"z": here.z, "y": here.y, "x": here.x}
    z, y, xh = here.z, here.y, here.xh
    x2 = flip2(here.x)
    greet(
        [here.at(**{a: f(place[a])}) for a in "zy" for f in (flip1, flip3, flip2)]
        + [here.at(x=f(here.x)) for f in (flip1, flip3, flip2)]
        + [here.at(core=1 - here.core)]
    )
    net = Net(send_sems, recv_sems)
    loads = []
    for k, (src, dst) in enumerate(
        ((term_hbm, term), (norm_hbm, norm_t), (tokens_hbm, tokens), (key_w, kw), (value_w, vw))
    ):
        loads.append(pltpu.make_async_copy(src, dst, load_sems.at[k]))

    def along(s, value):
        return here.at(z=value) if s == 0 else here.at(y=value)

    def across(s, value):
        return here.at(y=value) if s == 0 else here.at(z=value)

    head = [z, y]
    ring = [y, z]
    flips = ((flip3, flip1), (flip1, flip3))

    def slots(value):
        return pl.ds(value * 2, 2)

    one = {}
    for j in (1, 0):
        for s in range(2):
            for half in range(2):
                f, g = flips[half]
                target = f(ring[s])
                slot = target if j == 0 else g(target)
                one[s, half, j] = net.start(
                    term_hbm.at[s, slots(slot), 2 * half : 2 * half + 2],
                    got1.at[s, half, j],
                    across(s, target),
                )
    for copy in loads:
        copy.start()
    loads[0].wait()
    two = {}
    for s in range(2):
        for half in range(2):
            f, g = flips[half]
            one[s, half, 1].wait_recv()
            sum1[s, half] = (
                term[s, slots(g(ring[s])), 2 * half : 2 * half + 2].astype(F32)
                + got1[s, half, 1].astype(F32)
            ).astype(BF)
            two[s, half] = net.start(sum1.at[s, half], got2.at[s, half], across(s, g(ring[s])))
    three = {}
    for half in range(2):
        for s in range(2):
            at = slice(2 * half, 2 * half + 2)
            one[s, half, 0].wait_recv()
            two[s, half].wait_recv()
            part[s, :, at] = (
                term[s, slots(ring[s]), at].astype(F32)
                + got1[s, half, 0].astype(F32)
                + got2[s, half].astype(F32)
            ).astype(BF)
            three[s, half] = net.start(part.at[s, 1 - xh, at], got3.at[s, at], here.at(x=x2))
    rest = []
    local = []
    for f in (flip1, flip3, flip2):
        for s in range(2):
            to = f(head[s])
            for src, dst in ((att, att_out), (dq, dq_out)):
                rest.append(net.start(src.at[s, to], dst.at[s, :, cols(head[s], 512)], along(s, to)))
    for s in range(2):
        for src, dst in ((att, att_out), (dq, dq_out)):
            copy = pltpu.make_async_copy(
                src.at[s, head[s]], dst.at[s, :, cols(head[s], 512)], local_sems.at[len(local)]
            )
            copy.start()
            local.append(copy)

    for half in range(2):
        for s in range(2):
            at = slice(2 * half, 2 * half + 2)
            three[s, half].wait_recv()
            final[s, at] = (part[s, xh, at].astype(F32) + got3[s, at].astype(F32)).astype(BF)
    owners = []
    for s in range(2):
        for f in (flip2, flip1, flip3):
            to = f(head[s])
            owners.append(net.start(final.at[s, to], whole.at[s, head[s]], along(s, to)))
        whole[s, head[s]] = final[s, head[s]]
    for copy in owners:
        copy.wait_recv()

    both_cos = jnp.concatenate([cos[...], cos[...]], axis=0)
    both_sin = jnp.concatenate([sin[...], sin[...]], axis=0)
    for h in range(KV_HEADS):
        at = slice(h * 128, (h + 1) * 128)
        both = jnp.concatenate([whole[s, h] for s in range(2)], axis=0)
        u, v = both[:, :128].astype(F32), both[:, 128:]
        grads[0, :, at] = (u * both_cos - pltpu.roll(u, 64, 1) * both_sin).astype(BF)
        grads[1, :, at] = v
    swap_grad = net.start(grads.at[1 - here.core], got_grad, here.at(core=1 - here.core))
    loads[1].wait()
    swap_grad.wait_recv()
    pair = jnp.concatenate([grads[here.core], got_grad[...]], axis=0)

    @pl.loop(0, 16, unroll=4)
    def _(i):
        at = pl.ds(pl.multiple_of(i * 256, 256), 256)
        n = jnp.concatenate([norm_t[0, at, :], norm_t[1, at, :]], axis=1)
        w = jnp.dot(n, pair, preferred_element_type=F32).astype(BF)
        for x in range(4):
            for u in range(4):
                row = x * 64 + u * 16
                big[u, i // 4, i % 4, x] = w[row : row + 16]

    def backward_rows():
        for copy in loads[2:]:
            copy.wait()
        rms = rms_in[:, :1]
        key_grad, value_grad = grads[0], grads[1]
        nt = (((1,), (1,)), ((), ()))
        inner = jnp.zeros((128, 128), F32)
        for c in range(16):
            at = slice(c * 256, (c + 1) * 256)
            ng = lax.dot_general(key_grad, kw[at, :], nt, preferred_element_type=F32)
            ng = ng + lax.dot_general(value_grad, vw[at, :], nt, preferred_element_type=F32)
            t = tokens[:, at].astype(F32)
            wide_grad[:, at] = ng
            across_rows = jnp.sum(ng * t * rms, axis=0, keepdims=True)
            weighted = ng * norm_gain[:, at] * t
            inner = inner + weighted[:, :128] + weighted[:, 128:]
            for k in range(2):
                row = c * 2 + k
                gain[row // 8, row % 8 : row % 8 + 1, :] = across_rows[:, k * 128 : (k + 1) * 128]
        mean = jnp.sum(inner, axis=1, keepdims=True) / 4096.0
        cube = rms**3 * mean
        for c in range(16):
            at = slice(c * 256, (c + 1) * 256)
            grad_rows[:, at] = (
                rms * norm_gain[:, at] * wide_grad[:, at] - tokens[:, at].astype(F32) * cube
            ).astype(BF)

    def device(axis, value):
        return here.at(**{axis: value})

    plans = []
    for u, lo, width, order, up in PARTS:
        f, f2 = (flip1, flip3) if up else (flip3, flip1)
        a0, a1, a2 = order
        left = [a for a in "zyx" if a != a0]
        plans.append((u, pl.ds(lo, width), f, f2, a0, a1, a2, left.index(a1) == 0))

    def slab(ref, u, axis, value, lanes):
        if axis == "z":
            return ref.at[u, value, :, :, :, lanes]
        if axis == "y":
            return ref.at[u, :, value, :, :, lanes]
        return ref.at[u, :, :, value, :, lanes]

    def slab1(u, value, lanes, leading):
        return s1.at[u, value, :, :, lanes] if leading else s1.at[u, :, value, :, lanes]

    def wide(ref):
        return ref[...].astype(F32)

    waits = {}

    zf, yf, xf = place["z"], place["y"], place["x"]
    gain_routes = (
        [device("z", flip3(zf))]
        + [device("y", flip1(yf)), device("y", flip3(yf)), device("x", flip1(xf)), device("x", flip3(xf))]
        + [here.at(core=1 - here.core)]
    )
    gain_now = []

    def gain_step(step):
        if step == 0:
            gain_now.append(
                [
                    net.start(gain.at[flip1(zf)], gain_got.at[0], device("z", flip1(zf))),
                    net.start(gain.at[flip2(zf)], gain_got.at[1], device("z", flip1(zf))),
                ]
            )
            return
        for copy in gain_now[-1]:
            copy.wait_recv()
        if step == 1:
            gain_sent[0] = gain[flip3(zf)] + gain_got[1]
            gain_sent[1] = gain[zf] + gain_got[0]
            gain_now.append([net.start(gain_sent.at[0], gain_got.at[2], gain_routes[0])])
            return
        if step == 2:
            gain_sent[2] = gain_sent[1] + gain_got[2]
        else:
            gain_sent[step] = gain_sent[step - 1] + gain_got[step]
        if step < 7:
            gain_now.append(
                [net.start(gain_sent.at[step], gain_got.at[step + 1], gain_routes[step - 1])]
            )

    for step in range(6):
        for p, (u, lanes, f, f2, a0, a1, a2, leading) in enumerate(plans):
            m0, m1, m2 = place[a0], place[a1], place[a2]
            if step == 0:
                to = device(a0, f(m0))
                waits[p, 0, 1] = net.start(
                    slab(big, u, a0, flip2(m0), lanes), r0.at[u, 1, :, :, :, lanes], to
                )
                waits[p, 0, 0] = net.start(
                    slab(big, u, a0, f(m0), lanes), r0.at[u, 0, :, :, :, lanes], to
                )
            elif step == 1:
                waits[p, 0, 1].wait_recv()
                s0[u, :, :, :, lanes] = (
                    wide(slab(big, u, a0, f2(m0), lanes)) + r0[u, 1, :, :, :, lanes].astype(F32)
                ).astype(BF)
                waits[p, 1] = net.start(
                    s0.at[u, :, :, :, lanes], r1.at[u, :, :, :, lanes], device(a0, f2(m0))
                )
            elif step == 2:
                waits[p, 0, 0].wait_recv()
                waits[p, 1].wait_recv()
                s1[u, :, :, :, lanes] = (
                    wide(slab(big, u, a0, m0, lanes))
                    + r0[u, 0, :, :, :, lanes].astype(F32)
                    + r1[u, :, :, :, lanes].astype(F32)
                ).astype(BF)
                to = device(a1, f(m1))
                waits[p, 2, 1] = net.start(
                    slab1(u, flip2(m1), lanes, leading), r2.at[u, 1, :, :, lanes], to
                )
                waits[p, 2, 0] = net.start(
                    slab1(u, f(m1), lanes, leading), r2.at[u, 0, :, :, lanes], to
                )
            elif step == 3:
                waits[p, 2, 1].wait_recv()
                s2[u, :, :, lanes] = (
                    wide(slab1(u, f2(m1), lanes, leading)) + r2[u, 1, :, :, lanes].astype(F32)
                ).astype(BF)
                waits[p, 3] = net.start(
                    s2.at[u, :, :, lanes], r3.at[u, :, :, lanes], device(a1, f2(m1))
                )
            elif step == 4:
                waits[p, 2, 0].wait_recv()
                waits[p, 3].wait_recv()
                s3[u, :, :, lanes] = (
                    wide(slab1(u, m1, lanes, leading))
                    + r2[u, 0, :, :, lanes].astype(F32)
                    + r3[u, :, :, lanes].astype(F32)
                ).astype(BF)
                to = device(a2, f(m2))
                waits[p, 4, 1] = net.start(
                    s3.at[u, flip2(m2), :, lanes], r4.at[u, 1, :, lanes], to
                )
                waits[p, 4, 0] = net.start(s3.at[u, f(m2), :, lanes], r4.at[u, 0, :, lanes], to)
            else:
                waits[p, 4, 1].wait_recv()
                s4[u, :, lanes] = (
                    s3[u, f2(m2), :, lanes].astype(F32) + r4[u, 1, :, lanes].astype(F32)
                ).astype(BF)
                waits[p, 5] = net.start(
                    s4.at[u, :, lanes], r5.at[u, :, lanes], device(a2, f2(m2))
                )
        if step == 0:
            backward_rows()
            keep_rows = pltpu.make_async_copy(grad_rows, rows_out, load_sems.at[5])
            keep_rows.start()
        gain_step(step)
    for p, (u, lanes, f, f2, a0, a1, a2, leading) in enumerate(plans):
        waits[p, 4, 0].wait_recv()
        waits[p, 5].wait_recv()
        full[u // 2, u % 2, :, lanes] = (
            s3[u, place[a2], :, lanes].astype(F32)
            + r4[u, 0, :, lanes].astype(F32)
            + r5[u, :, lanes].astype(F32)
        )
    gain_step(6)
    swap = net.start(full.at[1 - here.core], out.at[here.core], here.at(core=1 - here.core))
    out[here.core] = full[here.core]
    gain_step(7)
    gain_out[...] = gain_sent[7]
    swap.wait_recv()
    for copy in rest:
        copy.wait_recv()
    for copy in local:
        copy.wait()
    keep_rows.wait()
    net.finish()


def tail(att, dq, term, tokens, norm_t, rms, norm_gain, key_w, value_w, cos, sin):
    vm = pl.BlockSpec(memory_space=VM)
    any_ = pl.BlockSpec(memory_space=pl.ANY)
    end = (16, 512)
    return pl.pallas_call(
        tail_kernel,
        name="tail",
        out_shape=(
            jax.ShapeDtypeStruct((2, 64, 2048), BF),
            jax.ShapeDtypeStruct((2, 64, 2048), BF),
            jax.ShapeDtypeStruct((128, 4096), BF),
            jax.ShapeDtypeStruct((2, 2, *end), F32),
            jax.ShapeDtypeStruct((8, 128), F32),
        ),
        in_specs=[any_] * 5 + [vm] * 2 + [any_] * 2 + [vm] * 2,
        out_specs=(any_,) * 3 + (vm,) * 2,
        scratch_shapes=[
            VM((2, 8, 4, 64, 256), BF),
            VM((128, 4096), BF),
            VM((2, 4096, 128), BF),
            VM((4096, 512), BF),
            VM((4096, 512), BF),
            VM((2, 2, 2, 2, 2, 64, 256), BF),
            VM((2, 2, 2, 2, 64, 256), BF),
            VM((2, 2, 2, 2, 64, 256), BF),
            VM((2, 2, 4, 64, 256), BF),
            VM((2, 4, 64, 256), BF),
            VM((2, 4, 64, 256), BF),
            VM((2, 4, 64, 256), BF),
            VM((128, 4096), BF),
            VM((2, 128, 512), BF),
            VM((128, 512), BF),
            VM((4, 4, 4, 4, *end), BF),
            VM((128, 4096), F32),
            VM((4, 8, 128), F32),
            VM((4, 2, 4, 4, *end), BF),
            VM((4, 4, 4, *end), BF),
            VM((4, 4, 4, *end), BF),
            VM((4, 4, 4, *end), BF),
            VM((4, 2, 4, *end), BF),
            VM((4, 4, *end), BF),
            VM((4, 4, *end), BF),
            VM((4, 4, *end), BF),
            VM((4, 2, *end), BF),
            VM((4, *end), BF),
            VM((4, *end), BF),
            VM((2, 2, *end), F32),
            VM((8, 8, 128), F32),
            VM((8, 8, 128), F32),
            pltpu.SemaphoreType.DMA((N_TAIL,)),
            pltpu.SemaphoreType.DMA((N_TAIL,)),
            pltpu.SemaphoreType.DMA((4,)),
            pltpu.SemaphoreType.DMA((6,)),
        ],
        compiler_params=pltpu.CompilerParams(
            collective_id=2, has_side_effects=True, vmem_limit_bytes=60 * 1024 * 1024
        ),
    )(att, dq, term, tokens, norm_t, rms, norm_gain, key_w, value_w, cos, sin)


def rotation(token_pos, head_size):
    half_dim = head_size // 2
    frequency = ROPE_BASE ** (-2.0 * jnp.arange(half_dim, dtype=F32) / head_size)
    angles = token_pos.astype(F32)[:, None] * frequency[None, :]
    angles = jnp.concatenate([angles, angles], axis=1)
    return (jnp.cos(angles), jnp.sin(angles))


def body(tokens, queries, d_attended, span_order, norm_gain, key_weight, value_weight):
    seqs, rows, width = tokens.shape
    count = seqs * rows
    ctx = lax.axis_index("ctx")
    span_len = rows // 2
    own_spans = lax.dynamic_slice_in_dim(span_order, ctx * 2, 2, 0)
    own_pos = (own_spans[:, None] * span_len + jnp.arange(span_len, dtype=jnp.int32)).reshape(-1)
    cosine, sine = rotation(own_pos, HEAD_DIM)
    sine = jnp.concatenate([-sine[:, : HEAD_DIM // 2], sine[:, HEAD_DIM // 2 :]], axis=1)

    flat = tokens.reshape(count, width)
    gain_row = norm_gain.reshape(1, width)
    qr, dr, kvr, norm_t, rms = front(
        queries, d_attended, flat, gain_row, key_weight, value_weight, cosine, sine
    )
    att, dq, term = attend(
        span_order, qr.reshape(2, 8, 32, 512), dr.reshape(2, 8, 32, 512), kvr.reshape(2, KEYS, 256)
    )
    done = tail(
        att.reshape(2, 4, rows, 512), dq.reshape(2, 4, rows, 512),
        term.reshape(2, 8, 4, rows, 256), flat, norm_t, rms, gain_row,
        key_weight, value_weight, cosine, sine,
    )
    attended, grad_queries, grad_rows, weights, gain = done
    attended, grad_queries, grad_rows, grad_keys, grad_values, gain = finish(
        attended, grad_queries, grad_rows, weights.reshape(2, 32, 512), gain
    )
    return (
        attended,
        grad_queries,
        grad_rows.reshape(seqs, rows, width),
        grad_keys,
        grad_values,
        gain.reshape(32),
    )


def solution(mesh):
    placed = (P("dp", "ctx", None), P("dp", "ctx", None), P("dp", "ctx", None), P(), P(), P(), P())
    return jax.shard_map(
        body,
        mesh=mesh,
        in_specs=placed,
        out_specs=(
            P("dp", "ctx", None),
            P("dp", "ctx", None),
            P("dp", "ctx", None),
            P(("ctx", "dp"), None),
            P(("ctx", "dp"), None),
            P(("ctx", "dp")),
        ),
        check_vma=False,
    )
```

```python
import functools
import math

import jax
import jax.numpy as jnp
from jax import lax
from jax.experimental import pallas as pl
from jax.experimental.pallas import tpu as pltpu
from jax.sharding import PartitionSpec as P

KV_HEADS = 4
HEAD_DIM = 128
ROPE_BASE = 500000.0
EPSILON = 1e-05
BF = jnp.bfloat16
F32 = jnp.float32
VM = pltpu.VMEM
MESH = pl.DeviceIdType.MESH


def flip1(a):
    return a + 1 - 2 * (a % 2)


def flip3(a):
    return 3 - a


def flip2(a):
    return (a + 2) % 4


class Here:
    def __init__(self):
        ctx = lax.axis_index("ctx")
        dp = lax.axis_index("dp")
        self.z = ctx // 8
        self.y = (ctx // 2) % 4
        self.xh = ctx % 2
        self.xl = dp // 2
        self.core = dp % 2
        self.x = self.xh * 2 + self.xl

    def at(self, z=None, y=None, x=None, core=None):
        z = self.z if z is None else z
        y = self.y if y is None else y
        core = self.core if core is None else core
        if x is None:
            xh, xl = self.xh, self.xl
        else:
            xh, xl = x // 2, x % 2
        return {"ctx": z * 8 + y * 2 + xh, "dp": xl * 2 + core}


class Net:
    def __init__(self, send_sems, recv_sems):
        self.send_sems = send_sems
        self.recv_sems = recv_sems
        self.made = []

    def start(self, src, dst, device):
        k = len(self.made)
        copy = pltpu.make_async_remote_copy(
            src_ref=src,
            dst_ref=dst,
            send_sem=self.send_sems.at[k],
            recv_sem=self.recv_sems.at[k],
            device_id=device,
            device_id_type=MESH,
        )
        copy.start()
        self.made.append(copy)
        return copy

    def finish(self):
        for copy in self.made:
            copy.wait_send()


def greet(devices):
    barrier = pltpu.get_barrier_semaphore()
    for device in devices:
        pl.semaphore_signal(barrier, inc=1, device_id=device, device_id_type=MESH)
    pl.semaphore_wait(barrier, len(devices))


def cols(index, width):
    return pl.ds(pl.multiple_of(index * width, width), width)


KEYS = 2048
CHUNK = 256
PIECES = 8
PARTS = (
    (0, 0, 128, "zyx", True),
    (1, 0, 128, "yxz", True),
    (2, 0, 256, "xzy", True),
    (0, 128, 384, "zyx", False),
    (1, 128, 384, "yxz", False),
    (2, 256, 256, "xzy", False),
    (3, 0, 256, "zyx", True),
    (3, 256, 256, "yxz", True),
)
N_COPIES = 47 + 46 + 1 + 9 * len(PARTS) + 10 + 1
SHAPES = dict(
    kw=((4096, 512), BF),
    vw=((4096, 512), BF),
    normed=((128, 4096), BF),
    acc=((2, 128, 512), F32),
    kv=((2, 64, 1024), BF),
    norm_t=((2, 4096, 128), BF),
    qr=((2, 4, 64, 512), BF),
    dr=((2, 4, 64, 512), BF),
    kvr=((2, 8, 4, 64, 256), BF),
    key_pos=((2, KEYS, 128), jnp.int32),
    score=((KEYS, 256), F32),
    prob=((KEYS, 256), BF),
    key_t=((128, KEYS), BF),
    value_t=((128, KEYS), BF),
    acc_k=((KEYS, 128), F32),
    acc_v=((KEYS, 128), F32),
    att=((2, 4, 64, 512), BF),
    dq=((2, 4, 64, 512), BF),
    term=((2, 8, 4, 64, 256), BF),
    got1=((2, 2, 2, 2, 2, 64, 256), BF),
    sum1=((2, 2, 2, 2, 64, 256), BF),
    got2=((2, 2, 2, 2, 64, 256), BF),
    part=((2, 4, 64, 256), BF),
    got3=((2, 4, 64, 256), BF),
    final=((2, 4, 64, 256), BF),
    whole=((2, 4, 64, 256), BF),
    grads=((2, 128, 512), BF),
    got_grad=((128, 512), BF),
    big=((4, 4, 4, 4, 16, 512), BF),
    wide_grad=((128, 4096), F32),
    grad_rows=((128, 4096), BF),
    gain=((4, 8, 128), F32),
    r0=((4, 2, 4, 4, 16, 512), BF),
    s0=((4, 4, 4, 16, 512), BF),
    r1=((4, 4, 4, 16, 512), BF),
    s1=((4, 4, 4, 16, 512), BF),
    r2=((4, 3, 4, 16, 512), BF),
    s3=((4, 4, 16, 512), BF),
    r4=((4, 3, 16, 512), BF),
    full=((2, 2, 16, 512), F32),
    gain_got=((10, 8, 128), F32),
    gain_sum=((3, 8, 128), F32),
)


class Box:
    pass


def layer_kernel(
    spans, q, do, tokens, norm_gain, key_w, value_w, cos, sin,
    att_out, dq_out, rows_out, out, gain_out, *scratch,
):
    b = Box()
    for name, ref in zip(SHAPES, scratch):
        setattr(b, name, ref)
    send_sems, recv_sems, local_sems, weight_sems = scratch[len(SHAPES) :]
    here = Here()
    place = {"z": here.z, "y": here.y, "x": here.x}
    z, y, xh = here.z, here.y, here.xh
    x2 = flip2(here.x)
    twin = here.at(core=1 - here.core)
    turns = (flip1, flip3, flip2)
    piece = 4096 // PIECES
    loads = []
    for c in range(PIECES):
        for w, (src, dst) in enumerate(((key_w, b.kw), (value_w, b.vw))):
            at = pl.ds(c * piece, piece)
            copy = pltpu.make_async_copy(src.at[at], dst.at[at], weight_sems.at[2 * c + w])
            copy.start()
            loads.append(copy)
    greet([here.at(**{a: f(place[a])}) for a in "zyx" for f in turns] + [twin])
    net = Net(send_sems, recv_sems)

    def along(s, value):
        return here.at(z=value) if s == 0 else here.at(y=value)

    def across(s, value):
        return here.at(y=value) if s == 0 else here.at(z=value)

    head = [z, y]
    ring = [y, z]
    mine = [ring[s] * 2 + xh for s in range(2)]
    local = []

    def keep(src, dst):
        copy = pltpu.make_async_copy(src, dst, local_sems.at[len(local)])
        copy.start()
        local.append(copy)
        return copy

    rows_in = [[], []]

    def send_rows(s, src, dst):
        for f in turns:
            to = f(head[s])
            rows_in[s].append(
                net.start(src.at[s, :, cols(to, 512)], dst.at[s, head[s]], along(s, to))
            )
        rows_in[s].append(keep(src.at[s, :, cols(head[s], 512)], dst.at[s, head[s]]))

    def arrived(copy):
        if any(copy is c for c in local):
            copy.wait()
        else:
            copy.wait_recv()

    for s in range(2):
        send_rows(s, q, b.qr)
    squares = jnp.zeros((128, 128), F32)
    for c in range(32):
        t = tokens[:, c * 128 : (c + 1) * 128].astype(F32)
        squares = squares + t * t
    rms = lax.rsqrt(jnp.sum(squares, axis=1, keepdims=True) / 4096.0 + EPSILON)
    for c in range(PIECES):
        at = slice(c * piece, (c + 1) * piece)
        b.normed[:, at] = (tokens[:, at].astype(F32) * rms * norm_gain[:, at]).astype(BF)
    for c in range(PIECES):
        at = slice(c * piece, (c + 1) * piece)
        n = b.normed[:, at]
        for w, ref in enumerate((b.kw, b.vw)):
            loads[2 * c + w].wait()
            product = jnp.dot(n, ref[at, :], preferred_element_type=F32)
            if c == 0:
                b.acc[w] = product
            else:
                b.acc[w] += product

    def widen(half):
        both = jnp.concatenate([half, half], axis=1)
        return jnp.concatenate([both, both], axis=0)

    lane = lax.broadcasted_iota(jnp.int32, (128, 128), 1)
    both_cos = widen(cos[...])
    both_sin = widen(sin[...])
    both_sin = jnp.where(lane < 64, -both_sin, both_sin)
    for h in range(KV_HEADS):
        at = slice(h * 128, (h + 1) * 128)
        u = b.acc[0, :, at]
        k = (u * both_cos + pltpu.roll(u, 64, 1) * both_sin).astype(BF)
        v = b.acc[1, :, at].astype(BF)
        for s in range(2):
            b.kv[s, :, h * 256 : h * 256 + 128] = k[s * 64 : (s + 1) * 64]
            b.kv[s, :, h * 256 + 128 : (h + 1) * 256] = v[s * 64 : (s + 1) * 64]

    kv_in = [[], []]
    for s in range(2):
        for f in (flip2, flip1, flip3):
            to = f(head[s])
            kv_in[s].append(
                net.start(b.kv.at[s, :, cols(to, 256)], b.kvr.at[s, mine[s], head[s]], along(s, to))
            )
        kv_in[s].append(keep(b.kv.at[s, :, cols(head[s], 256)], b.kvr.at[s, mine[s], head[s]]))
    send_rows(0, do, b.dr)
    for c in range(32):
        at = slice(c * 128, (c + 1) * 128)
        b.norm_t[0, at, :] = b.normed[:, at].T

    first = {}
    last = [[], []]
    swapped = {}

    def spread(s, of, half):
        f = (flip1, flip3)[half]
        block = b.kvr.at[s, ring[s] * 2 + (xh if of == 0 else 1 - xh), 2 * half : 2 * half + 2]
        first[s, of, half] = net.start(block, block, across(s, f(ring[s])))

    def spread_on(s, of):
        for half, f, g in ((0, flip1, flip3), (1, flip3, flip1)):
            first[s, of, half].wait_recv()
            for value in (ring[s], f(ring[s])):
                slot = value * 2 + (xh if of == 0 else 1 - xh)
                block = b.kvr.at[s, slot, 2 * half : 2 * half + 2]
                last[s].append(net.start(block, block, across(s, g(ring[s]))))

    def gather_own(s):
        for copy in kv_in[s]:
            arrived(copy)
        for half in range(2):
            block = b.kvr.at[s, mine[s], 2 * half : 2 * half + 2]
            swapped[s, half] = net.start(block, block, here.at(x=x2))
        for half in range(2):
            spread(s, 0, half)

    def gather_swapped(s):
        for half in range(2):
            swapped[s, half].wait_recv()
            spread(s, 1, half)

    gather_own(0)
    gather_own(1)
    norm_in = net.start(b.norm_t.at[0], b.norm_t.at[1], twin)
    offset = lax.broadcasted_iota(jnp.int32, (32, 128), 0)
    for i in range(64):
        m, w, n, half = i // 16, (i // 8) % 2, (i // 2) % 4, i % 2
        for s in range(2):
            zz, yy = (n, m) if s == 0 else (m, n)
            span = spans[((zz * 4 + yy) * 2 + w) * 2 + half]
            b.key_pos[s, i * 32 : (i + 1) * 32, :] = offset + span * 32
    spread_on(0, 0)
    send_rows(1, do, b.dr)
    gather_swapped(0)
    spread_on(0, 1)
    spread_on(1, 0)

    scale = HEAD_DIM ** (-0.5)
    to_two = scale * math.log2(math.e)
    slots_of = [slice(c * CHUNK, (c + 1) * CHUNK) for c in range(KEYS // CHUNK)]
    returned = []

    def keys_of(s, c):
        return b.kvr[s, c, :, :, :128].reshape(CHUNK, 128)

    def values_of(s, c):
        return b.kvr[s, c, :, :, 128:].reshape(CHUNK, 128)

    def ready(s):
        for copy in last[s]:
            copy.wait_recv()
        for copy in rows_in[s]:
            arrived(copy)
        for c, rows in enumerate(slots_of):
            b.key_t[:, rows] = keys_of(s, c).T
            b.value_t[:, rows] = values_of(s, c).T

    def stack(ref, s, block):
        both = ref[s, block]
        return jnp.concatenate([both[:, h * 128 : (h + 1) * 128] for h in range(4)], axis=0)

    def attention(s, order):
        f = (flip1, flip3, flip2, lambda a: a)[order]
        block = f(head[s])
        queries = stack(b.qr, s, block)
        grads = stack(b.dr, s, block)
        q_t = queries.T
        do_t = grads.T
        start = (block * 4 + y) * 4 + xh * 2 if s == 0 else (z * 4 + block) * 4 + xh * 2
        column = lax.broadcasted_iota(jnp.int32, (1, 256), 1)
        q_pos = column % 32 + 32 * jnp.where(column % 64 < 32, spans[start], spans[start + 1])
        top = jnp.full((8, 256), -1e30, F32)
        for c, rows in enumerate(slots_of):
            t = jnp.dot(keys_of(s, c), q_t, preferred_element_type=F32)
            k_pos = b.key_pos[s, rows, :]
            k_pos = jnp.concatenate([k_pos, k_pos], axis=1)
            t = jnp.where(k_pos <= q_pos, t, -1e30)
            b.score[rows, :] = t
            top = jnp.maximum(top, jnp.max(t.reshape(CHUNK // 8, 8, 256), axis=0))
        top = jnp.max(top, axis=0, keepdims=True)
        total = jnp.zeros((8, 256), F32)
        for rows in slots_of:
            e = jnp.exp2((b.score[rows, :] - top) * to_two)
            b.score[rows, :] = e
            total = total + jnp.sum(e.reshape(CHUNK // 8, 8, 256), axis=0)
        inverse = 1.0 / jnp.sum(total, axis=0, keepdims=True)
        out_t = jnp.zeros((128, 256), F32)
        for rows in slots_of:
            p = (b.score[rows, :] * inverse).astype(BF)
            b.prob[rows, :] = p
            out_t = out_t + jnp.dot(b.value_t[:, rows], p, preferred_element_type=F32)
        out_t = out_t.astype(BF)
        delta = jnp.sum(out_t.astype(F32) * do_t.astype(F32), axis=0, keepdims=True)
        dq_t = jnp.zeros((128, 256), F32)
        for c, rows in enumerate(slots_of):
            dp = jnp.dot(values_of(s, c), do_t, preferred_element_type=F32)
            ds = (b.score[rows, :] * inverse * (dp - delta)).astype(BF)
            k_term = jnp.dot(ds, queries, preferred_element_type=F32)
            v_term = jnp.dot(b.prob[rows, :], grads, preferred_element_type=F32)
            if order > 0:
                k_term = k_term + b.acc_k[rows, :]
                v_term = v_term + b.acc_v[rows, :]
            if order < 3:
                b.acc_k[rows, :] = k_term
                b.acc_v[rows, :] = v_term
            else:
                b.term[s, c, :, :, :128] = (k_term * scale).astype(BF).reshape(4, 64, 128)
                b.term[s, c, :, :, 128:] = v_term.astype(BF).reshape(4, 64, 128)
            dq_t = dq_t + jnp.dot(b.key_t[:, rows], ds, preferred_element_type=F32)
        attended = out_t.T
        dq = (dq_t * scale).astype(BF).T
        for h in range(4):
            at = slice(h * 64, (h + 1) * 64)
            b.att[s, block, :, h * 128 : (h + 1) * 128] = attended[at]
            b.dq[s, block, :, h * 128 : (h + 1) * 128] = dq[at]
        for src, dst in ((b.att, att_out), (b.dq, dq_out)):
            dst = dst.at[s, :, cols(head[s], 512)]
            if order < 3:
                returned.append(net.start(src.at[s, block], dst, along(s, block)))
            else:
                returned.append(keep(src.at[s, block], dst))

    flips = ((flip3, flip1), (flip1, flip3))
    one, two, three, owners = {}, {}, {}, [[], []]

    def half_of(half):
        return slice(2 * half, 2 * half + 2)

    def side(k):
        return 1 - xh if k == 0 else xh

    def sum_one(s, k):
        for j in (1, 0):
            for half in range(2):
                f, g = flips[half]
                target = f(ring[s])
                slot = target if j == 0 else g(target)
                one[s, half, j, k] = net.start(
                    b.term.at[s, slot * 2 + side(k), half_of(half)],
                    b.got1.at[s, half, j, k],
                    across(s, target),
                )

    def sum_two(s, k):
        for half in range(2):
            f, g = flips[half]
            one[s, half, 1, k].wait_recv()
            b.sum1[s, half, k] = (
                b.term[s, g(ring[s]) * 2 + side(k), half_of(half)].astype(F32)
                + b.got1[s, half, 1, k].astype(F32)
            ).astype(BF)
            two[s, half, k] = net.start(
                b.sum1.at[s, half, k], b.got2.at[s, half, k], across(s, g(ring[s]))
            )

    def summed(s, half, k):
        one[s, half, 0, k].wait_recv()
        two[s, half, k].wait_recv()
        return (
            b.term[s, ring[s] * 2 + side(k), half_of(half)].astype(F32)
            + b.got1[s, half, 0, k].astype(F32)
            + b.got2[s, half, k].astype(F32)
        )

    def sum_three(s):
        for half in range(2):
            at = half_of(half)
            b.part[s, at] = summed(s, half, 0).astype(BF)
            three[s, half] = net.start(b.part.at[s, at], b.got3.at[s, at], here.at(x=x2))

    def sum_four(s):
        for half in range(2):
            at = half_of(half)
            total = summed(s, half, 1)
            three[s, half].wait_recv()
            b.final[s, at] = (total + b.got3[s, at].astype(F32)).astype(BF)
        for f in (flip2, flip1, flip3):
            to = f(head[s])
            owners[s].append(
                net.start(b.final.at[s, to], b.whole.at[s, head[s]], along(s, to))
            )
        b.whole[s, head[s]] = b.final[s, head[s]]

    def rotate_rows(s):
        for copy in owners[s]:
            copy.wait_recv()
        rows = slice(s * 64, (s + 1) * 64)
        for h in range(KV_HEADS):
            at = slice(h * 128, (h + 1) * 128)
            u = b.whole[s, h, :, :128].astype(F32)
            b.grads[0, rows, at] = (
                u * both_cos[:64] - pltpu.roll(u, 64, 1) * both_sin[:64]
            ).astype(BF)
            b.grads[1, rows, at] = b.whole[s, h, :, 128:]

    ready(0)
    attention(0, 0)
    gather_swapped(1)
    attention(0, 1)
    spread_on(1, 1)
    attention(0, 2)
    attention(0, 3)
    sum_one(0, 0)
    sum_one(0, 1)
    ready(1)
    attention(1, 0)
    sum_two(0, 0)
    sum_two(0, 1)
    attention(1, 1)
    sum_three(0)
    attention(1, 2)
    sum_four(0)
    attention(1, 3)
    sum_one(1, 0)
    rotate_rows(0)
    sum_two(1, 0)
    sum_one(1, 1)
    sum_three(1)
    sum_two(1, 1)
    sum_four(1)
    rotate_rows(1)

    swap_grad = net.start(b.grads.at[1 - here.core], b.got_grad, twin)
    norm_in.wait_recv()
    swap_grad.wait_recv()
    pair = jnp.concatenate([b.grads[here.core], b.got_grad[...]], axis=0)

    @pl.loop(0, 16, unroll=4)
    def _(i):
        at = pl.ds(pl.multiple_of(i * 256, 256), 256)
        n = jnp.concatenate([b.norm_t[0, at, :], b.norm_t[1, at, :]], axis=1)
        w = jnp.dot(n, pair, preferred_element_type=F32).astype(BF)
        for x in range(4):
            for u in range(4):
                row = x * 64 + u * 16
                b.big[u, i // 4, i % 4, x] = w[row : row + 16]

    def backward_rows():
        key_grad, value_grad = b.grads[0], b.grads[1]
        nt = (((1,), (1,)), ((), ()))
        inner = jnp.zeros((128, 128), F32)
        for c in range(16):
            at = slice(c * 256, (c + 1) * 256)
            ng = lax.dot_general(key_grad, b.kw[at, :], nt, preferred_element_type=F32)
            ng = ng + lax.dot_general(value_grad, b.vw[at, :], nt, preferred_element_type=F32)
            t = tokens[:, at].astype(F32)
            b.wide_grad[:, at] = ng
            across_rows = jnp.sum(ng * t * rms, axis=0, keepdims=True)
            weighted = ng * norm_gain[:, at] * t
            inner = inner + weighted[:, :128] + weighted[:, 128:]
            for k in range(2):
                row = c * 2 + k
                b.gain[row // 8, row % 8 : row % 8 + 1, :] = across_rows[:, k * 128 : (k + 1) * 128]
        mean = jnp.sum(inner, axis=1, keepdims=True) / 4096.0
        cube = rms**3 * mean
        for c in range(16):
            at = slice(c * 256, (c + 1) * 256)
            b.grad_rows[:, at] = (
                rms * norm_gain[:, at] * b.wide_grad[:, at] - tokens[:, at].astype(F32) * cube
            ).astype(BF)

    def device(axis, value):
        return here.at(**{axis: value})

    plans = []
    for u, lo, width, order, up in PARTS:
        f, f2 = (flip1, flip3) if up else (flip3, flip1)
        a0, a1, a2 = order
        left = [a for a in "zyx" if a != a0]
        plans.append((u, pl.ds(lo, width), f, f2, a0, a1, a2, left.index(a1) == 0))

    def slab(u, axis, value, lanes):
        if axis == "z":
            return b.big.at[u, value, :, :, :, lanes]
        if axis == "y":
            return b.big.at[u, :, value, :, :, lanes]
        return b.big.at[u, :, :, value, :, lanes]

    def slab1(u, value, lanes, leading):
        return b.s1.at[u, value, :, :, lanes] if leading else b.s1.at[u, :, value, :, lanes]

    def wide(ref):
        return ref[...].astype(F32)

    gains = []

    def gain_step(step):
        if step == 0:
            tiles = [b.gain.at[f(z)] for f in turns]
            own = None
        else:
            own = b.gain[z] if step == 1 else b.gain_sum[step - 2]
            for k in range(3):
                gains[k].wait_recv()
                own = own + b.gain_got[3 * (step - 1) + k]
            del gains[:]
            b.gain_sum[step - 1] = own
            tiles = [b.gain_sum.at[step - 1]] * 3
        if step < 3:
            axis = "zyx"[step]
            for k, f in enumerate(turns):
                gains.append(
                    net.start(tiles[k], b.gain_got.at[3 * step + k], device(axis, f(place[axis])))
                )
        else:
            gains.append(net.start(tiles[0], b.gain_got.at[9], twin))

    waits = {}
    for j in (1, 0):
        for p, (u, lanes, f, f2, a0, a1, a2, leading) in enumerate(plans):
            m0 = place[a0]
            slot = flip2(m0) if j == 1 else f(m0)
            waits[p, 0, j] = net.start(
                slab(u, a0, slot, lanes), b.r0.at[u, j, :, :, :, lanes], device(a0, f(m0))
            )
    backward_rows()
    keep_rows = keep(b.grad_rows, rows_out)
    gain_step(0)
    for p, (u, lanes, f, f2, a0, a1, a2, leading) in enumerate(plans):
        m0 = place[a0]
        waits[p, 0, 1].wait_recv()
        b.s0[u, :, :, :, lanes] = (
            wide(slab(u, a0, f2(m0), lanes)) + b.r0[u, 1, :, :, :, lanes].astype(F32)
        ).astype(BF)
        waits[p, 1] = net.start(
            b.s0.at[u, :, :, :, lanes], b.r1.at[u, :, :, :, lanes], device(a0, f2(m0))
        )
    gain_step(1)
    for p, (u, lanes, f, f2, a0, a1, a2, leading) in enumerate(plans):
        m0, m1 = place[a0], place[a1]
        waits[p, 0, 0].wait_recv()
        waits[p, 1].wait_recv()
        b.s1[u, :, :, :, lanes] = (
            wide(slab(u, a0, m0, lanes))
            + b.r0[u, 0, :, :, :, lanes].astype(F32)
            + b.r1[u, :, :, :, lanes].astype(F32)
        ).astype(BF)
        for k, turn in enumerate(turns):
            waits[p, 2, k] = net.start(
                slab1(u, turn(m1), lanes, leading),
                b.r2.at[u, k, :, :, lanes],
                device(a1, turn(m1)),
            )
    gain_step(2)
    for p, (u, lanes, f, f2, a0, a1, a2, leading) in enumerate(plans):
        m1, m2 = place[a1], place[a2]
        total = wide(slab1(u, m1, lanes, leading))
        for k in range(3):
            waits[p, 2, k].wait_recv()
            total = total + b.r2[u, k, :, :, lanes].astype(F32)
        b.s3[u, :, :, lanes] = total.astype(BF)
        for k, turn in enumerate(turns):
            waits[p, 3, k] = net.start(
                b.s3.at[u, turn(m2), :, lanes], b.r4.at[u, k, :, lanes], device(a2, turn(m2))
            )
    gain_step(3)
    for p, (u, lanes, f, f2, a0, a1, a2, leading) in enumerate(plans):
        total = b.s3[u, place[a2], :, lanes].astype(F32)
        for k in range(3):
            waits[p, 3, k].wait_recv()
            total = total + b.r4[u, k, :, lanes].astype(F32)
        b.full[u // 2, u % 2, :, lanes] = total
    swap = net.start(b.full.at[1 - here.core], out.at[here.core], twin)
    out[here.core] = b.full[here.core]
    gains[0].wait_recv()
    gain_out[...] = b.gain_sum[2] + b.gain_got[9]
    swap.wait_recv()
    for copy in returned:
        arrived(copy)
    keep_rows.wait()
    net.finish()


def layer(spans, q, do, tokens, norm_gain, key_w, value_w, cos, sin):
    vm = pl.BlockSpec(memory_space=VM)
    any_ = pl.BlockSpec(memory_space=pl.ANY)
    return pl.pallas_call(
        layer_kernel,
        name="layer",
        out_shape=(
            jax.ShapeDtypeStruct((2, 64, 2048), BF),
            jax.ShapeDtypeStruct((2, 64, 2048), BF),
            jax.ShapeDtypeStruct((128, 4096), BF),
            jax.ShapeDtypeStruct((2, 2, 16, 512), F32),
            jax.ShapeDtypeStruct((8, 128), F32),
        ),
        in_specs=[pl.BlockSpec(memory_space=pltpu.SMEM), any_, any_, vm, vm, any_, any_, vm, vm],
        out_specs=(any_,) * 3 + (vm,) * 2,
        scratch_shapes=[VM(*shape) for shape in SHAPES.values()]
        + [
            pltpu.SemaphoreType.DMA((N_COPIES,)),
            pltpu.SemaphoreType.DMA((N_COPIES,)),
            pltpu.SemaphoreType.DMA((12,)),
            pltpu.SemaphoreType.DMA((2 * PIECES,)),
        ],
        compiler_params=pltpu.CompilerParams(
            collective_id=1, has_side_effects=True, vmem_limit_bytes=60 * 1024 * 1024
        ),
    )(spans, q, do, tokens, norm_gain, key_w, value_w, cos, sin)


def finish_kernel(
    att, dq, rows, weights, gain, att_to, dq_to, rows_to, keys_to, values_to, gain_to,
    att_v, dq_v, rows_v, weights_v, gain_v, sems,
):
    here = Here()
    loads = []
    for k, (src, dst) in enumerate(
        ((gain, gain_v), (att, att_v), (dq, dq_v), (rows, rows_v), (weights, weights_v))
    ):
        copy = pltpu.make_async_copy(src, dst, sems.at[k])
        copy.start()
        loads.append(copy)
    loads[0].wait()
    row = gain_v[pl.ds(here.y * 2 + here.xh, 1), :]
    dp = here.xl * 2 + here.core
    gain_to[...] = pltpu.roll(row, (128 - dp * 32) % 128, 1)[:, :32]
    stores = []
    for k, (load, src, dst) in enumerate(
        (
            (loads[1], att_v, att_to),
            (loads[2], dq_v, dq_to),
            (loads[3], rows_v, rows_to),
            (loads[4], weights_v.at[0], keys_to),
            (None, weights_v.at[1], values_to),
        )
    ):
        if load is not None:
            load.wait()
        copy = pltpu.make_async_copy(src, dst, sems.at[5 + k])
        copy.start()
        stores.append(copy)
    for copy in stores:
        copy.wait()


def finish(att, dq, rows, weights, gain):
    any_ = pl.BlockSpec(memory_space=pl.ANY)
    return pl.pallas_call(
        finish_kernel,
        name="finish",
        out_shape=(
            jax.ShapeDtypeStruct((2, 64, 2048), BF),
            jax.ShapeDtypeStruct((2, 64, 2048), BF),
            jax.ShapeDtypeStruct((128, 4096), BF),
            jax.ShapeDtypeStruct((32, 512), F32),
            jax.ShapeDtypeStruct((32, 512), F32),
            jax.ShapeDtypeStruct((1, 32), F32),
        ),
        in_specs=[any_] * 5,
        out_specs=(any_,) * 5 + (pl.BlockSpec(memory_space=VM),),
        scratch_shapes=[
            VM((2, 64, 2048), BF),
            VM((2, 64, 2048), BF),
            VM((128, 4096), BF),
            VM((2, 32, 512), F32),
            VM((8, 128), F32),
            pltpu.SemaphoreType.DMA((10,)),
        ],
        compiler_params=pltpu.CompilerParams(vmem_limit_bytes=60 * 1024 * 1024),
    )(att, dq, rows, weights, gain)


def body(tokens, queries, d_attended, span_order, norm_gain, key_weight, value_weight):
    seqs, rows, width = tokens.shape
    count = seqs * rows
    half_dim = HEAD_DIM // 2
    span_len = rows // 2
    own_spans = lax.dynamic_slice_in_dim(span_order, lax.axis_index("ctx") * 2, 2, 0)
    own_pos = (own_spans[:, None] * span_len + jnp.arange(span_len, dtype=jnp.int32)).reshape(-1)
    frequency = ROPE_BASE ** (-2.0 * jnp.arange(half_dim, dtype=F32) / HEAD_DIM)
    angles = own_pos.astype(F32)[:, None] * frequency[None, :]
    attended, grad_queries, grad_rows, weights, gain = layer(
        span_order, queries, d_attended, tokens.reshape(count, width), norm_gain.reshape(1, width),
        key_weight, value_weight, jnp.cos(angles), jnp.sin(angles),
    )
    attended, grad_queries, grad_rows, grad_keys, grad_values, gain = finish(
        attended, grad_queries, grad_rows, weights.reshape(2, 32, 512), gain
    )
    return (
        attended,
        grad_queries,
        grad_rows.reshape(seqs, rows, width),
        grad_keys,
        grad_values,
        gain.reshape(32),
    )


def solution(mesh):
    placed = (P("dp", "ctx", None), P("dp", "ctx", None), P("dp", "ctx", None), P(), P(), P(), P())
    return jax.shard_map(
        body,
        mesh=mesh,
        in_specs=placed,
        out_specs=(
            P("dp", "ctx", None),
            P("dp", "ctx", None),
            P("dp", "ctx", None),
            P(("ctx", "dp"), None),
            P(("ctx", "dp"), None),
            P(("ctx", "dp")),
        ),
        check_vma=False,
    )
```

```python
import functools
import math

import jax
import jax.numpy as jnp
from jax import lax
from jax.experimental import pallas as pl
from jax.experimental.pallas import tpu as pltpu
from jax.sharding import PartitionSpec as P

KV_HEADS = 4
HEAD_DIM = 128
ROPE_BASE = 500000.0
EPSILON = 1e-05
BF = jnp.bfloat16
F32 = jnp.float32
VM = pltpu.VMEM
MESH = pl.DeviceIdType.MESH


def flip1(a):
    return a + 1 - 2 * (a % 2)


def flip3(a):
    return 3 - a


def flip2(a):
    return (a + 2) % 4


class Here:
    def __init__(self):
        ctx = lax.axis_index("ctx")
        dp = lax.axis_index("dp")
        self.z = ctx // 8
        self.y = (ctx // 2) % 4
        self.xh = ctx % 2
        self.xl = dp // 2
        self.core = dp % 2
        self.x = self.xh * 2 + self.xl

    def at(self, z=None, y=None, x=None, core=None):
        z = self.z if z is None else z
        y = self.y if y is None else y
        core = self.core if core is None else core
        if x is None:
            xh, xl = self.xh, self.xl
        else:
            xh, xl = x // 2, x % 2
        return {"ctx": z * 8 + y * 2 + xh, "dp": xl * 2 + core}


class Net:
    def __init__(self, send_sems, recv_sems):
        self.send_sems = send_sems
        self.recv_sems = recv_sems
        self.made = []

    def start(self, src, dst, device):
        k = len(self.made)
        copy = pltpu.make_async_remote_copy(
            src_ref=src,
            dst_ref=dst,
            send_sem=self.send_sems.at[k],
            recv_sem=self.recv_sems.at[k],
            device_id=device,
            device_id_type=MESH,
        )
        copy.start()
        self.made.append(copy)
        return copy

    def finish(self):
        for copy in self.made:
            copy.wait_send()


def greet(devices):
    barrier = pltpu.get_barrier_semaphore()
    for device in devices:
        pl.semaphore_signal(barrier, inc=1, device_id=device, device_id_type=MESH)
    pl.semaphore_wait(barrier, len(devices))


def cols(index, width):
    return pl.ds(pl.multiple_of(index * width, width), width)


KEYS = 2048
CHUNK = 256
PIECES = 8
PARTS = (
    (0, 0, 128, "zyx", True),
    (1, 0, 128, "yxz", True),
    (2, 0, 256, "xzy", True),
    (0, 128, 384, "zyx", False),
    (1, 128, 384, "yxz", False),
    (2, 256, 256, "xzy", False),
    (3, 0, 256, "zyx", True),
    (3, 256, 256, "yxz", True),
)
N_COPIES = 47 + 46 + 1 + 9 * len(PARTS) + 10 + 1
SHAPES = dict(
    tokens=((128, 4096), BF),
    kw=((4096, 512), BF),
    vw=((4096, 512), BF),
    normed=((128, 4096), BF),
    acc=((2, 128, 512), F32),
    kv=((2, 64, 1024), BF),
    norm_t=((2, 4096, 128), BF),
    qr=((2, 4, 64, 512), BF),
    dr=((2, 4, 64, 512), BF),
    kvr=((2, 8, 4, 64, 256), BF),
    key_pos=((2, KEYS, 128), jnp.int32),
    score=((4, KEYS, 256), F32),
    prob=((4, KEYS, 256), BF),
    query_s=((4, 256, 128), BF),
    grad_s=((4, 256, 128), BF),
    grad_t=((4, 128, 256), BF),
    stats=((4, 2, 8, 256), F32),
    dq_t=((4, 128, 256), F32),
    key_t=((128, KEYS), BF),
    value_t=((128, KEYS), BF),
    att=((2, 4, 64, 512), BF),
    dq=((2, 4, 64, 512), BF),
    term=((2, 8, 4, 64, 256), BF),
    got1=((2, 2, 2, 2, 2, 64, 256), BF),
    sum1=((2, 2, 2, 2, 64, 256), BF),
    got2=((2, 2, 2, 2, 64, 256), BF),
    part=((2, 4, 64, 256), BF),
    got3=((2, 4, 64, 256), BF),
    final=((2, 4, 64, 256), BF),
    whole=((2, 4, 64, 256), BF),
    grads=((2, 128, 512), BF),
    got_grad=((128, 512), BF),
    big=((4, 4, 4, 4, 16, 512), BF),
    wide_grad=((128, 4096), F32),
    grad_rows=((128, 4096), BF),
    gain=((4, 8, 128), F32),
    r0=((4, 2, 4, 4, 16, 512), BF),
    s0=((4, 4, 4, 16, 512), BF),
    r1=((4, 4, 4, 16, 512), BF),
    s1=((4, 4, 4, 16, 512), BF),
    r2=((4, 3, 4, 16, 512), BF),
    s3=((4, 4, 16, 512), BF),
    r4=((4, 3, 16, 512), BF),
    full=((2, 2, 16, 512), F32),
    gain_got=((10, 8, 128), F32),
    gain_sum=((3, 8, 128), F32),
)


class Box:
    pass


def layer_kernel(
    spans, q, do, tokens_in, norm_gain, key_w, value_w, cos, sin,
    att_out, dq_out, rows_out, out, gain_out, *scratch,
):
    b = Box()
    for name, ref in zip(SHAPES, scratch):
        setattr(b, name, ref)
    send_sems, recv_sems, local_sems, weight_sems = scratch[len(SHAPES) :]
    tokens = b.tokens
    token_load = pltpu.make_async_copy(tokens_in, tokens, weight_sems.at[2 * PIECES])
    token_load.start()
    here = Here()
    place = {"z": here.z, "y": here.y, "x": here.x}
    z, y, xh = here.z, here.y, here.xh
    x2 = flip2(here.x)
    twin = here.at(core=1 - here.core)
    turns = (flip1, flip3, flip2)
    piece = 4096 // PIECES
    loads = []
    for c in range(PIECES):
        for w, (src, dst) in enumerate(((key_w, b.kw), (value_w, b.vw))):
            at = pl.ds(c * piece, piece)
            copy = pltpu.make_async_copy(src.at[at], dst.at[at], weight_sems.at[2 * c + w])
            copy.start()
            loads.append(copy)
    greet([here.at(**{a: f(place[a])}) for a in "zyx" for f in turns] + [twin])
    net = Net(send_sems, recv_sems)

    def along(s, value):
        return here.at(z=value) if s == 0 else here.at(y=value)

    def across(s, value):
        return here.at(y=value) if s == 0 else here.at(z=value)

    head = [z, y]
    ring = [y, z]
    mine = [ring[s] * 2 + xh for s in range(2)]
    local = []

    def keep(src, dst):
        copy = pltpu.make_async_copy(src, dst, local_sems.at[len(local)])
        copy.start()
        local.append(copy)
        return copy

    rows_in = [[], []]

    def send_rows(s, src, dst):
        for f in turns:
            to = f(head[s])
            rows_in[s].append(
                net.start(src.at[s, :, cols(to, 512)], dst.at[s, head[s]], along(s, to))
            )
        rows_in[s].append(keep(src.at[s, :, cols(head[s], 512)], dst.at[s, head[s]]))

    def arrived(copy):
        if any(copy is c for c in local):
            copy.wait()
        else:
            copy.wait_recv()

    send_rows(0, q, b.qr)
    token_load.wait()
    squares = jnp.zeros((128, 128), F32)
    for c in range(32):
        t = tokens[:, c * 128 : (c + 1) * 128].astype(F32)
        squares = squares + t * t
    rms = lax.rsqrt(jnp.sum(squares, axis=1, keepdims=True) / 4096.0 + EPSILON)
    for c in range(PIECES):
        at = slice(c * piece, (c + 1) * piece)
        b.normed[:, at] = (tokens[:, at].astype(F32) * rms * norm_gain[:, at]).astype(BF)
    for c in range(PIECES):
        at = slice(c * piece, (c + 1) * piece)
        n = b.normed[:, at]
        for w, ref in enumerate((b.kw, b.vw)):
            loads[2 * c + w].wait()
            product = jnp.dot(n, ref[at, :], preferred_element_type=F32)
            if c == 0:
                b.acc[w] = product
            else:
                b.acc[w] += product

    def widen(half):
        both = jnp.concatenate([half, half], axis=1)
        return jnp.concatenate([both, both], axis=0)

    lane = lax.broadcasted_iota(jnp.int32, (128, 128), 1)
    both_cos = widen(cos[...])
    both_sin = widen(sin[...])
    both_sin = jnp.where(lane < 64, -both_sin, both_sin)
    for h in range(KV_HEADS):
        at = slice(h * 128, (h + 1) * 128)
        u = b.acc[0, :, at]
        k = (u * both_cos + pltpu.roll(u, 64, 1) * both_sin).astype(BF)
        v = b.acc[1, :, at].astype(BF)
        for s in range(2):
            b.kv[s, :, h * 256 : h * 256 + 128] = k[s * 64 : (s + 1) * 64]
            b.kv[s, :, h * 256 + 128 : (h + 1) * 256] = v[s * 64 : (s + 1) * 64]

    kv_in = [[], []]
    for s in range(2):
        for f in (flip2, flip1, flip3):
            to = f(head[s])
            kv_in[s].append(
                net.start(b.kv.at[s, :, cols(to, 256)], b.kvr.at[s, mine[s], head[s]], along(s, to))
            )
        kv_in[s].append(keep(b.kv.at[s, :, cols(head[s], 256)], b.kvr.at[s, mine[s], head[s]]))
    for c in range(32):
        at = slice(c * 128, (c + 1) * 128)
        b.norm_t[0, at, :] = b.normed[:, at].T

    first = {}
    last = [[], []]
    swapped = {}

    def spread(s, of, half):
        f = (flip1, flip3)[half]
        block = b.kvr.at[s, ring[s] * 2 + (xh if of == 0 else 1 - xh), 2 * half : 2 * half + 2]
        first[s, of, half] = net.start(block, block, across(s, f(ring[s])))

    def spread_on(s, of):
        for half, f, g in ((0, flip1, flip3), (1, flip3, flip1)):
            first[s, of, half].wait_recv()
            for value in (ring[s], f(ring[s])):
                slot = value * 2 + (xh if of == 0 else 1 - xh)
                block = b.kvr.at[s, slot, 2 * half : 2 * half + 2]
                last[s].append(net.start(block, block, across(s, g(ring[s]))))

    def gather_own(s):
        for copy in kv_in[s]:
            arrived(copy)
        for half in range(2):
            block = b.kvr.at[s, mine[s], 2 * half : 2 * half + 2]
            swapped[s, half] = net.start(block, block, here.at(x=x2))
        for half in range(2):
            spread(s, 0, half)

    def gather_swapped(s):
        for half in range(2):
            swapped[s, half].wait_recv()
            spread(s, 1, half)

    gather_own(0)
    send_rows(0, do, b.dr)
    offset = lax.broadcasted_iota(jnp.int32, (32, 128), 0)
    for i in range(64):
        m, w, n, half = i // 16, (i // 8) % 2, (i // 2) % 4, i % 2
        for s in range(2):
            zz, yy = (n, m) if s == 0 else (m, n)
            span = spans[((zz * 4 + yy) * 2 + w) * 2 + half]
            b.key_pos[s, i * 32 : (i + 1) * 32, :] = offset + span * 32
    spread_on(0, 0)
    gather_own(1)
    gather_swapped(0)
    spread_on(0, 1)
    send_rows(1, q, b.qr)
    send_rows(1, do, b.dr)
    norm_in = net.start(b.norm_t.at[0], b.norm_t.at[1], twin)

    scale = HEAD_DIM ** (-0.5)
    to_two = scale * math.log2(math.e)
    slots_of = [slice(c * CHUNK, (c + 1) * CHUNK) for c in range(KEYS // CHUNK)]
    returned = []

    def keys_of(s, c):
        return b.kvr[s, c, :, :, :128].reshape(CHUNK, 128)

    def values_of(s, c):
        return b.kvr[s, c, :, :, 128:].reshape(CHUNK, 128)

    def ready(s):
        for copy in last[s]:
            copy.wait_recv()
        for copy in rows_in[s]:
            arrived(copy)
        for c, rows in enumerate(slots_of):
            b.key_t[:, rows] = keys_of(s, c).T
            b.value_t[:, rows] = values_of(s, c).T

    def stack(ref, s, block):
        both = ref[s, block]
        return jnp.concatenate([both[:, h * 128 : (h + 1) * 128] for h in range(4)], axis=0)

    def side(k):
        return 1 - xh if k == 0 else xh

    def block_of(s, order):
        return (flip1, flip3, flip2, lambda a: a)[order](head[s])

    def give_back(s, order, src, dst):
        block = block_of(s, order)
        dst = dst.at[s, :, cols(head[s], 512)]
        if order < 3:
            returned.append(net.start(src.at[s, block], dst, along(s, block)))
        else:
            returned.append(keep(src.at[s, block], dst))

    def attention(s, order):
        block = block_of(s, order)
        score, prob = b.score.at[order], b.prob.at[order]
        queries = stack(b.qr, s, block)
        grads = stack(b.dr, s, block)
        q_t = queries.T
        do_t = grads.T
        b.query_s[order] = queries
        b.grad_s[order] = grads
        b.grad_t[order] = do_t
        start = (block * 4 + y) * 4 + xh * 2 if s == 0 else (z * 4 + block) * 4 + xh * 2
        column = lax.broadcasted_iota(jnp.int32, (1, 256), 1)
        q_pos = column % 32 + 32 * jnp.where(column % 64 < 32, spans[start], spans[start + 1])
        top = jnp.full((8, 256), -1e30, F32)
        for c, rows in enumerate(slots_of):
            t = jnp.dot(keys_of(s, c), q_t, preferred_element_type=F32)
            k_pos = b.key_pos[s, rows, :]
            k_pos = jnp.concatenate([k_pos, k_pos], axis=1)
            t = jnp.where(k_pos <= q_pos, t, -1e30)
            score[rows, :] = t
            top = jnp.maximum(top, jnp.max(t.reshape(CHUNK // 8, 8, 256), axis=0))
        top = jnp.max(top, axis=0, keepdims=True)
        total = jnp.zeros((8, 256), F32)
        for rows in slots_of:
            e = jnp.exp2((score[rows, :] - top) * to_two)
            score[rows, :] = e
            total = total + jnp.sum(e.reshape(CHUNK // 8, 8, 256), axis=0)
        inverse = 1.0 / jnp.sum(total, axis=0, keepdims=True)
        out_t = jnp.zeros((128, 256), F32)
        for rows in slots_of:
            p = (score[rows, :] * inverse).astype(BF)
            prob[rows, :] = p
            out_t = out_t + jnp.dot(b.value_t[:, rows], p, preferred_element_type=F32)
        out_t = out_t.astype(BF)
        delta = jnp.sum(out_t.astype(F32) * do_t.astype(F32), axis=0, keepdims=True)
        b.stats[order, 0] = jnp.broadcast_to(inverse, (8, 256))
        b.stats[order, 1] = jnp.broadcast_to(delta, (8, 256))
        attended = out_t.T
        for h in range(4):
            b.att[s, block, :, h * 128 : (h + 1) * 128] = attended[h * 64 : (h + 1) * 64]
        give_back(s, order, b.att, att_out)

    def gradients(s, k):
        for c in range(4):
            slot = c * 2 + side(k)
            rows = pl.ds(pl.multiple_of(slot * CHUNK, CHUNK), CHUNK)
            values = values_of(s, slot)
            keys = b.key_t[:, rows]
            k_term = jnp.zeros((CHUNK, 128), F32)
            v_term = jnp.zeros((CHUNK, 128), F32)
            for order in range(4):
                inverse, delta = b.stats[order, 0, :1], b.stats[order, 1, :1]
                dp = jnp.dot(values, b.grad_t[order], preferred_element_type=F32)
                ds = (b.score[order, rows, :] * inverse * (dp - delta)).astype(BF)
                k_term = k_term + jnp.dot(ds, b.query_s[order], preferred_element_type=F32)
                v_term = v_term + jnp.dot(
                    b.prob[order, rows, :], b.grad_s[order], preferred_element_type=F32
                )
                dq = jnp.dot(keys, ds, preferred_element_type=F32)
                if k == 0 and c == 0:
                    b.dq_t[order] = dq
                else:
                    b.dq_t[order] += dq
            b.term[s, slot, :, :, :128] = (k_term * scale).astype(BF).reshape(4, 64, 128)
            b.term[s, slot, :, :, 128:] = v_term.astype(BF).reshape(4, 64, 128)

    def give_query_grads(s):
        for order in range(4):
            dq = (b.dq_t[order] * scale).astype(BF).T
            for h in range(4):
                b.dq[s, block_of(s, order), :, h * 128 : (h + 1) * 128] = dq[h * 64 : (h + 1) * 64]
            give_back(s, order, b.dq, dq_out)

    flips = ((flip3, flip1), (flip1, flip3))
    one, two, three, owners = {}, {}, {}, [[], []]

    def half_of(half):
        return slice(2 * half, 2 * half + 2)

    def sum_one(s, k):
        for j in (1, 0):
            for half in range(2):
                f, g = flips[half]
                target = f(ring[s])
                slot = target if j == 0 else g(target)
                one[s, half, j, k] = net.start(
                    b.term.at[s, slot * 2 + side(k), half_of(half)],
                    b.got1.at[s, half, j, k],
                    across(s, target),
                )

    def sum_two(s, k):
        for half in range(2):
            f, g = flips[half]
            one[s, half, 1, k].wait_recv()
            b.sum1[s, half, k] = (
                b.term[s, g(ring[s]) * 2 + side(k), half_of(half)].astype(F32)
                + b.got1[s, half, 1, k].astype(F32)
            ).astype(BF)
            two[s, half, k] = net.start(
                b.sum1.at[s, half, k], b.got2.at[s, half, k], across(s, g(ring[s]))
            )

    def summed(s, half, k):
        one[s, half, 0, k].wait_recv()
        two[s, half, k].wait_recv()
        return (
            b.term[s, ring[s] * 2 + side(k), half_of(half)].astype(F32)
            + b.got1[s, half, 0, k].astype(F32)
            + b.got2[s, half, k].astype(F32)
        )

    def sum_three(s):
        for half in range(2):
            at = half_of(half)
            b.part[s, at] = summed(s, half, 0).astype(BF)
            three[s, half] = net.start(b.part.at[s, at], b.got3.at[s, at], here.at(x=x2))

    def sum_four(s):
        for half in range(2):
            at = half_of(half)
            total = summed(s, half, 1)
            three[s, half].wait_recv()
            b.final[s, at] = (total + b.got3[s, at].astype(F32)).astype(BF)
        for f in (flip2, flip1, flip3):
            to = f(head[s])
            owners[s].append(
                net.start(b.final.at[s, to], b.whole.at[s, head[s]], along(s, to))
            )
        b.whole[s, head[s]] = b.final[s, head[s]]

    def rotate_rows(s):
        for copy in owners[s]:
            copy.wait_recv()
        rows = slice(s * 64, (s + 1) * 64)
        for h in range(KV_HEADS):
            at = slice(h * 128, (h + 1) * 128)
            u = b.whole[s, h, :, :128].astype(F32)
            b.grads[0, rows, at] = (
                u * both_cos[:64] - pltpu.roll(u, 64, 1) * both_sin[:64]
            ).astype(BF)
            b.grads[1, rows, at] = b.whole[s, h, :, 128:]

    spread_on(1, 0)
    ready(0)
    attention(0, 0)
    gather_swapped(1)
    attention(0, 1)
    attention(0, 2)
    spread_on(1, 1)
    attention(0, 3)
    gradients(0, 0)
    sum_one(0, 0)
    gradients(0, 1)
    sum_one(0, 1)
    give_query_grads(0)
    ready(1)
    attention(1, 0)
    attention(1, 1)
    sum_two(0, 0)
    attention(1, 2)
    sum_two(0, 1)
    attention(1, 3)
    sum_three(0)
    gradients(1, 0)
    sum_one(1, 0)
    sum_four(0)
    gradients(1, 1)
    sum_two(1, 0)
    sum_one(1, 1)
    give_query_grads(1)
    rotate_rows(0)
    sum_three(1)
    sum_two(1, 1)
    sum_four(1)
    rotate_rows(1)

    swap_grad = net.start(b.grads.at[1 - here.core], b.got_grad, twin)
    norm_in.wait_recv()
    swap_grad.wait_recv()
    pair = jnp.concatenate([b.grads[here.core], b.got_grad[...]], axis=0)

    @pl.loop(0, 16, unroll=4)
    def _(i):
        at = pl.ds(pl.multiple_of(i * 256, 256), 256)
        n = jnp.concatenate([b.norm_t[0, at, :], b.norm_t[1, at, :]], axis=1)
        w = jnp.dot(n, pair, preferred_element_type=F32).astype(BF)
        for x in range(4):
            for u in range(4):
                row = x * 64 + u * 16
                b.big[u, i // 4, i % 4, x] = w[row : row + 16]

    def backward_rows():
        key_grad, value_grad = b.grads[0], b.grads[1]
        nt = (((1,), (1,)), ((), ()))
        inner = jnp.zeros((128, 128), F32)
        for c in range(16):
            at = slice(c * 256, (c + 1) * 256)
            ng = lax.dot_general(key_grad, b.kw[at, :], nt, preferred_element_type=F32)
            ng = ng + lax.dot_general(value_grad, b.vw[at, :], nt, preferred_element_type=F32)
            t = tokens[:, at].astype(F32)
            b.wide_grad[:, at] = ng
            across_rows = jnp.sum(ng * t * rms, axis=0, keepdims=True)
            weighted = ng * norm_gain[:, at] * t
            inner = inner + weighted[:, :128] + weighted[:, 128:]
            for k in range(2):
                row = c * 2 + k
                b.gain[row // 8, row % 8 : row % 8 + 1, :] = across_rows[:, k * 128 : (k + 1) * 128]
        mean = jnp.sum(inner, axis=1, keepdims=True) / 4096.0
        cube = rms**3 * mean
        for c in range(16):
            at = slice(c * 256, (c + 1) * 256)
            b.grad_rows[:, at] = (
                rms * norm_gain[:, at] * b.wide_grad[:, at] - tokens[:, at].astype(F32) * cube
            ).astype(BF)

    def device(axis, value):
        return here.at(**{axis: value})

    plans = []
    for u, lo, width, order, up in PARTS:
        f, f2 = (flip1, flip3) if up else (flip3, flip1)
        a0, a1, a2 = order
        left = [a for a in "zyx" if a != a0]
        plans.append((u, pl.ds(lo, width), f, f2, a0, a1, a2, left.index(a1) == 0))

    def slab(u, axis, value, lanes):
        if axis == "z":
            return b.big.at[u, value, :, :, :, lanes]
        if axis == "y":
            return b.big.at[u, :, value, :, :, lanes]
        return b.big.at[u, :, :, value, :, lanes]

    def slab1(u, value, lanes, leading):
        return b.s1.at[u, value, :, :, lanes] if leading else b.s1.at[u, :, value, :, lanes]

    def wide(ref):
        return ref[...].astype(F32)

    gains = []

    def gain_step(step):
        if step == 0:
            tiles = [b.gain.at[f(z)] for f in turns]
            own = None
        else:
            own = b.gain[z] if step == 1 else b.gain_sum[step - 2]
            for k in range(3):
                gains[k].wait_recv()
                own = own + b.gain_got[3 * (step - 1) + k]
            del gains[:]
            b.gain_sum[step - 1] = own
            tiles = [b.gain_sum.at[step - 1]] * 3
        if step < 3:
            axis = "zyx"[step]
            for k, f in enumerate(turns):
                gains.append(
                    net.start(tiles[k], b.gain_got.at[3 * step + k], device(axis, f(place[axis])))
                )
        else:
            gains.append(net.start(tiles[0], b.gain_got.at[9], twin))

    waits = {}
    for j in (1, 0):
        for p, (u, lanes, f, f2, a0, a1, a2, leading) in enumerate(plans):
            m0 = place[a0]
            slot = flip2(m0) if j == 1 else f(m0)
            waits[p, 0, j] = net.start(
                slab(u, a0, slot, lanes), b.r0.at[u, j, :, :, :, lanes], device(a0, f(m0))
            )
    backward_rows()
    keep_rows = keep(b.grad_rows, rows_out)
    gain_step(0)
    for p, (u, lanes, f, f2, a0, a1, a2, leading) in enumerate(plans):
        m0 = place[a0]
        waits[p, 0, 1].wait_recv()
        b.s0[u, :, :, :, lanes] = (
            wide(slab(u, a0, f2(m0), lanes)) + b.r0[u, 1, :, :, :, lanes].astype(F32)
        ).astype(BF)
        waits[p, 1] = net.start(
            b.s0.at[u, :, :, :, lanes], b.r1.at[u, :, :, :, lanes], device(a0, f2(m0))
        )
    gain_step(1)
    for p, (u, lanes, f, f2, a0, a1, a2, leading) in enumerate(plans):
        m0, m1 = place[a0], place[a1]
        waits[p, 0, 0].wait_recv()
        waits[p, 1].wait_recv()
        b.s1[u, :, :, :, lanes] = (
            wide(slab(u, a0, m0, lanes))
            + b.r0[u, 0, :, :, :, lanes].astype(F32)
            + b.r1[u, :, :, :, lanes].astype(F32)
        ).astype(BF)
        for k, turn in enumerate(turns):
            waits[p, 2, k] = net.start(
                slab1(u, turn(m1), lanes, leading),
                b.r2.at[u, k, :, :, lanes],
                device(a1, turn(m1)),
            )
    gain_step(2)
    for p, (u, lanes, f, f2, a0, a1, a2, leading) in enumerate(plans):
        m1, m2 = place[a1], place[a2]
        total = wide(slab1(u, m1, lanes, leading))
        for k in range(3):
            waits[p, 2, k].wait_recv()
            total = total + b.r2[u, k, :, :, lanes].astype(F32)
        b.s3[u, :, :, lanes] = total.astype(BF)
        for k, turn in enumerate(turns):
            waits[p, 3, k] = net.start(
                b.s3.at[u, turn(m2), :, lanes], b.r4.at[u, k, :, lanes], device(a2, turn(m2))
            )
    gain_step(3)
    for p, (u, lanes, f, f2, a0, a1, a2, leading) in enumerate(plans):
        total = b.s3[u, place[a2], :, lanes].astype(F32)
        for k in range(3):
            waits[p, 3, k].wait_recv()
            total = total + b.r4[u, k, :, lanes].astype(F32)
        b.full[u // 2, u % 2, :, lanes] = total
    swap = net.start(b.full.at[1 - here.core], out.at[here.core], twin)
    out[here.core] = b.full[here.core]
    gains[0].wait_recv()
    gain_out[...] = b.gain_sum[2] + b.gain_got[9]
    swap.wait_recv()
    for copy in returned:
        arrived(copy)
    keep_rows.wait()
    net.finish()


def layer(spans, q, do, tokens, norm_gain, key_w, value_w, cos, sin):
    vm = pl.BlockSpec(memory_space=VM)
    any_ = pl.BlockSpec(memory_space=pl.ANY)
    return pl.pallas_call(
        layer_kernel,
        name="layer",
        out_shape=(
            jax.ShapeDtypeStruct((2, 64, 2048), BF),
            jax.ShapeDtypeStruct((2, 64, 2048), BF),
            jax.ShapeDtypeStruct((128, 4096), BF),
            jax.ShapeDtypeStruct((2, 2, 16, 512), F32),
            jax.ShapeDtypeStruct((8, 128), F32),
        ),
        in_specs=[pl.BlockSpec(memory_space=pltpu.SMEM), any_, any_, any_, vm, any_, any_, vm, vm],
        out_specs=(any_,) * 3 + (vm,) * 2,
        scratch_shapes=[VM(*shape) for shape in SHAPES.values()]
        + [
            pltpu.SemaphoreType.DMA((N_COPIES,)),
            pltpu.SemaphoreType.DMA((N_COPIES,)),
            pltpu.SemaphoreType.DMA((12,)),
            pltpu.SemaphoreType.DMA((2 * PIECES + 1,)),
        ],
        compiler_params=pltpu.CompilerParams(
            collective_id=1, has_side_effects=True, vmem_limit_bytes=60 * 1024 * 1024
        ),
    )(spans, q, do, tokens, norm_gain, key_w, value_w, cos, sin)


def finish_kernel(
    att, dq, rows, weights, gain, att_to, dq_to, rows_to, keys_to, values_to, gain_to,
    att_v, dq_v, rows_v, weights_v, gain_v, sems,
):
    here = Here()
    loads = []
    for k, (src, dst) in enumerate(
        ((gain, gain_v), (att, att_v), (dq, dq_v), (rows, rows_v), (weights, weights_v))
    ):
        copy = pltpu.make_async_copy(src, dst, sems.at[k])
        copy.start()
        loads.append(copy)
    loads[0].wait()
    row = gain_v[pl.ds(here.y * 2 + here.xh, 1), :]
    dp = here.xl * 2 + here.core
    gain_to[...] = pltpu.roll(row, (128 - dp * 32) % 128, 1)[:, :32]
    stores = []
    for k, (load, src, dst) in enumerate(
        (
            (loads[1], att_v, att_to),
            (loads[2], dq_v, dq_to),
            (loads[3], rows_v, rows_to),
            (loads[4], weights_v.at[0], keys_to),
            (None, weights_v.at[1], values_to),
        )
    ):
        if load is not None:
            load.wait()
        copy = pltpu.make_async_copy(src, dst, sems.at[5 + k])
        copy.start()
        stores.append(copy)
    for copy in stores:
        copy.wait()


def finish(att, dq, rows, weights, gain):
    any_ = pl.BlockSpec(memory_space=pl.ANY)
    return pl.pallas_call(
        finish_kernel,
        name="finish",
        out_shape=(
            jax.ShapeDtypeStruct((2, 64, 2048), BF),
            jax.ShapeDtypeStruct((2, 64, 2048), BF),
            jax.ShapeDtypeStruct((128, 4096), BF),
            jax.ShapeDtypeStruct((32, 512), F32),
            jax.ShapeDtypeStruct((32, 512), F32),
            jax.ShapeDtypeStruct((1, 32), F32),
        ),
        in_specs=[any_] * 5,
        out_specs=(any_,) * 5 + (pl.BlockSpec(memory_space=VM),),
        scratch_shapes=[
            VM((2, 64, 2048), BF),
            VM((2, 64, 2048), BF),
            VM((128, 4096), BF),
            VM((2, 32, 512), F32),
            VM((8, 128), F32),
            pltpu.SemaphoreType.DMA((10,)),
        ],
        compiler_params=pltpu.CompilerParams(vmem_limit_bytes=60 * 1024 * 1024),
    )(att, dq, rows, weights, gain)


def body(tokens, queries, d_attended, span_order, norm_gain, key_weight, value_weight):
    seqs, rows, width = tokens.shape
    count = seqs * rows
    half_dim = HEAD_DIM // 2
    span_len = rows // 2
    own_spans = lax.dynamic_slice_in_dim(span_order, lax.axis_index("ctx") * 2, 2, 0)
    own_pos = (own_spans[:, None] * span_len + jnp.arange(span_len, dtype=jnp.int32)).reshape(-1)
    frequency = ROPE_BASE ** (-2.0 * jnp.arange(half_dim, dtype=F32) / HEAD_DIM)
    angles = own_pos.astype(F32)[:, None] * frequency[None, :]
    attended, grad_queries, grad_rows, weights, gain = layer(
        span_order, queries, d_attended, tokens.reshape(count, width), norm_gain.reshape(1, width),
        key_weight, value_weight, jnp.cos(angles), jnp.sin(angles),
    )
    attended, grad_queries, grad_rows, grad_keys, grad_values, gain = finish(
        attended, grad_queries, grad_rows, weights.reshape(2, 32, 512), gain
    )
    return (
        attended,
        grad_queries,
        grad_rows.reshape(seqs, rows, width),
        grad_keys,
        grad_values,
        gain.reshape(32),
    )


def solution(mesh):
    placed = (P("dp", "ctx", None), P("dp", "ctx", None), P("dp", "ctx", None), P(), P(), P(), P())
    return jax.shard_map(
        body,
        mesh=mesh,
        in_specs=placed,
        out_specs=(
            P("dp", "ctx", None),
            P("dp", "ctx", None),
            P("dp", "ctx", None),
            P(("ctx", "dp"), None),
            P(("ctx", "dp"), None),
            P(("ctx", "dp")),
        ),
        check_vma=False,
    )
```

```python
import functools
import math

import jax
import jax.numpy as jnp
from jax import lax
from jax.experimental import pallas as pl
from jax.experimental.pallas import tpu as pltpu
from jax.sharding import PartitionSpec as P

KV_HEADS = 4
HEAD_DIM = 128
ROPE_BASE = 500000.0
EPSILON = 1e-05
BF = jnp.bfloat16
F32 = jnp.float32
VM = pltpu.VMEM
MESH = pl.DeviceIdType.MESH


def flip1(a):
    return a + 1 - 2 * (a % 2)


def flip3(a):
    return 3 - a


def flip2(a):
    return (a + 2) % 4


class Here:
    def __init__(self):
        ctx = lax.axis_index("ctx")
        dp = lax.axis_index("dp")
        self.z = ctx // 8
        self.y = (ctx // 2) % 4
        self.xh = ctx % 2
        self.xl = dp // 2
        self.core = dp % 2
        self.x = self.xh * 2 + self.xl

    def at(self, z=None, y=None, x=None, core=None):
        z = self.z if z is None else z
        y = self.y if y is None else y
        core = self.core if core is None else core
        if x is None:
            xh, xl = self.xh, self.xl
        else:
            xh, xl = x // 2, x % 2
        return {"ctx": z * 8 + y * 2 + xh, "dp": xl * 2 + core}


class Net:
    def __init__(self, send_sems, recv_sems):
        self.send_sems = send_sems
        self.recv_sems = recv_sems
        self.made = []

    def start(self, src, dst, device):
        k = len(self.made)
        copy = pltpu.make_async_remote_copy(
            src_ref=src,
            dst_ref=dst,
            send_sem=self.send_sems.at[k],
            recv_sem=self.recv_sems.at[k],
            device_id=device,
            device_id_type=MESH,
        )
        copy.start()
        self.made.append(copy)
        return copy

    def finish(self):
        for copy in self.made:
            copy.wait_send()


def greet(devices):
    barrier = pltpu.get_barrier_semaphore()
    for device in devices:
        pl.semaphore_signal(barrier, inc=1, device_id=device, device_id_type=MESH)
    pl.semaphore_wait(barrier, len(devices))


def cols(index, width):
    return pl.ds(pl.multiple_of(index * width, width), width)


KEYS = 2048
CHUNK = 256
PIECES = 8
PARTS = (
    (0, 0, 128, "zyx", True),
    (1, 0, 128, "yxz", True),
    (2, 0, 256, "xzy", True),
    (0, 128, 384, "zyx", False),
    (1, 128, 384, "yxz", False),
    (2, 256, 256, "xzy", False),
    (3, 0, 256, "zyx", True),
    (3, 256, 256, "yxz", True),
)
N_COPIES = 41 + 34 + 1 + 9 * len(PARTS) + 10 + 1
SHAPES = dict(
    tokens=((128, 4096), BF),
    kw=((4096, 512), BF),
    vw=((4096, 512), BF),
    normed=((128, 4096), BF),
    acc=((2, 128, 512), F32),
    kv=((2, 64, 1024), BF),
    norm_t=((2, 4096, 128), BF),
    qr=((2, 4, 64, 512), BF),
    dr=((2, 4, 64, 512), BF),
    kvr=((2, 8, 4, 64, 256), BF),
    key_pos=((2, KEYS, 128), jnp.int32),
    score=((4, KEYS, 256), F32),
    prob=((4, KEYS, 256), BF),
    query_s=((4, 256, 128), BF),
    grad_s=((4, 256, 128), BF),
    grad_t=((4, 128, 256), BF),
    stats=((4, 2, 8, 256), F32),
    dq_t=((4, 128, 256), F32),
    key_t=((128, KEYS), BF),
    value_t=((128, KEYS), BF),
    att=((2, 4, 64, 512), BF),
    dq=((2, 4, 64, 512), BF),
    term=((2, 8, 4, 64, 256), BF),
    got1=((2, 3, 2, 4, 64, 256), BF),
    part=((2, 4, 64, 256), BF),
    got3=((2, 4, 64, 256), BF),
    final=((2, 4, 64, 256), BF),
    whole=((2, 4, 64, 256), BF),
    grads=((2, 128, 512), BF),
    got_grad=((128, 512), BF),
    big=((4, 4, 4, 4, 16, 512), BF),
    wide_grad=((128, 4096), F32),
    grad_rows=((128, 4096), BF),
    gain=((4, 8, 128), F32),
    r0=((4, 2, 4, 4, 16, 512), BF),
    s0=((4, 4, 4, 16, 512), BF),
    r1=((4, 4, 4, 16, 512), BF),
    s1=((4, 4, 4, 16, 512), BF),
    r2=((4, 3, 4, 16, 512), BF),
    s3=((4, 4, 16, 512), BF),
    r4=((4, 3, 16, 512), BF),
    full=((2, 2, 16, 512), F32),
    gain_got=((10, 8, 128), F32),
    gain_sum=((3, 8, 128), F32),
)


class Box:
    pass


def layer_kernel(
    spans, q, do, tokens_in, norm_gain, key_w, value_w, cos, sin,
    att_out, dq_out, rows_out, out, gain_out, *scratch,
):
    b = Box()
    for name, ref in zip(SHAPES, scratch):
        setattr(b, name, ref)
    send_sems, recv_sems, local_sems, weight_sems = scratch[len(SHAPES) :]
    tokens = b.tokens
    token_load = pltpu.make_async_copy(tokens_in, tokens, weight_sems.at[2 * PIECES])
    token_load.start()
    here = Here()
    place = {"z": here.z, "y": here.y, "x": here.x}
    z, y, xh = here.z, here.y, here.xh
    x2 = flip2(here.x)
    twin = here.at(core=1 - here.core)
    turns = (flip1, flip3, flip2)
    piece = 4096 // PIECES
    loads = []
    for c in range(PIECES):
        for w, (src, dst) in enumerate(((key_w, b.kw), (value_w, b.vw))):
            at = pl.ds(c * piece, piece)
            copy = pltpu.make_async_copy(src.at[at], dst.at[at], weight_sems.at[2 * c + w])
            copy.start()
            loads.append(copy)
    greet([here.at(**{a: f(place[a])}) for a in "zyx" for f in turns] + [twin])
    net = Net(send_sems, recv_sems)

    seq = [here.core, 1 - here.core]

    def either(s, a, b):
        return a * (1 - seq[s]) + b * seq[s]

    def along(s, value):
        return here.at(z=either(s, value, z), y=either(s, y, value))

    def across(s, value):
        return here.at(z=either(s, z, value), y=either(s, value, y))

    head = [either(s, z, y) for s in range(2)]
    ring = [either(s, y, z) for s in range(2)]
    mine = [ring[s] * 2 + xh for s in range(2)]
    local = []

    def keep(src, dst):
        copy = pltpu.make_async_copy(src, dst, local_sems.at[len(local)])
        copy.start()
        local.append(copy)
        return copy

    rows_in = [[], []]

    def send_rows(s, src, dst):
        for f in turns:
            to = f(head[s])
            rows_in[s].append(
                net.start(src.at[seq[s], :, cols(to, 512)], dst.at[s, head[s]], along(s, to))
            )
        rows_in[s].append(keep(src.at[seq[s], :, cols(head[s], 512)], dst.at[s, head[s]]))

    def arrived(copy):
        if any(copy is c for c in local):
            copy.wait()
        else:
            copy.wait_recv()

    send_rows(0, q, b.qr)
    token_load.wait()
    squares = jnp.zeros((128, 128), F32)
    for c in range(32):
        t = tokens[:, c * 128 : (c + 1) * 128].astype(F32)
        squares = squares + t * t
    rms = lax.rsqrt(jnp.sum(squares, axis=1, keepdims=True) / 4096.0 + EPSILON)
    for c in range(PIECES):
        at = slice(c * piece, (c + 1) * piece)
        b.normed[:, at] = (tokens[:, at].astype(F32) * rms * norm_gain[:, at]).astype(BF)
    for c in range(PIECES):
        at = slice(c * piece, (c + 1) * piece)
        n = b.normed[:, at]
        for w, ref in enumerate((b.kw, b.vw)):
            loads[2 * c + w].wait()
            product = jnp.dot(n, ref[at, :], preferred_element_type=F32)
            if c == 0:
                b.acc[w] = product
            else:
                b.acc[w] += product

    def widen(half):
        both = jnp.concatenate([half, half], axis=1)
        return jnp.concatenate([both, both], axis=0)

    lane = lax.broadcasted_iota(jnp.int32, (128, 128), 1)
    both_cos = widen(cos[...])
    both_sin = widen(sin[...])
    both_sin = jnp.where(lane < 64, -both_sin, both_sin)
    for h in range(KV_HEADS):
        at = slice(h * 128, (h + 1) * 128)
        u = b.acc[0, :, at]
        k = (u * both_cos + pltpu.roll(u, 64, 1) * both_sin).astype(BF)
        v = b.acc[1, :, at].astype(BF)
        for s in range(2):
            b.kv[s, :, h * 256 : h * 256 + 128] = k[s * 64 : (s + 1) * 64]
            b.kv[s, :, h * 256 + 128 : (h + 1) * 256] = v[s * 64 : (s + 1) * 64]

    kv_in = [[], []]
    for s in range(2):
        for f in (flip2, flip1, flip3):
            to = f(head[s])
            kv_in[s].append(
                net.start(
                    b.kv.at[seq[s], :, cols(to, 256)], b.kvr.at[s, mine[s], head[s]], along(s, to)
                )
            )
        own = b.kv.at[seq[s], :, cols(head[s], 256)]
        kv_in[s].append(keep(own, b.kvr.at[s, mine[s], head[s]]))
    for c in range(32):
        at = slice(c * 128, (c + 1) * 128)
        b.norm_t[0, at, :] = b.normed[:, at].T

    last = [[], []]
    swapped = {}

    def half_of(half):
        return slice(2 * half, 2 * half + 2)

    def spread(s, of, rows):
        block = b.kvr.at[s, ring[s] * 2 + (xh if of == 0 else 1 - xh), rows]
        for f in (flip2, flip1, flip3):
            last[s].append(net.start(block, block, across(s, f(ring[s]))))

    def gather_own(s):
        for copy in kv_in[s]:
            arrived(copy)
        for half in range(2):
            block = b.kvr.at[s, mine[s], half_of(half)]
            swapped[s, half] = net.start(block, block, here.at(x=x2))
        spread(s, 0, slice(0, 4))

    def gather_swapped(s):
        for half in range(2):
            swapped[s, half].wait_recv()
            spread(s, 1, half_of(half))

    gather_own(0)
    send_rows(0, do, b.dr)
    offset = lax.broadcasted_iota(jnp.int32, (32, 128), 0)
    for i in range(64):
        m, w, n, half = i // 16, (i // 8) % 2, (i // 2) % 4, i % 2
        for s in range(2):
            at_z, at_y = ((n * 4 + m) * 2 + w) * 2 + half, ((m * 4 + n) * 2 + w) * 2 + half
            span = spans[either(s, at_z, at_y)]
            b.key_pos[s, i * 32 : (i + 1) * 32, :] = offset + span * 32
    gather_swapped(0)
    gather_own(1)
    send_rows(1, q, b.qr)
    send_rows(1, do, b.dr)
    norm_in = net.start(b.norm_t.at[0], b.norm_t.at[1], twin)

    scale = HEAD_DIM ** (-0.5)
    to_two = scale * math.log2(math.e)
    slots_of = [slice(c * CHUNK, (c + 1) * CHUNK) for c in range(KEYS // CHUNK)]
    returned = []

    def keys_of(s, c):
        return b.kvr[s, c, :, :, :128].reshape(CHUNK, 128)

    def values_of(s, c):
        return b.kvr[s, c, :, :, 128:].reshape(CHUNK, 128)

    def ready(s):
        for copy in last[s]:
            copy.wait_recv()
        for copy in rows_in[s]:
            arrived(copy)
        for c, rows in enumerate(slots_of):
            b.key_t[:, rows] = keys_of(s, c).T
            b.value_t[:, rows] = values_of(s, c).T

    def stack(ref, s, block):
        both = ref[s, block]
        return jnp.concatenate([both[:, h * 128 : (h + 1) * 128] for h in range(4)], axis=0)

    def side(k):
        return 1 - xh if k == 0 else xh

    def block_of(s, order):
        return (flip1, flip3, flip2, lambda a: a)[order](head[s])

    def give_back(s, order, src, dst):
        block = block_of(s, order)
        dst = dst.at[seq[s], :, cols(head[s], 512)]
        if order < 3:
            returned.append(net.start(src.at[s, block], dst, along(s, block)))
        else:
            returned.append(keep(src.at[s, block], dst))

    def attention(s, order):
        block = block_of(s, order)
        score, prob = b.score.at[order], b.prob.at[order]
        queries = stack(b.qr, s, block)
        grads = stack(b.dr, s, block)
        q_t = queries.T
        do_t = grads.T
        b.query_s[order] = queries
        b.grad_s[order] = grads
        b.grad_t[order] = do_t
        start = either(s, (block * 4 + y) * 4, (z * 4 + block) * 4) + xh * 2
        column = lax.broadcasted_iota(jnp.int32, (1, 256), 1)
        q_pos = column % 32 + 32 * jnp.where(column % 64 < 32, spans[start], spans[start + 1])
        top = jnp.full((8, 256), -1e30, F32)
        for c, rows in enumerate(slots_of):
            t = jnp.dot(keys_of(s, c), q_t, preferred_element_type=F32)
            k_pos = b.key_pos[s, rows, :]
            k_pos = jnp.concatenate([k_pos, k_pos], axis=1)
            t = jnp.where(k_pos <= q_pos, t, -1e30)
            score[rows, :] = t
            top = jnp.maximum(top, jnp.max(t.reshape(CHUNK // 8, 8, 256), axis=0))
        top = jnp.max(top, axis=0, keepdims=True)
        total = jnp.zeros((8, 256), F32)
        for rows in slots_of:
            e = jnp.exp2((score[rows, :] - top) * to_two)
            score[rows, :] = e
            total = total + jnp.sum(e.reshape(CHUNK // 8, 8, 256), axis=0)
        inverse = 1.0 / jnp.sum(total, axis=0, keepdims=True)
        out_t = jnp.zeros((128, 256), F32)
        for rows in slots_of:
            p = (score[rows, :] * inverse).astype(BF)
            prob[rows, :] = p
            out_t = out_t + jnp.dot(b.value_t[:, rows], p, preferred_element_type=F32)
        out_t = out_t.astype(BF)
        delta = jnp.sum(out_t.astype(F32) * do_t.astype(F32), axis=0, keepdims=True)
        b.stats[order, 0] = jnp.broadcast_to(inverse, (8, 256))
        b.stats[order, 1] = jnp.broadcast_to(delta, (8, 256))
        attended = out_t.T
        for h in range(4):
            b.att[s, block, :, h * 128 : (h + 1) * 128] = attended[h * 64 : (h + 1) * 64]
        give_back(s, order, b.att, att_out)

    def gradients(s, k):
        for c in range(4):
            slot = c * 2 + side(k)
            rows = pl.ds(pl.multiple_of(slot * CHUNK, CHUNK), CHUNK)
            values = values_of(s, slot)
            keys = b.key_t[:, rows]
            k_term = jnp.zeros((CHUNK, 128), F32)
            v_term = jnp.zeros((CHUNK, 128), F32)
            for order in range(4):
                inverse, delta = b.stats[order, 0, :1], b.stats[order, 1, :1]
                dp = jnp.dot(values, b.grad_t[order], preferred_element_type=F32)
                ds = (b.score[order, rows, :] * inverse * (dp - delta)).astype(BF)
                k_term = k_term + jnp.dot(ds, b.query_s[order], preferred_element_type=F32)
                v_term = v_term + jnp.dot(
                    b.prob[order, rows, :], b.grad_s[order], preferred_element_type=F32
                )
                dq = jnp.dot(keys, ds, preferred_element_type=F32)
                if k == 0 and c == 0:
                    b.dq_t[order] = dq
                else:
                    b.dq_t[order] += dq
            b.term[s, slot, :, :, :128] = (k_term * scale).astype(BF).reshape(4, 64, 128)
            b.term[s, slot, :, :, 128:] = v_term.astype(BF).reshape(4, 64, 128)

    def give_query_grads(s):
        for order in range(4):
            dq = (b.dq_t[order] * scale).astype(BF).T
            for h in range(4):
                b.dq[s, block_of(s, order), :, h * 128 : (h + 1) * 128] = dq[h * 64 : (h + 1) * 64]
            give_back(s, order, b.dq, dq_out)

    one, three, owners = {}, {}, [[], []]

    def sum_one(s, k):
        for i, f in enumerate((flip2, flip1, flip3)):
            target = f(ring[s])
            one[s, i, k] = net.start(
                b.term.at[s, target * 2 + side(k)], b.got1.at[s, i, k], across(s, target)
            )

    def summed(s, k):
        total = b.term[s, ring[s] * 2 + side(k)].astype(F32)
        for i in range(3):
            one[s, i, k].wait_recv()
            total = total + b.got1[s, i, k].astype(F32)
        return total

    def sum_three(s):
        b.part[s] = summed(s, 0).astype(BF)
        three[s] = net.start(b.part.at[s], b.got3.at[s], here.at(x=x2))

    def sum_four(s):
        total = summed(s, 1)
        three[s].wait_recv()
        b.final[s] = (total + b.got3[s].astype(F32)).astype(BF)
        for f in (flip2, flip1, flip3):
            to = f(head[s])
            owners[s].append(
                net.start(b.final.at[s, to], b.whole.at[s, head[s]], along(s, to))
            )
        b.whole[s, head[s]] = b.final[s, head[s]]

    def rotate_rows(s):
        for copy in owners[s]:
            copy.wait_recv()
        rows = pl.ds(pl.multiple_of(seq[s] * 64, 64), 64)
        for h in range(KV_HEADS):
            at = slice(h * 128, (h + 1) * 128)
            u = b.whole[s, h, :, :128].astype(F32)
            b.grads[0, rows, at] = (
                u * both_cos[:64] - pltpu.roll(u, 64, 1) * both_sin[:64]
            ).astype(BF)
            b.grads[1, rows, at] = b.whole[s, h, :, 128:]

    ready(0)
    attention(0, 0)
    gather_swapped(1)
    attention(0, 1)
    attention(0, 2)
    attention(0, 3)
    gradients(0, 0)
    sum_one(0, 0)
    gradients(0, 1)
    sum_one(0, 1)
    give_query_grads(0)
    ready(1)
    attention(1, 0)
    attention(1, 1)
    attention(1, 2)
    sum_three(0)
    attention(1, 3)
    gradients(1, 0)
    sum_one(1, 0)
    sum_four(0)
    gradients(1, 1)
    sum_one(1, 1)
    sum_three(1)
    give_query_grads(1)
    rotate_rows(0)
    sum_four(1)
    rotate_rows(1)

    swap_grad = net.start(b.grads.at[1 - here.core], b.got_grad, twin)
    norm_in.wait_recv()
    swap_grad.wait_recv()
    pair = jnp.concatenate([b.grads[here.core], b.got_grad[...]], axis=0)

    @pl.loop(0, 16, unroll=4)
    def _(i):
        at = pl.ds(pl.multiple_of(i * 256, 256), 256)
        n = jnp.concatenate([b.norm_t[0, at, :], b.norm_t[1, at, :]], axis=1)
        w = jnp.dot(n, pair, preferred_element_type=F32).astype(BF)
        for x in range(4):
            for u in range(4):
                row = x * 64 + u * 16
                b.big[u, i // 4, i % 4, x] = w[row : row + 16]

    def backward_rows():
        key_grad, value_grad = b.grads[0], b.grads[1]
        nt = (((1,), (1,)), ((), ()))
        inner = jnp.zeros((128, 128), F32)
        for c in range(16):
            at = slice(c * 256, (c + 1) * 256)
            ng = lax.dot_general(key_grad, b.kw[at, :], nt, preferred_element_type=F32)
            ng = ng + lax.dot_general(value_grad, b.vw[at, :], nt, preferred_element_type=F32)
            t = tokens[:, at].astype(F32)
            b.wide_grad[:, at] = ng
            across_rows = jnp.sum(ng * t * rms, axis=0, keepdims=True)
            weighted = ng * norm_gain[:, at] * t
            inner = inner + weighted[:, :128] + weighted[:, 128:]
            for k in range(2):
                row = c * 2 + k
                b.gain[row // 8, row % 8 : row % 8 + 1, :] = across_rows[:, k * 128 : (k + 1) * 128]
        mean = jnp.sum(inner, axis=1, keepdims=True) / 4096.0
        cube = rms**3 * mean
        for c in range(16):
            at = slice(c * 256, (c + 1) * 256)
            b.grad_rows[:, at] = (
                rms * norm_gain[:, at] * b.wide_grad[:, at] - tokens[:, at].astype(F32) * cube
            ).astype(BF)

    def device(axis, value):
        return here.at(**{axis: value})

    plans = []
    for u, lo, width, order, up in PARTS:
        f, f2 = (flip1, flip3) if up else (flip3, flip1)
        a0, a1, a2 = order
        left = [a for a in "zyx" if a != a0]
        plans.append((u, pl.ds(lo, width), f, f2, a0, a1, a2, left.index(a1) == 0))

    def slab(u, axis, value, lanes):
        if axis == "z":
            return b.big.at[u, value, :, :, :, lanes]
        if axis == "y":
            return b.big.at[u, :, value, :, :, lanes]
        return b.big.at[u, :, :, value, :, lanes]

    def slab1(u, value, lanes, leading):
        return b.s1.at[u, value, :, :, lanes] if leading else b.s1.at[u, :, value, :, lanes]

    def wide(ref):
        return ref[...].astype(F32)

    gains = []

    def gain_step(step):
        if step == 0:
            tiles = [b.gain.at[f(z)] for f in turns]
            own = None
        else:
            own = b.gain[z] if step == 1 else b.gain_sum[step - 2]
            for k in range(3):
                gains[k].wait_recv()
                own = own + b.gain_got[3 * (step - 1) + k]
            del gains[:]
            b.gain_sum[step - 1] = own
            tiles = [b.gain_sum.at[step - 1]] * 3
        if step < 3:
            axis = "zyx"[step]
            for k, f in enumerate(turns):
                gains.append(
                    net.start(tiles[k], b.gain_got.at[3 * step + k], device(axis, f(place[axis])))
                )
        else:
            gains.append(net.start(tiles[0], b.gain_got.at[9], twin))

    waits = {}
    for j in (1, 0):
        for p, (u, lanes, f, f2, a0, a1, a2, leading) in enumerate(plans):
            m0 = place[a0]
            slot = flip2(m0) if j == 1 else f(m0)
            waits[p, 0, j] = net.start(
                slab(u, a0, slot, lanes), b.r0.at[u, j, :, :, :, lanes], device(a0, f(m0))
            )
    backward_rows()
    keep_rows = keep(b.grad_rows, rows_out)
    gain_step(0)
    for p, (u, lanes, f, f2, a0, a1, a2, leading) in enumerate(plans):
        m0 = place[a0]
        waits[p, 0, 1].wait_recv()
        b.s0[u, :, :, :, lanes] = (
            wide(slab(u, a0, f2(m0), lanes)) + b.r0[u, 1, :, :, :, lanes].astype(F32)
        ).astype(BF)
        waits[p, 1] = net.start(
            b.s0.at[u, :, :, :, lanes], b.r1.at[u, :, :, :, lanes], device(a0, f2(m0))
        )
    gain_step(1)
    for p, (u, lanes, f, f2, a0, a1, a2, leading) in enumerate(plans):
        m0, m1 = place[a0], place[a1]
        waits[p, 0, 0].wait_recv()
        waits[p, 1].wait_recv()
        b.s1[u, :, :, :, lanes] = (
            wide(slab(u, a0, m0, lanes))
            + b.r0[u, 0, :, :, :, lanes].astype(F32)
            + b.r1[u, :, :, :, lanes].astype(F32)
        ).astype(BF)
        for k, turn in enumerate(turns):
            waits[p, 2, k] = net.start(
                slab1(u, turn(m1), lanes, leading),
                b.r2.at[u, k, :, :, lanes],
                device(a1, turn(m1)),
            )
    gain_step(2)
    for p, (u, lanes, f, f2, a0, a1, a2, leading) in enumerate(plans):
        m1, m2 = place[a1], place[a2]
        total = wide(slab1(u, m1, lanes, leading))
        for k in range(3):
            waits[p, 2, k].wait_recv()
            total = total + b.r2[u, k, :, :, lanes].astype(F32)
        b.s3[u, :, :, lanes] = total.astype(BF)
        for k, turn in enumerate(turns):
            waits[p, 3, k] = net.start(
                b.s3.at[u, turn(m2), :, lanes], b.r4.at[u, k, :, lanes], device(a2, turn(m2))
            )
    gain_step(3)
    for p, (u, lanes, f, f2, a0, a1, a2, leading) in enumerate(plans):
        total = b.s3[u, place[a2], :, lanes].astype(F32)
        for k in range(3):
            waits[p, 3, k].wait_recv()
            total = total + b.r4[u, k, :, lanes].astype(F32)
        b.full[u // 2, u % 2, :, lanes] = total
    swap = net.start(b.full.at[1 - here.core], out.at[here.core], twin)
    out[here.core] = b.full[here.core]
    gains[0].wait_recv()
    gain_out[...] = b.gain_sum[2] + b.gain_got[9]
    swap.wait_recv()
    for copy in returned:
        arrived(copy)
    keep_rows.wait()
    net.finish()


def layer(spans, q, do, tokens, norm_gain, key_w, value_w, cos, sin):
    vm = pl.BlockSpec(memory_space=VM)
    any_ = pl.BlockSpec(memory_space=pl.ANY)
    return pl.pallas_call(
        layer_kernel,
        name="layer",
        out_shape=(
            jax.ShapeDtypeStruct((2, 64, 2048), BF),
            jax.ShapeDtypeStruct((2, 64, 2048), BF),
            jax.ShapeDtypeStruct((128, 4096), BF),
            jax.ShapeDtypeStruct((2, 2, 16, 512), F32),
            jax.ShapeDtypeStruct((8, 128), F32),
        ),
        in_specs=[pl.BlockSpec(memory_space=pltpu.SMEM), any_, any_, any_, vm, any_, any_, vm, vm],
        out_specs=(any_,) * 3 + (vm,) * 2,
        scratch_shapes=[VM(*shape) for shape in SHAPES.values()]
        + [
            pltpu.SemaphoreType.DMA((N_COPIES,)),
            pltpu.SemaphoreType.DMA((N_COPIES,)),
            pltpu.SemaphoreType.DMA((12,)),
            pltpu.SemaphoreType.DMA((2 * PIECES + 1,)),
        ],
        compiler_params=pltpu.CompilerParams(
            collective_id=1, has_side_effects=True, vmem_limit_bytes=60 * 1024 * 1024
        ),
    )(spans, q, do, tokens, norm_gain, key_w, value_w, cos, sin)


def finish_kernel(
    att, dq, rows, weights, gain, att_to, dq_to, rows_to, keys_to, values_to, gain_to,
    att_v, dq_v, rows_v, weights_v, gain_v, sems,
):
    here = Here()
    loads = []
    for k, (src, dst) in enumerate(
        ((gain, gain_v), (att, att_v), (dq, dq_v), (rows, rows_v), (weights, weights_v))
    ):
        copy = pltpu.make_async_copy(src, dst, sems.at[k])
        copy.start()
        loads.append(copy)
    loads[0].wait()
    row = gain_v[pl.ds(here.y * 2 + here.xh, 1), :]
    dp = here.xl * 2 + here.core
    gain_to[...] = pltpu.roll(row, (128 - dp * 32) % 128, 1)[:, :32]
    stores = []
    for k, (load, src, dst) in enumerate(
        (
            (loads[1], att_v, att_to),
            (loads[2], dq_v, dq_to),
            (loads[3], rows_v, rows_to),
            (loads[4], weights_v.at[0], keys_to),
            (None, weights_v.at[1], values_to),
        )
    ):
        if load is not None:
            load.wait()
        copy = pltpu.make_async_copy(src, dst, sems.at[5 + k])
        copy.start()
        stores.append(copy)
    for copy in stores:
        copy.wait()


def finish(att, dq, rows, weights, gain):
    any_ = pl.BlockSpec(memory_space=pl.ANY)
    return pl.pallas_call(
        finish_kernel,
        name="finish",
        out_shape=(
            jax.ShapeDtypeStruct((2, 64, 2048), BF),
            jax.ShapeDtypeStruct((2, 64, 2048), BF),
            jax.ShapeDtypeStruct((128, 4096), BF),
            jax.ShapeDtypeStruct((32, 512), F32),
            jax.ShapeDtypeStruct((32, 512), F32),
            jax.ShapeDtypeStruct((1, 32), F32),
        ),
        in_specs=[any_] * 5,
        out_specs=(any_,) * 5 + (pl.BlockSpec(memory_space=VM),),
        scratch_shapes=[
            VM((2, 64, 2048), BF),
            VM((2, 64, 2048), BF),
            VM((128, 4096), BF),
            VM((2, 32, 512), F32),
            VM((8, 128), F32),
            pltpu.SemaphoreType.DMA((10,)),
        ],
        compiler_params=pltpu.CompilerParams(vmem_limit_bytes=60 * 1024 * 1024),
    )(att, dq, rows, weights, gain)


def body(tokens, queries, d_attended, span_order, norm_gain, key_weight, value_weight):
    seqs, rows, width = tokens.shape
    count = seqs * rows
    half_dim = HEAD_DIM // 2
    span_len = rows // 2
    own_spans = lax.dynamic_slice_in_dim(span_order, lax.axis_index("ctx") * 2, 2, 0)
    own_pos = (own_spans[:, None] * span_len + jnp.arange(span_len, dtype=jnp.int32)).reshape(-1)
    frequency = ROPE_BASE ** (-2.0 * jnp.arange(half_dim, dtype=F32) / HEAD_DIM)
    angles = own_pos.astype(F32)[:, None] * frequency[None, :]
    attended, grad_queries, grad_rows, weights, gain = layer(
        span_order, queries, d_attended, tokens.reshape(count, width), norm_gain.reshape(1, width),
        key_weight, value_weight, jnp.cos(angles), jnp.sin(angles),
    )
    attended, grad_queries, grad_rows, grad_keys, grad_values, gain = finish(
        attended, grad_queries, grad_rows, weights.reshape(2, 32, 512), gain
    )
    return (
        attended,
        grad_queries,
        grad_rows.reshape(seqs, rows, width),
        grad_keys,
        grad_values,
        gain.reshape(32),
    )


def solution(mesh):
    placed = (P("dp", "ctx", None), P("dp", "ctx", None), P("dp", "ctx", None), P(), P(), P(), P())
    return jax.shard_map(
        body,
        mesh=mesh,
        in_specs=placed,
        out_specs=(
            P("dp", "ctx", None),
            P("dp", "ctx", None),
            P("dp", "ctx", None),
            P(("ctx", "dp"), None),
            P(("ctx", "dp"), None),
            P(("ctx", "dp")),
        ),
        check_vma=False,
    )
```

```python
import functools
import math

import jax
import jax.numpy as jnp
from jax import lax
from jax.experimental import pallas as pl
from jax.experimental.pallas import tpu as pltpu
from jax.sharding import PartitionSpec as P

KV_HEADS = 4
HEAD_DIM = 128
ROPE_BASE = 500000.0
EPSILON = 1e-05
BF = jnp.bfloat16
F32 = jnp.float32
VM = pltpu.VMEM
MESH = pl.DeviceIdType.MESH


def flip1(a):
    return a + 1 - 2 * (a % 2)


def flip3(a):
    return 3 - a


def flip2(a):
    return (a + 2) % 4


class Here:
    def __init__(self):
        ctx = lax.axis_index("ctx")
        dp = lax.axis_index("dp")
        self.z = ctx // 8
        self.y = (ctx // 2) % 4
        self.xh = ctx % 2
        self.xl = dp // 2
        self.core = dp % 2
        self.x = self.xh * 2 + self.xl

    def at(self, z=None, y=None, x=None, core=None):
        z = self.z if z is None else z
        y = self.y if y is None else y
        core = self.core if core is None else core
        if x is None:
            xh, xl = self.xh, self.xl
        else:
            xh, xl = x // 2, x % 2
        return {"ctx": z * 8 + y * 2 + xh, "dp": xl * 2 + core}


class Net:
    def __init__(self, send_sems, recv_sems):
        self.send_sems = send_sems
        self.recv_sems = recv_sems
        self.made = []

    def start(self, src, dst, device):
        k = len(self.made)
        copy = pltpu.make_async_remote_copy(
            src_ref=src,
            dst_ref=dst,
            send_sem=self.send_sems.at[k],
            recv_sem=self.recv_sems.at[k],
            device_id=device,
            device_id_type=MESH,
        )
        copy.start()
        self.made.append(copy)
        return copy

    def finish(self):
        for copy in self.made:
            copy.wait_send()


def greet(devices):
    barrier = pltpu.get_barrier_semaphore()
    for device in devices:
        pl.semaphore_signal(barrier, inc=1, device_id=device, device_id_type=MESH)
    pl.semaphore_wait(barrier, len(devices))


def cols(index, width):
    return pl.ds(pl.multiple_of(index * width, width), width)


KEYS = 2048
CHUNK = 256
PIECES = 8
PARTS = (
    (0, 0, 128, "zyx", True),
    (1, 0, 128, "yxz", True),
    (2, 0, 256, "xzy", True),
    (0, 128, 384, "zyx", False),
    (1, 128, 384, "yxz", False),
    (2, 256, 256, "xzy", False),
    (3, 0, 256, "zyx", True),
    (3, 256, 256, "yxz", True),
)
N_COPIES = 41 + 34 + 1 + 9 * len(PARTS) + 10 + 1
SHAPES = dict(
    tokens=((128, 4096), BF),
    kw=((4096, 512), BF),
    vw=((4096, 512), BF),
    normed=((128, 4096), BF),
    acc=((2, 128, 512), F32),
    kv=((2, 64, 1024), BF),
    norm_t=((2, 4096, 128), BF),
    qr=((2, 4, 64, 512), BF),
    dr=((2, 4, 64, 512), BF),
    kvr=((2, 8, 4, 64, 256), BF),
    key_pos=((2, KEYS, 128), jnp.int32),
    score=((4, KEYS, 256), F32),
    prob=((4, KEYS, 256), BF),
    query_s=((4, 256, 128), BF),
    grad_s=((4, 256, 128), BF),
    grad_t=((4, 128, 256), BF),
    stats=((4, 2, 8, 256), F32),
    dq_t=((4, 128, 256), F32),
    key_t=((128, KEYS), BF),
    value_t=((128, KEYS), BF),
    att=((2, 4, 64, 512), BF),
    dq=((2, 4, 64, 512), BF),
    term=((2, 8, 4, 64, 256), BF),
    got1=((2, 3, 2, 4, 64, 256), BF),
    part=((2, 4, 64, 256), BF),
    got3=((2, 4, 64, 256), BF),
    final=((2, 4, 64, 256), BF),
    whole=((2, 4, 64, 256), BF),
    grads=((2, 128, 512), BF),
    got_grad=((128, 512), BF),
    big=((4, 4, 4, 4, 16, 512), BF),
    wide_grad=((128, 4096), F32),
    grad_rows=((128, 4096), BF),
    gain=((4, 8, 128), F32),
    r0=((4, 2, 4, 4, 16, 512), BF),
    s0=((4, 4, 4, 16, 512), BF),
    r1=((4, 4, 4, 16, 512), BF),
    s1=((4, 4, 4, 16, 512), BF),
    r2=((4, 3, 4, 16, 512), BF),
    s3=((4, 4, 16, 512), BF),
    r4=((4, 3, 16, 512), BF),
    full=((2, 2, 16, 512), F32),
    gain_got=((10, 8, 128), F32),
    gain_sum=((3, 8, 128), F32),
)


class Box:
    pass


def layer_kernel(
    spans, q, do, tokens_in, norm_gain, key_w, value_w, cos, sin,
    att_out, dq_out, rows_out, out, gain_out, *scratch,
):
    b = Box()
    for name, ref in zip(SHAPES, scratch):
        setattr(b, name, ref)
    send_sems, recv_sems, local_sems, weight_sems = scratch[len(SHAPES) :]
    tokens = b.tokens
    token_load = pltpu.make_async_copy(tokens_in, tokens, weight_sems.at[2 * PIECES])
    token_load.start()
    here = Here()
    place = {"z": here.z, "y": here.y, "x": here.x}
    z, y, xh = here.z, here.y, here.xh
    x2 = flip2(here.x)
    twin = here.at(core=1 - here.core)
    turns = (flip1, flip3, flip2)
    piece = 4096 // PIECES
    loads = []
    for c in range(PIECES):
        for w, (src, dst) in enumerate(((key_w, b.kw), (value_w, b.vw))):
            at = pl.ds(c * piece, piece)
            copy = pltpu.make_async_copy(src.at[at], dst.at[at], weight_sems.at[2 * c + w])
            copy.start()
            loads.append(copy)
    greet([here.at(**{a: f(place[a])}) for a in "zyx" for f in turns] + [twin])
    net = Net(send_sems, recv_sems)

    seq = [here.core, 1 - here.core]

    def either(s, a, b):
        return a * (1 - seq[s]) + b * seq[s]

    def along(s, value):
        return here.at(z=either(s, value, z), y=either(s, y, value))

    def across(s, value):
        return here.at(z=either(s, z, value), y=either(s, value, y))

    head = [either(s, z, y) for s in range(2)]
    ring = [either(s, y, z) for s in range(2)]
    mine = [ring[s] * 2 + xh for s in range(2)]
    local = []

    def keep(src, dst):
        copy = pltpu.make_async_copy(src, dst, local_sems.at[len(local)])
        copy.start()
        local.append(copy)
        return copy

    rows_in = [[], []]

    def send_rows(s, src, dst):
        for f in turns:
            to = f(head[s])
            rows_in[s].append(
                net.start(src.at[seq[s], :, cols(to, 512)], dst.at[s, head[s]], along(s, to))
            )
        rows_in[s].append(keep(src.at[seq[s], :, cols(head[s], 512)], dst.at[s, head[s]]))

    def arrived(copy):
        if any(copy is c for c in local):
            copy.wait()
        else:
            copy.wait_recv()

    send_rows(0, q, b.qr)
    token_load.wait()
    squares = jnp.zeros((128, 128), F32)
    for c in range(32):
        t = tokens[:, c * 128 : (c + 1) * 128].astype(F32)
        squares = squares + t * t
    rms = lax.rsqrt(jnp.sum(squares, axis=1, keepdims=True) / 4096.0 + EPSILON)
    for c in range(PIECES):
        at = slice(c * piece, (c + 1) * piece)
        b.normed[:, at] = (tokens[:, at].astype(F32) * rms * norm_gain[:, at]).astype(BF)
    for c in range(PIECES):
        at = slice(c * piece, (c + 1) * piece)
        n = b.normed[:, at]
        for w, ref in enumerate((b.kw, b.vw)):
            loads[2 * c + w].wait()
            product = jnp.dot(n, ref[at, :], preferred_element_type=F32)
            if c == 0:
                b.acc[w] = product
            else:
                b.acc[w] += product

    def widen(half):
        both = jnp.concatenate([half, half], axis=1)
        return jnp.concatenate([both, both], axis=0)

    lane = lax.broadcasted_iota(jnp.int32, (128, 128), 1)
    both_cos = widen(cos[...])
    both_sin = widen(sin[...])
    both_sin = jnp.where(lane < 64, -both_sin, both_sin)
    for h in range(KV_HEADS):
        at = slice(h * 128, (h + 1) * 128)
        u = b.acc[0, :, at]
        k = (u * both_cos + pltpu.roll(u, 64, 1) * both_sin).astype(BF)
        v = b.acc[1, :, at].astype(BF)
        for s in range(2):
            b.kv[s, :, h * 256 : h * 256 + 128] = k[s * 64 : (s + 1) * 64]
            b.kv[s, :, h * 256 + 128 : (h + 1) * 256] = v[s * 64 : (s + 1) * 64]

    kv_in = [[], []]
    for s in range(2):
        for f in (flip2, flip1, flip3):
            to = f(head[s])
            kv_in[s].append(
                net.start(
                    b.kv.at[seq[s], :, cols(to, 256)], b.kvr.at[s, mine[s], head[s]], along(s, to)
                )
            )
        own = b.kv.at[seq[s], :, cols(head[s], 256)]
        kv_in[s].append(keep(own, b.kvr.at[s, mine[s], head[s]]))
    for c in range(32):
        at = slice(c * 128, (c + 1) * 128)
        b.norm_t[0, at, :] = b.normed[:, at].T

    last = [[], []]
    swapped = {}

    def half_of(half):
        return slice(2 * half, 2 * half + 2)

    def spread(s, of, rows):
        block = b.kvr.at[s, ring[s] * 2 + (xh if of == 0 else 1 - xh), rows]
        for f in (flip2, flip1, flip3):
            last[s].append(net.start(block, block, across(s, f(ring[s]))))

    def gather_own(s):
        for copy in kv_in[s]:
            arrived(copy)
        for half in range(2):
            block = b.kvr.at[s, mine[s], half_of(half)]
            swapped[s, half] = net.start(block, block, here.at(x=x2))
        spread(s, 0, slice(0, 4))

    def gather_swapped(s):
        for half in range(2):
            swapped[s, half].wait_recv()
            spread(s, 1, half_of(half))

    gather_own(0)
    offset = lax.broadcasted_iota(jnp.int32, (32, 128), 0)
    for i in range(64):
        m, w, n, half = i // 16, (i // 8) % 2, (i // 2) % 4, i % 2
        for s in range(2):
            at_z, at_y = ((n * 4 + m) * 2 + w) * 2 + half, ((m * 4 + n) * 2 + w) * 2 + half
            span = spans[either(s, at_z, at_y)]
            b.key_pos[s, i * 32 : (i + 1) * 32, :] = offset + span * 32
    gather_swapped(0)
    send_rows(0, do, b.dr)
    gather_own(1)

    scale = HEAD_DIM ** (-0.5)
    to_two = scale * math.log2(math.e)
    slots_of = [slice(c * CHUNK, (c + 1) * CHUNK) for c in range(KEYS // CHUNK)]
    returned = []

    def keys_of(s, c):
        return b.kvr[s, c, :, :, :128].reshape(CHUNK, 128)

    def values_of(s, c):
        return b.kvr[s, c, :, :, 128:].reshape(CHUNK, 128)

    def ready(s):
        for copy in last[s]:
            copy.wait_recv()
        for copy in rows_in[s]:
            arrived(copy)
        for c, rows in enumerate(slots_of):
            b.key_t[:, rows] = keys_of(s, c).T
            b.value_t[:, rows] = values_of(s, c).T

    def stack(ref, s, block):
        both = ref[s, block]
        return jnp.concatenate([both[:, h * 128 : (h + 1) * 128] for h in range(4)], axis=0)

    def side(k):
        return 1 - xh if k == 0 else xh

    def block_of(s, order):
        return (flip1, flip3, flip2, lambda a: a)[order](head[s])

    def give_back(s, order, src, dst):
        block = block_of(s, order)
        dst = dst.at[seq[s], :, cols(head[s], 512)]
        if order < 3:
            returned.append(net.start(src.at[s, block], dst, along(s, block)))
        else:
            returned.append(keep(src.at[s, block], dst))

    def attention(s, order):
        block = block_of(s, order)
        score, prob = b.score.at[order], b.prob.at[order]
        queries = stack(b.qr, s, block)
        grads = stack(b.dr, s, block)
        q_t = queries.T
        do_t = grads.T
        b.query_s[order] = queries
        b.grad_s[order] = grads
        b.grad_t[order] = do_t
        start = either(s, (block * 4 + y) * 4, (z * 4 + block) * 4) + xh * 2
        column = lax.broadcasted_iota(jnp.int32, (1, 256), 1)
        q_pos = column % 32 + 32 * jnp.where(column % 64 < 32, spans[start], spans[start + 1])
        top = jnp.full((8, 256), -1e30, F32)
        for c, rows in enumerate(slots_of):
            t = jnp.dot(keys_of(s, c), q_t, preferred_element_type=F32)
            k_pos = b.key_pos[s, rows, :]
            k_pos = jnp.concatenate([k_pos, k_pos], axis=1)
            t = jnp.where(k_pos <= q_pos, t, -1e30)
            score[rows, :] = t
            top = jnp.maximum(top, jnp.max(t.reshape(CHUNK // 8, 8, 256), axis=0))
        top = jnp.max(top, axis=0, keepdims=True)
        total = jnp.zeros((8, 256), F32)
        for rows in slots_of:
            e = jnp.exp2((score[rows, :] - top) * to_two)
            score[rows, :] = e
            total = total + jnp.sum(e.reshape(CHUNK // 8, 8, 256), axis=0)
        inverse = 1.0 / jnp.sum(total, axis=0, keepdims=True)
        out_t = jnp.zeros((128, 256), F32)
        for rows in slots_of:
            p = (score[rows, :] * inverse).astype(BF)
            prob[rows, :] = p
            out_t = out_t + jnp.dot(b.value_t[:, rows], p, preferred_element_type=F32)
        out_t = out_t.astype(BF)
        delta = jnp.sum(out_t.astype(F32) * do_t.astype(F32), axis=0, keepdims=True)
        b.stats[order, 0] = jnp.broadcast_to(inverse, (8, 256))
        b.stats[order, 1] = jnp.broadcast_to(delta, (8, 256))
        attended = out_t.T
        for h in range(4):
            b.att[s, block, :, h * 128 : (h + 1) * 128] = attended[h * 64 : (h + 1) * 64]
        give_back(s, order, b.att, att_out)

    def gradients(s, k):
        for c in range(4):
            slot = c * 2 + side(k)
            rows = pl.ds(pl.multiple_of(slot * CHUNK, CHUNK), CHUNK)
            values = values_of(s, slot)
            keys = b.key_t[:, rows]
            k_term = jnp.zeros((CHUNK, 128), F32)
            v_term = jnp.zeros((CHUNK, 128), F32)
            for order in range(4):
                inverse, delta = b.stats[order, 0, :1], b.stats[order, 1, :1]
                dp = jnp.dot(values, b.grad_t[order], preferred_element_type=F32)
                ds = (b.score[order, rows, :] * inverse * (dp - delta)).astype(BF)
                k_term = k_term + jnp.dot(ds, b.query_s[order], preferred_element_type=F32)
                v_term = v_term + jnp.dot(
                    b.prob[order, rows, :], b.grad_s[order], preferred_element_type=F32
                )
                dq = jnp.dot(keys, ds, preferred_element_type=F32)
                if k == 0 and c == 0:
                    b.dq_t[order] = dq
                else:
                    b.dq_t[order] += dq
            b.term[s, slot, :, :, :128] = (k_term * scale).astype(BF).reshape(4, 64, 128)
            b.term[s, slot, :, :, 128:] = v_term.astype(BF).reshape(4, 64, 128)

    def give_query_grads(s):
        for order in range(4):
            dq = (b.dq_t[order] * scale).astype(BF).T
            for h in range(4):
                b.dq[s, block_of(s, order), :, h * 128 : (h + 1) * 128] = dq[h * 64 : (h + 1) * 64]
            give_back(s, order, b.dq, dq_out)

    one, three, owners = {}, {}, [[], []]

    def sum_one(s, k):
        for i, f in enumerate((flip2, flip1, flip3)):
            target = f(ring[s])
            one[s, i, k] = net.start(
                b.term.at[s, target * 2 + side(k)], b.got1.at[s, i, k], across(s, target)
            )

    def summed(s, k):
        total = b.term[s, ring[s] * 2 + side(k)].astype(F32)
        for i in range(3):
            one[s, i, k].wait_recv()
            total = total + b.got1[s, i, k].astype(F32)
        return total

    def sum_three(s):
        b.part[s] = summed(s, 0).astype(BF)
        three[s] = net.start(b.part.at[s], b.got3.at[s], here.at(x=x2))

    def sum_four(s):
        total = summed(s, 1)
        three[s].wait_recv()
        b.final[s] = (total + b.got3[s].astype(F32)).astype(BF)
        for f in (flip2, flip1, flip3):
            to = f(head[s])
            owners[s].append(
                net.start(b.final.at[s, to], b.whole.at[s, head[s]], along(s, to))
            )
        b.whole[s, head[s]] = b.final[s, head[s]]

    def rotate_rows(s):
        for copy in owners[s]:
            copy.wait_recv()
        rows = pl.ds(pl.multiple_of(seq[s] * 64, 64), 64)
        for h in range(KV_HEADS):
            at = slice(h * 128, (h + 1) * 128)
            u = b.whole[s, h, :, :128].astype(F32)
            b.grads[0, rows, at] = (
                u * both_cos[:64] - pltpu.roll(u, 64, 1) * both_sin[:64]
            ).astype(BF)
            b.grads[1, rows, at] = b.whole[s, h, :, 128:]

    ready(0)
    send_rows(1, q, b.qr)
    send_rows(1, do, b.dr)
    norm_in = net.start(b.norm_t.at[0], b.norm_t.at[1], twin)
    attention(0, 0)
    gather_swapped(1)
    attention(0, 1)
    attention(0, 2)
    attention(0, 3)
    gradients(0, 0)
    sum_one(0, 0)
    gradients(0, 1)
    sum_one(0, 1)
    give_query_grads(0)
    ready(1)
    attention(1, 0)
    attention(1, 1)
    attention(1, 2)
    sum_three(0)
    attention(1, 3)
    gradients(1, 0)
    sum_one(1, 0)
    sum_four(0)
    gradients(1, 1)
    sum_one(1, 1)
    sum_three(1)
    give_query_grads(1)
    rotate_rows(0)
    sum_four(1)
    rotate_rows(1)

    swap_grad = net.start(b.grads.at[1 - here.core], b.got_grad, twin)
    norm_in.wait_recv()
    swap_grad.wait_recv()
    pair = jnp.concatenate([b.grads[here.core], b.got_grad[...]], axis=0)

    @pl.loop(0, 16, unroll=4)
    def _(i):
        at = pl.ds(pl.multiple_of(i * 256, 256), 256)
        n = jnp.concatenate([b.norm_t[0, at, :], b.norm_t[1, at, :]], axis=1)
        w = jnp.dot(n, pair, preferred_element_type=F32).astype(BF)
        for x in range(4):
            for u in range(4):
                row = x * 64 + u * 16
                b.big[u, i // 4, i % 4, x] = w[row : row + 16]

    def backward_rows():
        key_grad, value_grad = b.grads[0], b.grads[1]
        nt = (((1,), (1,)), ((), ()))
        inner = jnp.zeros((128, 128), F32)
        for c in range(16):
            at = slice(c * 256, (c + 1) * 256)
            ng = lax.dot_general(key_grad, b.kw[at, :], nt, preferred_element_type=F32)
            ng = ng + lax.dot_general(value_grad, b.vw[at, :], nt, preferred_element_type=F32)
            t = tokens[:, at].astype(F32)
            b.wide_grad[:, at] = ng
            across_rows = jnp.sum(ng * t * rms, axis=0, keepdims=True)
            weighted = ng * norm_gain[:, at] * t
            inner = inner + weighted[:, :128] + weighted[:, 128:]
            for k in range(2):
                row = c * 2 + k
                b.gain[row // 8, row % 8 : row % 8 + 1, :] = across_rows[:, k * 128 : (k + 1) * 128]
        mean = jnp.sum(inner, axis=1, keepdims=True) / 4096.0
        cube = rms**3 * mean
        for c in range(16):
            at = slice(c * 256, (c + 1) * 256)
            b.grad_rows[:, at] = (
                rms * norm_gain[:, at] * b.wide_grad[:, at] - tokens[:, at].astype(F32) * cube
            ).astype(BF)

    def device(axis, value):
        return here.at(**{axis: value})

    plans = []
    for u, lo, width, order, up in PARTS:
        f, f2 = (flip1, flip3) if up else (flip3, flip1)
        a0, a1, a2 = order
        left = [a for a in "zyx" if a != a0]
        plans.append((u, pl.ds(lo, width), f, f2, a0, a1, a2, left.index(a1) == 0))

    def slab(u, axis, value, lanes):
        if axis == "z":
            return b.big.at[u, value, :, :, :, lanes]
        if axis == "y":
            return b.big.at[u, :, value, :, :, lanes]
        return b.big.at[u, :, :, value, :, lanes]

    def slab1(u, value, lanes, leading):
        return b.s1.at[u, value, :, :, lanes] if leading else b.s1.at[u, :, value, :, lanes]

    def wide(ref):
        return ref[...].astype(F32)

    gains = []

    def gain_step(step):
        if step == 0:
            tiles = [b.gain.at[f(z)] for f in turns]
            own = None
        else:
            own = b.gain[z] if step == 1 else b.gain_sum[step - 2]
            for k in range(3):
                gains[k].wait_recv()
                own = own + b.gain_got[3 * (step - 1) + k]
            del gains[:]
            b.gain_sum[step - 1] = own
            tiles = [b.gain_sum.at[step - 1]] * 3
        if step < 3:
            axis = "zyx"[step]
            for k, f in enumerate(turns):
                gains.append(
                    net.start(tiles[k], b.gain_got.at[3 * step + k], device(axis, f(place[axis])))
                )
        else:
            gains.append(net.start(tiles[0], b.gain_got.at[9], twin))

    waits = {}
    for j in (1, 0):
        for p, (u, lanes, f, f2, a0, a1, a2, leading) in enumerate(plans):
            m0 = place[a0]
            slot = flip2(m0) if j == 1 else f(m0)
            waits[p, 0, j] = net.start(
                slab(u, a0, slot, lanes), b.r0.at[u, j, :, :, :, lanes], device(a0, f(m0))
            )
    backward_rows()
    keep_rows = keep(b.grad_rows, rows_out)
    gain_step(0)
    for p, (u, lanes, f, f2, a0, a1, a2, leading) in enumerate(plans):
        m0 = place[a0]
        waits[p, 0, 1].wait_recv()
        b.s0[u, :, :, :, lanes] = (
            wide(slab(u, a0, f2(m0), lanes)) + b.r0[u, 1, :, :, :, lanes].astype(F32)
        ).astype(BF)
        waits[p, 1] = net.start(
            b.s0.at[u, :, :, :, lanes], b.r1.at[u, :, :, :, lanes], device(a0, f2(m0))
        )
    gain_step(1)
    for p, (u, lanes, f, f2, a0, a1, a2, leading) in enumerate(plans):
        m0, m1 = place[a0], place[a1]
        waits[p, 0, 0].wait_recv()
        waits[p, 1].wait_recv()
        b.s1[u, :, :, :, lanes] = (
            wide(slab(u, a0, m0, lanes))
            + b.r0[u, 0, :, :, :, lanes].astype(F32)
            + b.r1[u, :, :, :, lanes].astype(F32)
        ).astype(BF)
        for k, turn in enumerate(turns):
            waits[p, 2, k] = net.start(
                slab1(u, turn(m1), lanes, leading),
                b.r2.at[u, k, :, :, lanes],
                device(a1, turn(m1)),
            )
    gain_step(2)
    for p, (u, lanes, f, f2, a0, a1, a2, leading) in enumerate(plans):
        m1, m2 = place[a1], place[a2]
        total = wide(slab1(u, m1, lanes, leading))
        for k in range(3):
            waits[p, 2, k].wait_recv()
            total = total + b.r2[u, k, :, :, lanes].astype(F32)
        b.s3[u, :, :, lanes] = total.astype(BF)
        for k, turn in enumerate(turns):
            waits[p, 3, k] = net.start(
                b.s3.at[u, turn(m2), :, lanes], b.r4.at[u, k, :, lanes], device(a2, turn(m2))
            )
    gain_step(3)
    for p, (u, lanes, f, f2, a0, a1, a2, leading) in enumerate(plans):
        total = b.s3[u, place[a2], :, lanes].astype(F32)
        for k in range(3):
            waits[p, 3, k].wait_recv()
            total = total + b.r4[u, k, :, lanes].astype(F32)
        b.full[u // 2, u % 2, :, lanes] = total
    swap = net.start(b.full.at[1 - here.core], out.at[here.core], twin)
    out[here.core] = b.full[here.core]
    gains[0].wait_recv()
    gain_out[...] = b.gain_sum[2] + b.gain_got[9]
    swap.wait_recv()
    for copy in returned:
        arrived(copy)
    keep_rows.wait()
    net.finish()


def layer(spans, q, do, tokens, norm_gain, key_w, value_w, cos, sin):
    vm = pl.BlockSpec(memory_space=VM)
    any_ = pl.BlockSpec(memory_space=pl.ANY)
    return pl.pallas_call(
        layer_kernel,
        name="layer",
        out_shape=(
            jax.ShapeDtypeStruct((2, 64, 2048), BF),
            jax.ShapeDtypeStruct((2, 64, 2048), BF),
            jax.ShapeDtypeStruct((128, 4096), BF),
            jax.ShapeDtypeStruct((2, 2, 16, 512), F32),
            jax.ShapeDtypeStruct((8, 128), F32),
        ),
        in_specs=[pl.BlockSpec(memory_space=pltpu.SMEM), any_, any_, any_, vm, any_, any_, vm, vm],
        out_specs=(any_,) * 3 + (vm,) * 2,
        scratch_shapes=[VM(*shape) for shape in SHAPES.values()]
        + [
            pltpu.SemaphoreType.DMA((N_COPIES,)),
            pltpu.SemaphoreType.DMA((N_COPIES,)),
            pltpu.SemaphoreType.DMA((12,)),
            pltpu.SemaphoreType.DMA((2 * PIECES + 1,)),
        ],
        compiler_params=pltpu.CompilerParams(
            collective_id=1, has_side_effects=True, vmem_limit_bytes=60 * 1024 * 1024
        ),
    )(spans, q, do, tokens, norm_gain, key_w, value_w, cos, sin)


def finish_kernel(
    att, dq, rows, weights, gain, att_to, dq_to, rows_to, keys_to, values_to, gain_to,
    att_v, dq_v, rows_v, weights_v, gain_v, sems,
):
    here = Here()
    loads = []
    for k, (src, dst) in enumerate(
        ((gain, gain_v), (att, att_v), (dq, dq_v), (rows, rows_v), (weights, weights_v))
    ):
        copy = pltpu.make_async_copy(src, dst, sems.at[k])
        copy.start()
        loads.append(copy)
    loads[0].wait()
    row = gain_v[pl.ds(here.y * 2 + here.xh, 1), :]
    dp = here.xl * 2 + here.core
    gain_to[...] = pltpu.roll(row, (128 - dp * 32) % 128, 1)[:, :32]
    stores = []
    for k, (load, src, dst) in enumerate(
        (
            (loads[1], att_v, att_to),
            (loads[2], dq_v, dq_to),
            (loads[3], rows_v, rows_to),
            (loads[4], weights_v.at[0], keys_to),
            (None, weights_v.at[1], values_to),
        )
    ):
        if load is not None:
            load.wait()
        copy = pltpu.make_async_copy(src, dst, sems.at[5 + k])
        copy.start()
        stores.append(copy)
    for copy in stores:
        copy.wait()


def finish(att, dq, rows, weights, gain):
    any_ = pl.BlockSpec(memory_space=pl.ANY)
    return pl.pallas_call(
        finish_kernel,
        name="finish",
        out_shape=(
            jax.ShapeDtypeStruct((2, 64, 2048), BF),
            jax.ShapeDtypeStruct((2, 64, 2048), BF),
            jax.ShapeDtypeStruct((128, 4096), BF),
            jax.ShapeDtypeStruct((32, 512), F32),
            jax.ShapeDtypeStruct((32, 512), F32),
            jax.ShapeDtypeStruct((1, 32), F32),
        ),
        in_specs=[any_] * 5,
        out_specs=(any_,) * 5 + (pl.BlockSpec(memory_space=VM),),
        scratch_shapes=[
            VM((2, 64, 2048), BF),
            VM((2, 64, 2048), BF),
            VM((128, 4096), BF),
            VM((2, 32, 512), F32),
            VM((8, 128), F32),
            pltpu.SemaphoreType.DMA((10,)),
        ],
        compiler_params=pltpu.CompilerParams(vmem_limit_bytes=60 * 1024 * 1024),
    )(att, dq, rows, weights, gain)


def body(tokens, queries, d_attended, span_order, norm_gain, key_weight, value_weight):
    seqs, rows, width = tokens.shape
    count = seqs * rows
    half_dim = HEAD_DIM // 2
    span_len = rows // 2
    own_spans = lax.dynamic_slice_in_dim(span_order, lax.axis_index("ctx") * 2, 2, 0)
    own_pos = (own_spans[:, None] * span_len + jnp.arange(span_len, dtype=jnp.int32)).reshape(-1)
    frequency = ROPE_BASE ** (-2.0 * jnp.arange(half_dim, dtype=F32) / HEAD_DIM)
    angles = own_pos.astype(F32)[:, None] * frequency[None, :]
    attended, grad_queries, grad_rows, weights, gain = layer(
        span_order, queries, d_attended, tokens.reshape(count, width), norm_gain.reshape(1, width),
        key_weight, value_weight, jnp.cos(angles), jnp.sin(angles),
    )
    attended, grad_queries, grad_rows, grad_keys, grad_values, gain = finish(
        attended, grad_queries, grad_rows, weights.reshape(2, 32, 512), gain
    )
    return (
        attended,
        grad_queries,
        grad_rows.reshape(seqs, rows, width),
        grad_keys,
        grad_values,
        gain.reshape(32),
    )


def solution(mesh):
    placed = (P("dp", "ctx", None), P("dp", "ctx", None), P("dp", "ctx", None), P(), P(), P(), P())
    return jax.shard_map(
        body,
        mesh=mesh,
        in_specs=placed,
        out_specs=(
            P("dp", "ctx", None),
            P("dp", "ctx", None),
            P("dp", "ctx", None),
            P(("ctx", "dp"), None),
            P(("ctx", "dp"), None),
            P(("ctx", "dp")),
        ),
        check_vma=False,
    )
```
